32 devices in a mesh: dp: 16 (over z, x, core), tensor: 2 (over y).
Axes of the slice: x: 2, y: 2, z: 4, core: 2. Of those that a mesh axis runs over, the one named last changes fastest.
Arguments:
- layer_input: float32 [4096, 2048], P('dp'), may hold values from -6 to 6
- positions: int32 [4096], P('dp'), may hold values from 0 to 2047, as said below
- norm1_gain: bfloat16 [2048], P('dp'), may hold values from 0.5 to 1.5
- w_q: bfloat16 [2048, 2048], P('dp', 'tensor'), may hold values from -0.125 to 0.125
- w_k: bfloat16 [2048, 256], P('dp', 'tensor'), may hold values from -0.125 to 0.125
- w_v: bfloat16 [2048, 256], P('dp', 'tensor'), may hold values from -0.125 to 0.125
- w_o: bfloat16 [2048, 2048], P('tensor', 'dp'), may hold values from -0.5 to 0.5
- norm2_gain: bfloat16 [2048], P('dp'), may hold values from 0.5 to 1.5
- w_gate: bfloat16 [2048, 5632], P('dp', 'tensor'), may hold values from -0.125 to 0.125
- w_up: bfloat16 [2048, 5632], P('dp', 'tensor'), may hold values from -0.125 to 0.125
- w_down: bfloat16 [5632, 2048], P('tensor', 'dp'), may hold values from -0.078125 to 0.078125
- out_grad: float32 [4096, 2048], P('dp'), may hold values from -6 to 6
Outputs:
- layer_output: float32 [4096, 2048], P('dp')
- x_grad: float32 [4096, 2048], P('dp')
- grad_norm1: float32 [2048], P('dp')
- grad_w_q: float32 [2048, 2048], P('dp', 'tensor')
- grad_w_k: float32 [2048, 256], P('dp', 'tensor')
- grad_w_v: float32 [2048, 256], P('dp', 'tensor')
- grad_w_o: float32 [2048, 2048], P('tensor', 'dp')
- grad_norm2: float32 [2048], P('dp')
- grad_w_gate: float32 [2048, 5632], P('dp', 'tensor')
- grad_w_up: float32 [2048, 5632], P('dp', 'tensor')
- grad_w_down: float32 [5632, 2048], P('tensor', 'dp')
The draws below stay inside these ranges and needn't reach their ends.
Inputs may be any that keep to these rules, and one draw needn't show every extreme that they name: Each sequence of 256 tokens packs one or two documents; positions rise by one from token to token within a document and restart at 0 where a second document begins.
All inputs are finite; a program needn't handle non-finite values.
Results may differ from the reference program's by a relative error of at most 0.015.
Values may be sent and summed in bfloat16 or wider, within the bound.
A program may use at most 256 MiB of HBM per device.

```python
import math
import jax
import jax.numpy as jnp
from jax import lax

D = 2048
HQ = 32
KV = 4
HD = 64
FF = 5632
MAXPOS = 2048
L = 256
TOKENS = 4096


def draw_positions(key, part):
    seq_count = TOKENS // L
    starts = jax.random.randint(jax.random.fold_in(key, 21), (seq_count,), 0, MAXPOS - L + 1).astype(jnp.int32)
    cuts = jax.random.randint(jax.random.fold_in(key, 22), (seq_count,), 1, L).astype(jnp.int32)
    seq_order = jnp.arange(seq_count, dtype=jnp.int32)
    starts = jnp.where(seq_order == 0, 0, starts)
    starts = jnp.where(seq_order == seq_count - 1, MAXPOS - L, starts).astype(jnp.int32)
    cuts = jnp.where(seq_order == seq_count - 1, L, cuts).astype(jnp.int32)
    steps_in = jnp.arange(L, dtype=jnp.int32)[None, :]
    first_doc = starts[:, None] + steps_in
    second_doc = steps_in - cuts[:, None]
    rows = jnp.where(steps_in < cuts[:, None], first_doc, second_doc)
    return rows.reshape(TOKENS).astype(jnp.int32)


def shard_levels(stream_key, dims, shards, least, largest):
    def one(axis_at, parts):
        draws = jax.random.uniform(jax.random.fold_in(jax.random.fold_in(stream_key, 6), axis_at), (parts,), jnp.float32, least / len(shards), largest / len(shards))
        return jnp.repeat(jnp.exp(draws), dims[axis_at] // parts).reshape((-1,) + (1,) * (len(dims) - axis_at - 1))

    level = one(*shards[0])
    for cut in shards[1:]:
        level = level * one(*cut)
    return level


def bell_draw(rng, shape, deviation, reach, shards=(), kind=jnp.bfloat16):
    factor_of = shard_levels(rng, shape, shards, -0.22, 0.18) if shards else 1.0
    result = jax.random.normal(rng, shape, jnp.float32) * deviation * factor_of
    return jnp.minimum(jnp.maximum(result, -reach), reach).astype(kind)


def setup_inputs(seed: int = 0) -> dict:
    key_list = jax.random.split(jax.random.key(seed), 13)
    layer_input = bell_draw(key_list[0], (TOKENS, D), 1.0, 6.0, ((0, 16),), jnp.float32)
    positions = draw_positions(jax.random.fold_in(key_list[12], 71), 0)
    norm1_gain = jnp.clip(1.0 + 0.1 * jax.random.normal(key_list[2], (D,), jnp.float32), 0.5, 1.5).astype(jnp.bfloat16)
    w_q = bell_draw(key_list[3], (D, HQ * HD), D ** -0.5, 0.125, ((0, 16), (1, 2)))
    w_k = bell_draw(key_list[4], (D, KV * HD), D ** -0.5, 0.125, ((0, 16), (1, 2)))
    w_v = bell_draw(key_list[5], (D, KV * HD), D ** -0.5, 0.125, ((0, 16), (1, 2)))
    w_o = bell_draw(key_list[6], (HQ * HD, D), (max(HQ * HD // 16, 1)) ** -0.5, 0.5, ((0, 2), (1, 16)))
    norm2_gain = jnp.clip(1.0 + 0.1 * jax.random.normal(key_list[7], (D,), jnp.float32), 0.5, 1.5).astype(jnp.bfloat16)
    w_gate = bell_draw(key_list[8], (D, FF), D ** -0.5, 0.125, ((0, 16), (1, 2)))
    w_up = bell_draw(key_list[9], (D, FF), D ** -0.5, 0.125, ((0, 16), (1, 2)))
    w_down = bell_draw(key_list[10], (FF, D), FF ** -0.5, 0.078125, ((0, 2), (1, 16)))
    out_grad = bell_draw(key_list[11], (TOKENS, D), 1.0, 6.0, ((0, 16),), jnp.float32)
    return {"layer_input": layer_input, "positions": positions, "norm1_gain": norm1_gain, "w_q": w_q, "w_k": w_k, "w_v": w_v, "w_o": w_o, "norm2_gain": norm2_gain, "w_gate": w_gate, "w_up": w_up, "w_down": w_down, "out_grad": out_grad}


epsilon = 1e-05

def matmul(left_side, right_side):
    return jnp.dot(left_side, right_side, preferred_element_type=jnp.float32)

def matmul_nt(left_side, right_side):
    return lax.dot_general(left_side, right_side, (((1,), (1,)), ((), ())), preferred_element_type=jnp.float32)

def matmul_tn(left_side, right_side):
    return lax.dot_general(left_side, right_side, (((0,), (0,)), ((), ())), preferred_element_type=jnp.float32)

def rms_parts(row_values):
    inv_rms = lax.rsqrt(lax.optimization_barrier(jnp.mean(row_values * row_values, axis=-1, keepdims=True)) + epsilon)
    return (inv_rms, row_values * inv_rms)

def rope_tables(pos_rows, head_dim):
    half_dim = head_dim // 2
    frequency = jnp.exp(jnp.arange(half_dim, dtype=jnp.float32) * (-2.0 * math.log(10000.0) / head_dim))
    angles = pos_rows.astype(jnp.float32)[:, None] * frequency[None, :]
    return (jnp.cos(angles), jnp.sin(angles))

def rotate(row_values, cos_table, sin_table, direction_sign):
    half_dim = row_values.shape[-1] // 2
    first_half = row_values[..., :half_dim]
    second = row_values[..., half_dim:]
    cos_part = cos_table[:, None, :]
    sin_part = sin_table[:, None, :] * direction_sign
    return jnp.concatenate([first_half * cos_part - second * sin_part, second * cos_part + first_half * sin_part], axis=-1)

def causal_scores(queries, key_rows):
    length, head_count, head_dim = queries.shape
    kv_count = key_rows.shape[1]
    grouped = queries.reshape(length, kv_count, head_count // kv_count, head_dim)
    scores = jnp.einsum('qkgd,pkd->kgqp', grouped.astype(jnp.float32), key_rows.astype(jnp.float32)) * head_dim ** (-0.5)
    future_mask = jnp.arange(length)[None, :] > jnp.arange(length)[:, None]
    return (grouped, jnp.where(future_mask, -jnp.inf, scores))

def attend(queries, key_rows, value_rows):
    grouped, scores = causal_scores(queries, key_rows)
    row_top = lax.optimization_barrier(jnp.max(scores, axis=-1, keepdims=True))
    log_total = row_top + jnp.log(lax.optimization_barrier(jnp.sum(jnp.exp(scores - row_top), axis=-1, keepdims=True)))
    weights = jnp.exp(scores - log_total).astype(jnp.bfloat16)
    attended = jnp.einsum('kgqp,pkd->qkgd', weights.astype(jnp.float32), value_rows.astype(jnp.float32))
    return (attended.reshape(queries.shape[0], -1).astype(jnp.bfloat16), log_total)

def attend_back(queries, key_rows, value_rows, attended, d_attended, log_total):
    length, head_count, head_dim = queries.shape
    kv_count = key_rows.shape[1]
    grouped, scores = causal_scores(queries, key_rows)
    prob_rows = jnp.exp(scores - log_total)
    d_grouped = d_attended.reshape(length, kv_count, head_count // kv_count, head_dim)
    out_grouped = attended.reshape(length, kv_count, head_count // kv_count, head_dim)
    row_delta = lax.optimization_barrier(jnp.sum(out_grouped.astype(jnp.float32) * d_grouped.astype(jnp.float32), axis=-1))
    row_delta = jnp.transpose(row_delta, (1, 2, 0))[..., None]
    d_probs = jnp.einsum('qkgd,pkd->kgqp', d_grouped.astype(jnp.float32), value_rows.astype(jnp.float32))
    d_scores = (prob_rows * (d_probs - row_delta) * head_dim ** (-0.5)).astype(jnp.bfloat16)
    d_query = jnp.einsum('kgqp,pkd->qkgd', d_scores.astype(jnp.float32), key_rows.astype(jnp.float32))
    d_keys = jnp.einsum('kgqp,qkgd->pkd', d_scores.astype(jnp.float32), grouped.astype(jnp.float32))
    weights = prob_rows.astype(jnp.bfloat16).astype(jnp.float32)
    d_values = jnp.einsum('kgqp,qkgd->pkd', weights, d_grouped.astype(jnp.float32))
    return (d_query.reshape(length, head_count, head_dim), d_keys, d_values)

def layer_pass(x_rows, pos_rows, grad_in, norm1_gain, w_q, w_k, w_v, w_o, norm2_gain, w_gate, w_up, w_down):
    row_count = x_rows.shape[0]
    seq_count = row_count // L
    head_count = w_q.shape[1] // HD
    kv_count = w_k.shape[1] // HD
    gain_one = norm1_gain.astype(jnp.float32)
    gain_two = norm2_gain.astype(jnp.float32)
    inv_one, norm_one = rms_parts(x_rows)
    normed_one = (norm_one * gain_one).astype(jnp.bfloat16)
    cos_table, sin_table = rope_tables(pos_rows, HD)
    queries = rotate(matmul(normed_one, w_q).reshape(row_count, head_count, HD), cos_table, sin_table, 1.0).astype(jnp.bfloat16)
    key_rows = rotate(matmul(normed_one, w_k).reshape(row_count, kv_count, HD), cos_table, sin_table, 1.0).astype(jnp.bfloat16)
    value_rows = matmul(normed_one, w_v).astype(jnp.bfloat16).reshape(row_count, kv_count, HD)
    query_seq = queries.reshape(seq_count, L, head_count, HD)
    key_seq = key_rows.reshape(seq_count, L, kv_count, HD)
    value_seq = value_rows.reshape(seq_count, L, kv_count, HD)
    attended, log_total = lax.map(lambda block_in: attend(block_in[0], block_in[1], block_in[2]), (query_seq, key_seq, value_seq))
    attended_rows = attended.reshape(row_count, head_count * HD)
    hidden = x_rows + matmul(attended_rows, w_o)
    inv_two, norm_two = rms_parts(hidden)
    normed_two = (norm_two * gain_two).astype(jnp.bfloat16)
    gate_pre = matmul(normed_two, w_gate)
    up_pre = matmul(normed_two, w_up)
    activated = (jax.nn.silu(gate_pre) * up_pre).astype(jnp.bfloat16)
    out_rows = hidden + matmul(activated, w_down)
    grad_rows = grad_in.astype(jnp.bfloat16)
    d_act = matmul_nt(grad_rows, w_down)
    sigmoid_gate = jax.nn.sigmoid(gate_pre)
    d_gate = (d_act * up_pre * sigmoid_gate * (1.0 + gate_pre * (1.0 - sigmoid_gate))).astype(jnp.bfloat16)
    d_up = (d_act * jax.nn.silu(gate_pre)).astype(jnp.bfloat16)
    grad_down = matmul_tn(activated, grad_rows)
    grad_gate = matmul_tn(normed_two, d_gate)
    grad_up = matmul_tn(normed_two, d_up)
    d_norm_two = matmul_nt(d_gate, w_gate) + matmul_nt(d_up, w_up)
    grad_gain_two = lax.optimization_barrier(jnp.sum(d_norm_two * norm_two, axis=0))
    e_two = d_norm_two * gain_two
    d_hidden = grad_in + inv_two * (e_two - norm_two * lax.optimization_barrier(jnp.mean(e_two * norm_two, axis=-1, keepdims=True)))
    hidden_rows = d_hidden.astype(jnp.bfloat16)
    grad_out = matmul_tn(attended_rows, hidden_rows)
    d_attended = matmul_nt(hidden_rows, w_o).astype(jnp.bfloat16)
    d_query, d_keys, d_values = lax.map(lambda block_in: attend_back(block_in[0], block_in[1], block_in[2], block_in[3], block_in[4], block_in[5]), (query_seq, key_seq, value_seq, attended, d_attended.reshape(seq_count, L, head_count * HD), log_total))
    dq_raw = rotate(d_query.reshape(row_count, head_count, HD), cos_table, sin_table, -1.0).astype(jnp.bfloat16).reshape(row_count, head_count * HD)
    dk_raw = rotate(d_keys.reshape(row_count, kv_count, HD), cos_table, sin_table, -1.0).astype(jnp.bfloat16).reshape(row_count, kv_count * HD)
    dv_rows = d_values.astype(jnp.bfloat16).reshape(row_count, kv_count * HD)
    grad_query = matmul_tn(normed_one, dq_raw)
    grad_key = matmul_tn(normed_one, dk_raw)
    grad_value = matmul_tn(normed_one, dv_rows)
    d_norm_one = matmul_nt(dq_raw, w_q) + matmul_nt(dk_raw, w_k) + matmul_nt(dv_rows, w_v)
    grad_gain_one = lax.optimization_barrier(jnp.sum(d_norm_one * norm_one, axis=0))
    e_one = d_norm_one * gain_one
    x_grad = d_hidden + inv_one * (e_one - norm_one * lax.optimization_barrier(jnp.mean(e_one * norm_one, axis=-1, keepdims=True)))
    grad_list = (grad_gain_one, grad_query, grad_key, grad_value, grad_out, grad_gain_two, grad_gate, grad_up, grad_down)
    return (out_rows, x_grad, grad_list)

def reference(layer_input, positions, norm1_gain, w_q, w_k, w_v, w_o, norm2_gain, w_gate, w_up, w_down, out_grad):
    seq_count = TOKENS // L
    per_block = math.gcd(8, seq_count)
    block_count = seq_count // per_block
    row_count = per_block * L
    weights = (norm1_gain, w_q, w_k, w_v, w_o, norm2_gain, w_gate, w_up, w_down)
    initial = tuple((jnp.zeros(item.shape, jnp.float32) for item in weights))

    def one_block(carried, block_in):
        out_rows, x_grad, grad_list = layer_pass(block_in[0], block_in[1], block_in[2], *weights)
        return (tuple((running + grad_piece for running, grad_piece in zip(carried, grad_list))), (out_rows, x_grad))
    totals, stacked = lax.scan(one_block, initial, (layer_input.reshape(block_count, row_count, D), positions.reshape(block_count, row_count), out_grad.reshape(block_count, row_count, D)))
    layer_output = stacked[0].reshape(TOKENS, D)
    x_grad = stacked[1].reshape(TOKENS, D)
    return (layer_output, x_grad, totals[0], totals[1], totals[2], totals[3], totals[4], totals[5], totals[6], totals[7], totals[8])
```

```python
import functools
import math

import jax
import jax.numpy as jnp
from jax import lax
from jax.experimental import pallas as pl
from jax.experimental.pallas import tpu as pltpu
from jax.sharding import PartitionSpec as P

HD = 64
L = 256
TILE = 256
VMEM_BYTES = 67043328

epsilon = 1e-05

MESH_IDS = pl.DeviceIdType.MESH
VMEM_SPEC = pl.BlockSpec(memory_space=pltpu.VMEM)
ANY_SPEC = pl.BlockSpec(memory_space=pl.ANY)


def matmul(left_side, right_side):
    return jnp.dot(left_side, right_side, preferred_element_type=jnp.float32)


def matmul_nt(left_side, right_side):
    return lax.dot_general(
        left_side, right_side, (((1,), (1,)), ((), ())), preferred_element_type=jnp.float32
    )


def rms_parts(row_values):
    inv_rms = lax.rsqrt(jnp.mean(row_values * row_values, axis=-1, keepdims=True) + epsilon)
    return (inv_rms, row_values * inv_rms)


def rope_tables(pos_rows, head_dim):
    half_dim = head_dim // 2
    frequency = jnp.exp(
        jnp.arange(half_dim, dtype=jnp.float32) * (-2.0 * math.log(10000.0) / head_dim)
    )
    angles = pos_rows.astype(jnp.float32)[:, None] * frequency[None, :]
    return (jnp.cos(angles), jnp.sin(angles))


def rotate(row_values, cos_table, sin_table, direction_sign):
    half_dim = row_values.shape[-1] // 2
    first_half = row_values[..., :half_dim]
    second = row_values[..., half_dim:]
    cos_part = cos_table[:, None, :]
    sin_part = sin_table[:, None, :] * direction_sign
    return jnp.concatenate(
        [first_half * cos_part - second * sin_part, second * cos_part + first_half * sin_part],
        axis=-1,
    )


def causal_scores(queries, key_rows):
    length, head_count, head_dim = queries.shape
    kv_count = key_rows.shape[1]
    grouped = queries.reshape(length, kv_count, head_count // kv_count, head_dim)
    scores = jnp.einsum(
        "qkgd,pkd->kgqp", grouped, key_rows, preferred_element_type=jnp.float32
    ) * head_dim ** (-0.5)
    future_mask = jnp.arange(length)[None, :] > jnp.arange(length)[:, None]
    return (grouped, jnp.where(future_mask, -jnp.inf, scores))


def attend(queries, key_rows, value_rows):
    grouped, scores = causal_scores(queries, key_rows)
    row_top = jnp.max(scores, axis=-1, keepdims=True)
    log_total = row_top + jnp.log(jnp.sum(jnp.exp(scores - row_top), axis=-1, keepdims=True))
    weights = jnp.exp(scores - log_total).astype(jnp.bfloat16)
    attended = jnp.einsum("kgqp,pkd->qkgd", weights, value_rows, preferred_element_type=jnp.float32)
    return (attended.reshape(queries.shape[0], -1).astype(jnp.bfloat16), log_total)


def attend_back(queries, key_rows, value_rows, attended, d_attended, log_total):
    length, head_count, head_dim = queries.shape
    kv_count = key_rows.shape[1]
    grouped, scores = causal_scores(queries, key_rows)
    prob_rows = jnp.exp(scores - log_total)
    d_grouped = d_attended.reshape(length, kv_count, head_count // kv_count, head_dim)
    out_grouped = attended.reshape(length, kv_count, head_count // kv_count, head_dim)
    row_delta = jnp.sum(out_grouped.astype(jnp.float32) * d_grouped.astype(jnp.float32), axis=-1)
    row_delta = jnp.transpose(row_delta, (1, 2, 0))[..., None]
    d_probs = jnp.einsum(
        "qkgd,pkd->kgqp", d_grouped, value_rows, preferred_element_type=jnp.float32
    )
    d_scores = (prob_rows * (d_probs - row_delta) * head_dim ** (-0.5)).astype(jnp.bfloat16)
    d_query = jnp.einsum("kgqp,pkd->qkgd", d_scores, key_rows, preferred_element_type=jnp.float32)
    d_keys = jnp.einsum("kgqp,qkgd->pkd", d_scores, grouped, preferred_element_type=jnp.float32)
    d_values = jnp.einsum(
        "kgqp,qkgd->pkd",
        prob_rows.astype(jnp.bfloat16),
        d_grouped,
        preferred_element_type=jnp.float32,
    )
    return (d_query.reshape(length, head_count, head_dim), d_keys, d_values)


class Ring:
    def __init__(self, shards):
        self.count = shards // 2
        me = lax.axis_index("dp")
        self.me = me
        self.core = me % 2
        chip = me // 2
        side = chip % 2
        row = chip // 2
        self.place = row + side * (self.count - 1 - 2 * row)
        self.sign = 1 - 2 * self.core
        self.following = self.device(1, self.core)
        self.previous = self.device(-1, self.core)
        self.sibling = self.device(0, 1 - self.core)

    def chip(self, steps):
        place = (self.place + self.sign * steps + 2 * self.count) % self.count
        side = place // (self.count // 2)
        row = place + side * (self.count - 1 - 2 * place)
        return 2 * row + side

    def device(self, steps, core):
        return self.chip(steps) * 2 + core

    def behind(self, steps):
        return self.device(-steps, self.core)

    def greet(self, partner):
        barrier = pltpu.get_barrier_semaphore()
        for other in (self.following, self.previous, self.sibling):
            pl.semaphore_signal(barrier, inc=1, device_id={"dp": other}, device_id_type=MESH_IDS)
        if partner:
            pl.semaphore_signal(
                barrier,
                inc=1,
                device_id={"tensor": 1 - lax.axis_index("tensor")},
                device_id_type=MESH_IDS,
            )
        pl.semaphore_wait(barrier, 4 if partner else 3)


def send_to(device, source, target, send_sem, recv_sem):
    return pltpu.make_async_remote_copy(
        src_ref=source,
        dst_ref=target,
        send_sem=send_sem,
        recv_sem=recv_sem,
        device_id=device,
        device_id_type=MESH_IDS,
    )


def partner_id():
    return {"tensor": 1 - lax.axis_index("tensor")}


def gather_kernel(shards, *refs):
    kinds = (len(refs) - 5) // 2
    locals_ = refs[:kinds]
    fulls = refs[kinds : 2 * kinds]
    ring_send, ring_recv, side_send, side_recv, own_sem = refs[2 * kinds :]
    ring = Ring(shards)
    ring.greet(False)

    def ring_copy(step, kind, shard, source):
        return send_to(
            {"dp": ring.following},
            source,
            fulls[kind].at[shard],
            ring_send.at[step, kind],
            ring_recv.at[step, kind],
        )

    def side_copy(step, kind, shard, source):
        return send_to(
            {"dp": ring.sibling},
            source,
            fulls[kind].at[shard],
            side_send.at[step, kind],
            side_recv.at[step, kind],
        )

    for kind in range(kinds):
        ring_copy(0, kind, ring.me, locals_[kind]).start()
        side_copy(0, kind, ring.me, locals_[kind]).start()
        pltpu.make_async_copy(locals_[kind], fulls[kind].at[ring.me], own_sem.at[kind]).start()

    def forward(step, carry):
        shard = ring.behind(step)
        for kind in range(kinds):
            here = fulls[kind].at[shard]
            ring_copy(step - 1, kind, shard, here).wait_recv()

            @pl.when(step < ring.count - 1)
            def _():
                ring_copy(step, kind, shard, here).start()

            side_copy(step, kind, shard, here).start()
        return carry

    lax.fori_loop(1, ring.count, forward, 0)

    def drain(step, carry):
        shard = ring.behind(step)
        for kind in range(kinds):
            here = fulls[kind].at[shard]

            @pl.when(step < ring.count - 1)
            def _():
                ring_copy(step, kind, shard, here).wait_send()

            side_copy(step, kind, shard, here).wait_send()
            side_copy(step, kind, shard, here).wait_recv()
        return carry

    lax.fori_loop(0, ring.count, drain, 0)
    for kind in range(kinds):
        pltpu.make_async_copy(locals_[kind], fulls[kind].at[ring.me], own_sem.at[kind]).wait()


def gather_shards(shards, pieces):
    steps = shards // 2
    return pl.pallas_call(
        functools.partial(gather_kernel, shards),
        out_shape=tuple(
            jax.ShapeDtypeStruct((shards,) + piece.shape, piece.dtype) for piece in pieces
        ),
        in_specs=[VMEM_SPEC] * len(pieces),
        out_specs=(ANY_SPEC,) * len(pieces),
        scratch_shapes=[
            pltpu.SemaphoreType.DMA((steps, len(pieces))),
            pltpu.SemaphoreType.DMA((steps, len(pieces))),
            pltpu.SemaphoreType.DMA((steps, len(pieces))),
            pltpu.SemaphoreType.DMA((steps, len(pieces))),
            pltpu.SemaphoreType.DMA((len(pieces),)),
        ],
        compiler_params=pltpu.CompilerParams(
            collective_id=0, has_side_effects=True, vmem_limit_bytes=VMEM_BYTES
        ),
        name="gather_attention",
    )(*pieces)


def ffn_kernel(shards, groups, *refs):
    (
        x_ref,
        part_ref,
        gain_ref,
        grad_ref,
        gate_ref,
        up_ref,
        down_ref,
        hidden_ref,
        normed_ref,
        act_ref,
        d_gate_ref,
        d_up_ref,
        out_part_ref,
        norm_part_ref,
        norm_other_ref,
    ) = refs[:15]
    count = len(groups)
    full = [refs[15 + 3 * group : 18 + 3 * group] for group in range(count)]
    (
        part_other,
        out_total,
        norm_total,
        ring_send,
        ring_recv,
        side_send,
        side_recv,
        own_sem,
        part_sem,
        norm_send,
        norm_recv,
    ) = refs[15 + 3 * count :]
    shard_refs = (gate_ref, up_ref, down_ref)
    rows = gate_ref.shape[0]
    depth = normed_ref.shape[1]
    blocks = depth // TILE
    ring = Ring(shards)
    ring.greet(True)

    def place(group, kind, shard):
        return full[group][kind].at[pl.ds(pl.multiple_of(shard * rows, rows), rows)]

    def own_part(group, kind):
        low, size = groups[group]
        return shard_refs[kind].at[:, pl.ds(low, size)]

    def ring_copy(group, step, kind, shard, source):
        return send_to(
            {"dp": ring.following},
            source,
            place(group, kind, shard),
            ring_send.at[group, step, kind],
            ring_recv.at[group, step, kind],
        )

    def side_copy(group, step, kind, shard, source):
        return send_to(
            {"dp": ring.sibling},
            source,
            place(group, kind, shard),
            side_send.at[group, step, kind],
            side_recv.at[group, step, kind],
        )

    def own_copy(group, kind):
        return pltpu.make_async_copy(
            own_part(group, kind), place(group, kind, ring.me), own_sem.at[group, kind]
        )

    def begin(group):
        for kind in range(3):
            source = own_part(group, kind)
            ring_copy(group, 0, kind, ring.me, source).start()
            side_copy(group, 0, kind, ring.me, source).start()
            own_copy(group, kind).start()

    def forward(group, step):
        shard = ring.behind(step)
        for kind in range(3):
            here = place(group, kind, shard)
            ring_copy(group, step - 1, kind, shard, here).wait_recv()

            @pl.when(step < ring.count - 1)
            def _():
                ring_copy(group, step, kind, shard, here).start()

            side_copy(group, step, kind, shard, here).start()

    def arrived(group):
        for kind in range(3):
            own_copy(group, kind).wait()

        def one(step, carry):
            for kind in range(3):
                here = place(group, kind, ring.me)
                side_copy(group, step, kind, ring.me, here).wait_recv()
            return carry

        lax.fori_loop(0, ring.count, one, 0)

    def hidden_units(group, tile):
        low, _ = groups[group]
        part = pl.ds(pl.multiple_of(tile * TILE, TILE), TILE)
        target = pl.ds(pl.multiple_of(low + tile * TILE, TILE), TILE)
        gate_pre = matmul(normed_ref[...], full[group][0][:, part])
        up_pre = matmul(normed_ref[...], full[group][1][:, part])
        d_act = matmul(grad_ref[...], full[group][2][:, part])
        sigmoid_gate = jax.nn.sigmoid(gate_pre)
        silu_gate = gate_pre * sigmoid_gate
        act_ref[:, target] = (silu_gate * up_pre).astype(jnp.bfloat16)
        d_gate_ref[:, target] = (
            d_act * up_pre * sigmoid_gate * (1.0 + gate_pre * (1.0 - sigmoid_gate))
        ).astype(jnp.bfloat16)
        d_up_ref[:, target] = (d_act * silu_gate).astype(jnp.bfloat16)

    def norm_terms(group, block):
        low, size = groups[group]
        units = pl.ds(low, size)
        features = pl.ds(pl.multiple_of(block * TILE, TILE), TILE)
        return matmul_nt(d_gate_ref[:, units], full[group][0][features, :]) + matmul_nt(
            d_up_ref[:, units], full[group][1][features, :]
        )

    def out_terms(group, block):
        low, size = groups[group]
        features = pl.ds(pl.multiple_of(block * TILE, TILE), TILE)
        return matmul_nt(act_ref[:, pl.ds(low, size)], full[group][2][features, :])

    def accumulate(group, low_block, high_block):
        def one(block, carry):
            features = pl.ds(pl.multiple_of(block * TILE, TILE), TILE)
            norm_new = norm_terms(group, block)
            out_new = out_terms(group, block)
            if group > 0:
                norm_new += norm_total[:, features]
                out_new += out_total[:, features]
            norm_total[:, features] = norm_new
            out_total[:, features] = out_new
            return carry

        lax.fori_loop(low_block, high_block, one, 0)

    part_copy = send_to(partner_id(), part_ref, part_other, part_sem.at[0], part_sem.at[1])
    part_copy.start()
    begin(0)

    def first_steps(step, carry):
        forward(0, step)
        return carry

    lax.fori_loop(1, ring.count, first_steps, 0)
    begin(1)
    part_copy.wait()

    def norm_rows(block, carry):
        here = pl.ds(pl.multiple_of(block * 32, 32), 32)
        hidden = x_ref[here, :] + (
            part_ref[here, :].astype(jnp.float32) + part_other[here, :].astype(jnp.float32)
        )
        hidden_ref[here, :] = hidden
        _, norm_two = rms_parts(hidden)
        normed_ref[here, :] = (norm_two * gain_ref[...]).astype(jnp.bfloat16)
        return carry

    lax.fori_loop(0, normed_ref.shape[0] // 32, norm_rows, 0)

    for group in range(1, count):
        before = group - 1
        tiles = groups[before][1] // TILE
        if group > 1:
            begin(group)
        arrived(before)

        def step_and_work(step, carry):
            forward(group, step)

            @pl.when(step <= tiles)
            def _():
                hidden_units(before, step - 1)

            for half in range(2):

                @pl.when(step == tiles + 1 + half)
                def _():
                    accumulate(before, half * (blocks // 2), (half + 1) * (blocks // 2))

            return carry

        lax.fori_loop(1, ring.count, step_and_work, 0)

    last = count - 1
    arrived(last)

    def last_units(tile, carry):
        hidden_units(last, tile)
        return carry

    lax.fori_loop(0, groups[last][1] // TILE, last_units, 0)

    def norm_copy(block):
        features = pl.ds(pl.multiple_of(block * TILE, TILE), TILE)
        return send_to(
            partner_id(),
            norm_part_ref.at[:, features],
            norm_other_ref.at[:, features],
            norm_send.at[block],
            norm_recv.at[block],
        )

    def last_norm(block, carry):
        features = pl.ds(pl.multiple_of(block * TILE, TILE), TILE)
        norm_part_ref[:, features] = (norm_total[:, features] + norm_terms(last, block)).astype(
            jnp.bfloat16
        )

        @pl.when(block > 0)
        def _():
            norm_copy(block - 1).start()

        return carry

    lax.fori_loop(0, blocks, last_norm, 0)

    def last_out(block, carry):
        features = pl.ds(pl.multiple_of(block * TILE, TILE), TILE)
        out_part_ref[:, features] = (out_total[:, features] + out_terms(last, block)).astype(
            jnp.bfloat16
        )

        @pl.when(block == 0)
        def _():
            norm_copy(blocks - 1).start()

        return carry

    lax.fori_loop(0, blocks, last_out, 0)

    for group in range(count):

        def drain(step, carry):
            for kind in range(3):
                here = place(group, kind, ring.me)

                @pl.when(step < ring.count - 1)
                def _():
                    ring_copy(group, step, kind, ring.me, here).wait_send()

                side_copy(group, step, kind, ring.me, here).wait_send()
            return carry

        lax.fori_loop(0, ring.count, drain, 0)

    def drain_norm(block, carry):
        norm_copy(block).wait()
        return carry

    lax.fori_loop(0, blocks, drain_norm, 0)


def ffn_groups(units, steps):
    tiles = units // TILE
    last = max(1, min(2, tiles - 2))
    first = min(steps - 3, (tiles - last) // 2)
    sizes = [first, tiles - last - first, last]
    groups = []
    low = 0
    for size in sizes:
        groups.append((low * TILE, size * TILE))
        low += size
    return tuple(groups)


def ffn_pass(shards, x_rows, part, gain, grad_rows, gate_shard, up_shard, down_shard):
    tokens, depth = x_rows.shape
    units = gate_shard.shape[1]
    steps = shards // 2
    groups = ffn_groups(units, steps)
    wide = jax.ShapeDtypeStruct((tokens, depth), jnp.bfloat16)
    inner = jax.ShapeDtypeStruct((tokens, units), jnp.bfloat16)
    full = []
    for _, size in groups:
        full += [pltpu.VMEM((depth, size), jnp.bfloat16)] * 3
    sems = pltpu.SemaphoreType.DMA((len(groups), steps, 3))
    return pl.pallas_call(
        functools.partial(ffn_kernel, shards, groups),
        out_shape=(
            jax.ShapeDtypeStruct((tokens, depth), jnp.float32),
            wide,
            inner,
            inner,
            inner,
            wide,
            wide,
            wide,
        ),
        in_specs=[VMEM_SPEC] * 7,
        out_specs=(VMEM_SPEC,) * 8,
        scratch_shapes=full
        + [
            pltpu.VMEM((tokens, depth), jnp.bfloat16),
            pltpu.VMEM((tokens, depth), jnp.float32),
            pltpu.VMEM((tokens, depth), jnp.float32),
            sems,
            sems,
            sems,
            sems,
            pltpu.SemaphoreType.DMA((len(groups), 3)),
            pltpu.SemaphoreType.DMA((2,)),
            pltpu.SemaphoreType.DMA((depth // TILE,)),
            pltpu.SemaphoreType.DMA((depth // TILE,)),
        ],
        compiler_params=pltpu.CompilerParams(
            collective_id=1, has_side_effects=True, vmem_limit_bytes=VMEM_BYTES
        ),
        name="ffn_ring",
    )(x_rows, part, gain, grad_rows, gate_shard, up_shard, down_shard)


def reduce_kernel(shards, chunks, lefts, rights, *refs):
    left_refs = refs[:lefts]
    right_refs = refs[lefts : lefts + rights]
    at = lefts + rights
    out_part_ref, norm_part_ref, scaled_ref, sums_ref = refs[at : at + 4]
    result_ref, sums_out_ref, out_other_ref, norm_other_ref = refs[at + 4 : at + 8]
    at += 8
    left_all = refs[at : at + lefts]
    right_all = refs[at + lefts : at + lefts + rights]
    (
        turned,
        slots,
        norm_here,
        norm_there,
        sums_own,
        sums_side,
        sums_slots,
        ring_send,
        ring_recv,
        sums_send,
        sums_recv,
        own_sem,
        side_send,
        side_recv,
        part_sem,
        sums_sem,
    ) = refs[at + lefts + rights :]
    ring = Ring(shards)
    ring.greet(True)
    tokens = out_part_ref.shape[0]
    rows = slots.shape[1]
    mine = pl.ds(pl.multiple_of(ring.core * tokens, tokens), tokens)

    out_copy = send_to(partner_id(), out_part_ref, out_other_ref, part_sem.at[0], part_sem.at[1])
    norm_copy = send_to(partner_id(), norm_part_ref, norm_there, part_sem.at[2], part_sem.at[3])
    norm_load = pltpu.make_async_copy(norm_part_ref, norm_here, part_sem.at[4])
    sums_load = pltpu.make_async_copy(sums_ref, sums_own, sums_sem.at[0])

    def left_copies(index):
        source = left_refs[index]
        target = left_all[index].at[:, mine]
        return (
            send_to(
                {"dp": ring.sibling},
                source.at[:, 1 - ring.core],
                target,
                side_send.at[index],
                side_recv.at[index],
            ),
            pltpu.make_async_copy(source.at[:, ring.core], target, own_sem.at[index]),
        )

    def right_copies(index):
        source = right_refs[index]
        target = right_all[index].at[mine]
        return (
            send_to(
                {"dp": ring.sibling},
                source,
                target,
                side_send.at[lefts + index],
                side_recv.at[lefts + index],
            ),
            pltpu.make_async_copy(source, target, own_sem.at[lefts + index]),
        )

    copies = [left_copies(index) for index in range(lefts)] + [
        right_copies(index) for index in range(rights)
    ]
    norm_copy.start()
    norm_load.start()
    sums_load.start()
    for side, own in copies:
        side.start()
        own.start()
    out_copy.start()

    def turn(chip):
        for index in range(lefts):
            block = left_all[index][chip].astype(jnp.float32)
            turned[index] = jnp.transpose(block).astype(jnp.bfloat16)

    def terms(chunk):
        left, right, low, size, _ = chunks[chunk]
        return matmul(turned[left], right_all[right][:, low : low + size])

    def ring_copy(step, chunk):
        _, _, _, size, target = chunks[chunk]
        columns = pl.ds(target, size)
        return send_to(
            {"dp": ring.following},
            slots.at[step, :, columns],
            slots.at[step + 1, :, columns],
            ring_send.at[step, chunk],
            ring_recv.at[step, chunk],
        )

    def sums_copy(step):
        return send_to(
            {"dp": ring.following},
            sums_slots.at[step],
            sums_slots.at[step + 1],
            sums_send.at[step],
            sums_recv.at[step],
        )

    seen = set()
    for index in range(lefts):
        copies[index][0].wait_recv()
        copies[index][1].wait()
    turn(ring.chip(-1))
    for chunk in range(len(chunks)):
        _, right, _, size, target = chunks[chunk]
        if right not in seen:
            seen.add(right)
            copies[lefts + right][0].wait_recv()
            copies[lefts + right][1].wait()
        slots[0, :, target : target + size] = terms(chunk).astype(jnp.bfloat16)
        if chunk > 0:
            ring_copy(0, chunk - 1).start()

    norm_load.wait()
    norm_copy.wait_recv()
    sums_load.wait()
    pieces = sums_own.shape[0]
    width = norm_here.shape[1] // pieces

    def column_sums(low, size):
        columns = slice(low, low + size)
        total = norm_here[:, columns].astype(jnp.float32) + norm_there[:, columns].astype(
            jnp.float32
        )
        return jnp.sum(total * scaled_ref[:, columns], axis=0, keepdims=True)

    band = max(width, 128)
    for low in range(0, pieces * width, band):
        sums = column_sums(low, band)
        for inner in range(0, band, width):
            sums_own[(low + inner) // width, 1:2, 0:width] = sums[:, inner : inner + width]
    ring_copy(0, len(chunks) - 1).start()
    store = pltpu.make_async_copy(norm_there, norm_other_ref, sums_sem.at[1])
    store.start()
    sums_side_copy = send_to(
        {"dp": ring.sibling}, sums_own, sums_side, sums_sem.at[2], sums_sem.at[3]
    )
    sums_side_copy.start()
    sums_side_copy.wait_recv()

    def own_sums(steps):
        shard = ring.device(steps, ring.core)
        return sums_own[shard] + sums_side[shard]

    sums_slots[0] = own_sums(-1)

    def one_step(step, carry):
        turn(ring.chip(-1 - step))
        for chunk in range(len(chunks)):
            _, _, _, size, target = chunks[chunk]
            total = terms(chunk)
            ring_copy(step - 1, chunk).wait_recv()
            total += slots[step, :, target : target + size].astype(jnp.float32)
            slots[step, :, target : target + size] = total.astype(jnp.bfloat16)
            if chunk > 0:
                ring_copy(step, chunk - 1).start()
            else:
                sums_copy(step - 1).start()
        sums_copy(step - 1).wait_recv()
        ring_copy(step, len(chunks) - 1).start()
        sums_slots[step] = sums_slots[step] + own_sums(-1 - step)
        return carry

    lax.fori_loop(1, ring.count - 1, one_step, 0)
    final = ring.count - 1
    turn(ring.chip(0))
    for chunk in range(len(chunks)):
        _, _, _, size, target = chunks[chunk]
        total = terms(chunk)
        if chunk == 0:
            sums_copy(final - 1).start()
        ring_copy(final - 1, chunk).wait_recv()
        result_ref[:, target : target + size] = total + slots[
            final, :, target : target + size
        ].astype(jnp.float32)
    sums_copy(final - 1).wait_recv()
    sums_out_ref[...] = sums_slots[final] + own_sums(0)

    def drain(step, carry):
        for chunk in range(len(chunks)):
            ring_copy(step, chunk).wait_send()
        sums_copy(step).wait_send()
        return carry

    lax.fori_loop(0, final, drain, 0)
    for side, _ in copies:
        side.wait_send()
    sums_side_copy.wait_send()
    store.wait()
    norm_copy.wait_send()
    out_copy.wait()


def reduce_chunks(pairs, right_widths):
    chunks = []
    target = 0
    for left, right in pairs:
        width = right_widths[right]
        low = 0
        while low < width:
            size = min(1024, width - low)
            if width - low - size < 512:
                size = width - low
            chunks.append((left, right, low, size, target))
            low += size
            target += size
    return tuple(chunks), target


def reduce_pass(shards, pairs, lefts, rights, out_part, norm_part, scaled, sums):
    tokens, depth = out_part.shape
    steps = shards // 2
    rows = lefts[0].shape[3]
    chunks, total = reduce_chunks(pairs, [right.shape[1] for right in rights])
    operands = len(lefts) + len(rights)
    sums_shape = sums.shape[1:]
    return pl.pallas_call(
        functools.partial(reduce_kernel, shards, chunks, len(lefts), len(rights)),
        out_shape=(
            jax.ShapeDtypeStruct((rows, total), jnp.float32),
            jax.ShapeDtypeStruct(sums_shape, jnp.float32),
            jax.ShapeDtypeStruct((tokens, depth), jnp.bfloat16),
            jax.ShapeDtypeStruct((tokens, depth), jnp.bfloat16),
        ),
        in_specs=[ANY_SPEC] * operands + [ANY_SPEC, ANY_SPEC, VMEM_SPEC, ANY_SPEC],
        out_specs=(VMEM_SPEC, VMEM_SPEC, ANY_SPEC, ANY_SPEC),
        scratch_shapes=[
            pltpu.VMEM((steps, 2 * tokens, rows), jnp.bfloat16) for _ in lefts
        ]
        + [pltpu.VMEM((2 * tokens, right.shape[1]), jnp.bfloat16) for right in rights]
        + [
            pltpu.VMEM((len(lefts), rows, 2 * tokens), jnp.bfloat16),
            pltpu.VMEM((steps, rows, total), jnp.bfloat16),
            pltpu.VMEM((tokens, depth), jnp.bfloat16),
            pltpu.VMEM((tokens, depth), jnp.bfloat16),
            pltpu.VMEM(sums.shape, jnp.float32),
            pltpu.VMEM(sums.shape, jnp.float32),
            pltpu.VMEM((steps,) + sums_shape, jnp.float32),
            pltpu.SemaphoreType.DMA((steps, len(chunks))),
            pltpu.SemaphoreType.DMA((steps, len(chunks))),
            pltpu.SemaphoreType.DMA((steps,)),
            pltpu.SemaphoreType.DMA((steps,)),
            pltpu.SemaphoreType.DMA((operands,)),
            pltpu.SemaphoreType.DMA((operands,)),
            pltpu.SemaphoreType.DMA((operands,)),
            pltpu.SemaphoreType.DMA((5,)),
            pltpu.SemaphoreType.DMA((4,)),
        ],
        compiler_params=pltpu.CompilerParams(
            collective_id=2, has_side_effects=True, vmem_limit_bytes=VMEM_BYTES
        ),
        name="reduce_ring",
    )(*lefts, *rights, out_part, norm_part, scaled, sums)


def body(
    shards,
    layer_input,
    positions,
    norm1_gain,
    w_q,
    w_k,
    w_v,
    w_o,
    norm2_gain,
    w_gate,
    w_up,
    w_down,
    out_grad,
):
    tokens, depth = layer_input.shape
    rows = w_q.shape[0]
    head_count = w_q.shape[1] // HD
    kv_count = w_k.shape[1] // HD
    query_cols = head_count * HD
    kv_cols = kv_count * HD
    units = w_gate.shape[1]

    qkv_shard = jnp.concatenate([w_q, w_k, w_v], axis=1)
    out_shard = w_o.T
    gains = jnp.stack([norm1_gain, norm2_gain]).astype(jnp.float32)
    gains = jnp.pad(gains, ((0, 6), (0, max(128 - rows, 0))))
    gains_all, qkv_all, out_all = gather_shards(shards, (gains, qkv_shard, out_shard))
    gain_one = gains_all[:, 0, :rows].reshape(1, depth)
    gain_two = gains_all[:, 1, :rows].reshape(1, depth)
    qkv_w = qkv_all.reshape(depth, query_cols + 2 * kv_cols)
    out_w = out_all.reshape(depth, query_cols)

    inv_one, norm_one = rms_parts(layer_input)
    normed_one = (norm_one * gain_one).astype(jnp.bfloat16)
    cos_table, sin_table = rope_tables(positions, HD)
    qkv = matmul(normed_one, qkv_w)
    queries = rotate(
        qkv[:, :query_cols].reshape(tokens, head_count, HD), cos_table, sin_table, 1.0
    ).astype(jnp.bfloat16)
    key_rows = rotate(
        qkv[:, query_cols : query_cols + kv_cols].reshape(tokens, kv_count, HD),
        cos_table,
        sin_table,
        1.0,
    ).astype(jnp.bfloat16)
    value_rows = qkv[:, query_cols + kv_cols :].astype(jnp.bfloat16).reshape(tokens, kv_count, HD)
    seq_count = tokens // L
    query_seq = queries.reshape(seq_count, L, head_count, HD)
    key_seq = key_rows.reshape(seq_count, L, kv_count, HD)
    value_seq = value_rows.reshape(seq_count, L, kv_count, HD)
    attended, log_total = lax.map(
        lambda block_in: attend(block_in[0], block_in[1], block_in[2]),
        (query_seq, key_seq, value_seq),
    )
    attended_rows = attended.reshape(tokens, query_cols)
    part = matmul_nt(attended_rows, out_w).astype(jnp.bfloat16)
    grad_rows = out_grad.astype(jnp.bfloat16)

    (
        hidden,
        normed_two,
        activated,
        d_gate,
        d_up,
        out_part,
        norm_part,
        norm_other,
    ) = ffn_pass(shards, layer_input, part, gain_two, grad_rows, w_gate, w_up, w_down.T)

    inv_two, norm_two = rms_parts(hidden)
    d_norm_two = norm_part.astype(jnp.float32) + norm_other.astype(jnp.float32)
    grad_gain_two = jnp.sum(d_norm_two * norm_two, axis=0)
    e_two = d_norm_two * gain_two
    d_hidden = out_grad + inv_two * (
        e_two - norm_two * jnp.mean(e_two * norm_two, axis=-1, keepdims=True)
    )
    hidden_rows = d_hidden.astype(jnp.bfloat16)
    d_attended = matmul(hidden_rows, out_w).astype(jnp.bfloat16)
    d_query, d_keys, d_values = lax.map(
        lambda block_in: attend_back(
            block_in[0], block_in[1], block_in[2], block_in[3], block_in[4], block_in[5]
        ),
        (
            query_seq,
            key_seq,
            value_seq,
            attended,
            d_attended.reshape(seq_count, L, query_cols),
            log_total,
        ),
    )
    dq_raw = (
        rotate(d_query.reshape(tokens, head_count, HD), cos_table, sin_table, -1.0)
        .astype(jnp.bfloat16)
        .reshape(tokens, query_cols)
    )
    dk_raw = (
        rotate(d_keys.reshape(tokens, kv_count, HD), cos_table, sin_table, -1.0)
        .astype(jnp.bfloat16)
        .reshape(tokens, kv_cols)
    )
    dv_rows = d_values.astype(jnp.bfloat16).reshape(tokens, kv_cols)
    d_qkv = jnp.concatenate([dq_raw, dk_raw, dv_rows], axis=1)
    norm_one_part = matmul_nt(d_qkv, qkv_w).astype(jnp.bfloat16)

    def blocks(row_values):
        return jnp.transpose(
            row_values.reshape(tokens, shards // 2, 2, rows), (1, 2, 0, 3)
        )

    sums = grad_gain_two.reshape(shards, 1, rows)
    sums = jnp.pad(sums, ((0, 0), (0, 7), (0, max(128 - rows, 0))))
    result, sums_out, out_other, norm_one_other = reduce_pass(
        shards,
        ((0, 0), (0, 1), (1, 2), (2, 3), (3, 4)),
        [blocks(normed_two), blocks(grad_rows), blocks(hidden_rows), blocks(normed_one)],
        [d_gate, d_up, activated, attended_rows, d_qkv],
        out_part,
        norm_one_part,
        norm_one,
        sums,
    )

    layer_output = hidden + (out_part.astype(jnp.float32) + out_other.astype(jnp.float32))
    d_norm_one = norm_one_part.astype(jnp.float32) + norm_one_other.astype(jnp.float32)
    e_one = d_norm_one * gain_one
    x_grad = d_hidden + inv_one * (
        e_one - norm_one * jnp.mean(e_one * norm_one, axis=-1, keepdims=True)
    )
    at = 3 * units
    shard_qkv = result[:, at + query_cols :]
    return (
        layer_output,
        x_grad,
        sums_out[1, :rows],
        shard_qkv[:, :query_cols],
        shard_qkv[:, query_cols : query_cols + kv_cols],
        shard_qkv[:, query_cols + kv_cols :],
        result[:, at : at + query_cols].T,
        sums_out[0, :rows],
        result[:, :units],
        result[:, units : 2 * units],
        result[:, 2 * units : 3 * units].T,
    )


def solution(mesh):
    in_specs = (
        P("dp", None),
        P("dp"),
        P("dp"),
        P("dp", "tensor"),
        P("dp", "tensor"),
        P("dp", "tensor"),
        P("tensor", "dp"),
        P("dp"),
        P("dp", "tensor"),
        P("dp", "tensor"),
        P("tensor", "dp"),
        P("dp", None),
    )
    out_specs = (
        P("dp", None),
        P("dp", None),
        P("dp"),
        P("dp", "tensor"),
        P("dp", "tensor"),
        P("dp", "tensor"),
        P("tensor", "dp"),
        P("dp"),
        P("dp", "tensor"),
        P("dp", "tensor"),
        P("tensor", "dp"),
    )
    return jax.shard_map(
        functools.partial(body, mesh.shape["dp"]),
        mesh=mesh,
        in_specs=in_specs,
        out_specs=out_specs,
        check_vma=False,
    )
```

```python
import functools
import math

import jax
import jax.numpy as jnp
from jax import lax
from jax.experimental import pallas as pl
from jax.experimental.pallas import tpu as pltpu
from jax.sharding import PartitionSpec as P

HD = 64
L = 256
TILE = 256
VMEM_BYTES = 67043328

epsilon = 1e-05

MESH_IDS = pl.DeviceIdType.MESH
VMEM_SPEC = pl.BlockSpec(memory_space=pltpu.VMEM)
ANY_SPEC = pl.BlockSpec(memory_space=pl.ANY)


def matmul(left_side, right_side):
    return jnp.dot(left_side, right_side, preferred_element_type=jnp.float32)


def matmul_nt(left_side, right_side):
    return lax.dot_general(
        left_side, right_side, (((1,), (1,)), ((), ())), preferred_element_type=jnp.float32
    )


def rms_parts(row_values):
    inv_rms = lax.rsqrt(jnp.mean(row_values * row_values, axis=-1, keepdims=True) + epsilon)
    return (inv_rms, row_values * inv_rms)


def rope_tables(pos_rows, head_dim):
    half_dim = head_dim // 2
    frequency = jnp.exp(
        jnp.arange(half_dim, dtype=jnp.float32) * (-2.0 * math.log(10000.0) / head_dim)
    )
    angles = pos_rows.astype(jnp.float32)[:, None] * frequency[None, :]
    return (jnp.cos(angles), jnp.sin(angles))


def rotate(row_values, cos_table, sin_table, direction_sign):
    half_dim = row_values.shape[-1] // 2
    first_half = row_values[..., :half_dim]
    second = row_values[..., half_dim:]
    cos_part = cos_table[:, None, :]
    sin_part = sin_table[:, None, :] * direction_sign
    return jnp.concatenate(
        [first_half * cos_part - second * sin_part, second * cos_part + first_half * sin_part],
        axis=-1,
    )


def causal_scores(queries, key_rows):
    length, head_count, head_dim = queries.shape
    kv_count = key_rows.shape[1]
    grouped = queries.reshape(length, kv_count, head_count // kv_count, head_dim)
    scores = jnp.einsum(
        "qkgd,pkd->kgqp", grouped, key_rows, preferred_element_type=jnp.float32
    ) * head_dim ** (-0.5)
    future_mask = jnp.arange(length)[None, :] > jnp.arange(length)[:, None]
    return (grouped, jnp.where(future_mask, -jnp.inf, scores))


def attend(queries, key_rows, value_rows):
    grouped, scores = causal_scores(queries, key_rows)
    row_top = jnp.max(scores, axis=-1, keepdims=True)
    log_total = row_top + jnp.log(jnp.sum(jnp.exp(scores - row_top), axis=-1, keepdims=True))
    weights = jnp.exp(scores - log_total).astype(jnp.bfloat16)
    attended = jnp.einsum("kgqp,pkd->qkgd", weights, value_rows, preferred_element_type=jnp.float32)
    return (attended.reshape(queries.shape[0], -1).astype(jnp.bfloat16), log_total)


def attend_back(queries, key_rows, value_rows, attended, d_attended, log_total):
    length, head_count, head_dim = queries.shape
    kv_count = key_rows.shape[1]
    grouped, scores = causal_scores(queries, key_rows)
    prob_rows = jnp.exp(scores - log_total)
    d_grouped = d_attended.reshape(length, kv_count, head_count // kv_count, head_dim)
    out_grouped = attended.reshape(length, kv_count, head_count // kv_count, head_dim)
    row_delta = jnp.sum(out_grouped.astype(jnp.float32) * d_grouped.astype(jnp.float32), axis=-1)
    row_delta = jnp.transpose(row_delta, (1, 2, 0))[..., None]
    d_probs = jnp.einsum(
        "qkgd,pkd->kgqp", d_grouped, value_rows, preferred_element_type=jnp.float32
    )
    d_scores = (prob_rows * (d_probs - row_delta) * head_dim ** (-0.5)).astype(jnp.bfloat16)
    d_query = jnp.einsum("kgqp,pkd->qkgd", d_scores, key_rows, preferred_element_type=jnp.float32)
    d_keys = jnp.einsum("kgqp,qkgd->pkd", d_scores, grouped, preferred_element_type=jnp.float32)
    d_values = jnp.einsum(
        "kgqp,qkgd->pkd",
        prob_rows.astype(jnp.bfloat16),
        d_grouped,
        preferred_element_type=jnp.float32,
    )
    return (d_query.reshape(length, head_count, head_dim), d_keys, d_values)


def chip_at(place, count):
    side = place // (count // 2)
    row = place + side * (count - 1 - 2 * place)
    return 2 * row + side


def place_of(chip, count):
    side = chip % 2
    row = chip // 2
    return row + side * (count - 1 - 2 * row)


def ring_pairs(shards):
    count = shards // 2
    pairs = []
    for shard in range(shards):
        chip, core = divmod(shard, 2)
        place = (place_of(chip, count) + (1 - 2 * core)) % count
        pairs.append((shard, chip_at(place, count) * 2 + core))
    return pairs


class Ring:
    def __init__(self, shards):
        self.shards = shards
        self.count = shards // 2
        self.me = lax.axis_index("dp")
        self.core = self.me % 2
        self.place = place_of(self.me // 2, self.count)
        self.sign = 1 - 2 * self.core
        self.following = self.device(1, self.core)
        self.previous = self.device(-1, self.core)
        self.sibling = self.device(0, 1 - self.core)

    def chip(self, steps):
        place = (self.place + self.sign * steps + 2 * self.count) % self.count
        return chip_at(place, self.count)

    def device(self, steps, core):
        return self.chip(steps) * 2 + core

    def behind(self, steps):
        return self.device(-steps, self.core)

    def greet(self, partner=False, everyone=False):
        barrier = pltpu.get_barrier_semaphore()

        def signal(device):
            pl.semaphore_signal(barrier, inc=1, device_id=device, device_id_type=MESH_IDS)

        if everyone:

            def one(offset, carry):
                signal({"dp": (self.me + offset) % self.shards})
                return carry

            lax.fori_loop(1, self.shards, one, 0)
            expected = self.shards - 1
        else:
            for other in (self.following, self.previous, self.sibling):
                signal({"dp": other})
            expected = 3
        if partner:
            signal(partner_id())
            expected += 1
        pl.semaphore_wait(barrier, expected)


def send_to(device, source, target, send_sem, recv_sem):
    return pltpu.make_async_remote_copy(
        src_ref=source,
        dst_ref=target,
        send_sem=send_sem,
        recv_sem=recv_sem,
        device_id=device,
        device_id_type=MESH_IDS,
    )


def partner_id():
    return {"tensor": 1 - lax.axis_index("tensor")}


def turn_block(source, target):
    target[...] = jnp.transpose(source[...].astype(jnp.float32)).astype(target.dtype)


def turn_rows(source, target):
    def one(block, carry):
        here = pl.ds(pl.multiple_of(block * TILE, TILE), TILE)
        target[:, here] = jnp.transpose(source[here, :].astype(jnp.float32)).astype(target.dtype)
        return carry

    lax.fori_loop(0, source.shape[0] // TILE, one, 0)


def gather_kernel(shards, *refs):
    (
        gains_ref,
        q_ref,
        k_ref,
        v_ref,
        out_ref,
        down_ref,
        gains_all,
        qkv_all,
        out_all,
        down_turned,
        qkv_own,
        out_load,
        out_own,
        down_load,
        ring_send,
        ring_recv,
        side_send,
        side_recv,
        own_sem,
        load_sem,
    ) = refs
    fulls = (qkv_all, out_all, gains_all)
    locals_ = (qkv_own, out_own, gains_ref)
    kinds = len(fulls)
    ring = Ring(shards)

    loads = []
    low = 0
    for index, ref in enumerate((q_ref, k_ref, v_ref)):
        size = ref.shape[1]
        loads.append(
            pltpu.make_async_copy(ref, qkv_own.at[:, pl.ds(low, size)], load_sem.at[index])
        )
        low += size
    loads.append(pltpu.make_async_copy(out_ref, out_load, load_sem.at[3]))
    loads.append(pltpu.make_async_copy(down_ref, down_load, load_sem.at[4]))
    for load in loads:
        load.start()
    ring.greet()

    def ring_copy(step, kind, shard, source):
        return send_to(
            {"dp": ring.following},
            source,
            fulls[kind].at[shard],
            ring_send.at[step, kind],
            ring_recv.at[step, kind],
        )

    def side_copy(step, kind, shard, source):
        return send_to(
            {"dp": ring.sibling},
            source,
            fulls[kind].at[shard],
            side_send.at[step, kind],
            side_recv.at[step, kind],
        )

    def own_copy(kind):
        return pltpu.make_async_copy(locals_[kind], fulls[kind].at[ring.me], own_sem.at[kind])

    def begin(kind):
        ring_copy(0, kind, ring.me, locals_[kind]).start()
        side_copy(0, kind, ring.me, locals_[kind]).start()
        own_copy(kind).start()

    for load in loads[:3]:
        load.wait()
    begin(0)
    loads[3].wait()
    turn_rows(out_load, out_own)
    begin(2)
    begin(1)
    loads[4].wait()
    turn_rows(down_load, down_turned)

    def forward(step, carry):
        shard = ring.behind(step)
        for kind in (0, 2, 1):
            here = fulls[kind].at[shard]
            ring_copy(step - 1, kind, shard, here).wait_recv()

            @pl.when(step < ring.count - 1)
            def _():
                ring_copy(step, kind, shard, here).start()

            side_copy(step, kind, shard, here).start()
        return carry

    lax.fori_loop(1, ring.count, forward, 0)

    def drain(step, carry):
        shard = ring.behind(step)
        for kind in range(kinds):
            here = fulls[kind].at[shard]

            @pl.when(step < ring.count - 1)
            def _():
                ring_copy(step, kind, shard, here).wait_send()

            side_copy(step, kind, shard, here).wait_send()
            side_copy(step, kind, shard, here).wait_recv()
        return carry

    lax.fori_loop(0, ring.count, drain, 0)
    for kind in range(kinds):
        own_copy(kind).wait()


def gather_shards(shards, gains, w_q, w_k, w_v, w_o, w_down):
    steps = shards // 2
    rows = w_q.shape[0]
    columns = w_q.shape[1] + w_k.shape[1] + w_v.shape[1]
    sems = pltpu.SemaphoreType.DMA((steps, 3))
    half = jnp.bfloat16
    return pl.pallas_call(
        functools.partial(gather_kernel, shards),
        out_shape=(
            jax.ShapeDtypeStruct((shards,) + gains.shape, gains.dtype),
            jax.ShapeDtypeStruct((shards, rows, columns), half),
            jax.ShapeDtypeStruct((shards, rows, w_o.shape[0]), half),
            jax.ShapeDtypeStruct((rows, w_down.shape[0]), half),
        ),
        in_specs=[VMEM_SPEC] + [ANY_SPEC] * 5,
        out_specs=(ANY_SPEC,) * 3 + (VMEM_SPEC,),
        scratch_shapes=[
            pltpu.VMEM((rows, columns), half),
            pltpu.VMEM(w_o.shape, half),
            pltpu.VMEM((rows, w_o.shape[0]), half),
            pltpu.VMEM(w_down.shape, half),
            sems,
            sems,
            sems,
            sems,
            pltpu.SemaphoreType.DMA((3,)),
            pltpu.SemaphoreType.DMA((5,)),
        ],
        compiler_params=pltpu.CompilerParams(
            collective_id=0, has_side_effects=True, vmem_limit_bytes=VMEM_BYTES
        ),
        name="gather_attention",
    )(gains, w_q, w_k, w_v, w_o, w_down)


def turn_left(ring, left_all, turned, index, chip):
    rows = left_all.shape[1] // ring.shards
    first = (2 * chip + ring.core) * rows
    base = pl.multiple_of(first // 128 * 128, 128)
    block = left_all[:, pl.ds(base, 128)].astype(jnp.float32)
    turned[index] = jnp.transpose(block).astype(jnp.bfloat16)


def chunk_terms(ring, turned, index, right_all, low, size, chip, rows):
    if rows % 128 == 0:
        left = turned[index]
    else:
        first = (2 * chip + ring.core) * rows % 128
        left = turned[index, pl.ds(pl.multiple_of(first, rows), rows), :]
    return matmul(left, right_all[:, low : low + size])


def cut_columns(pairs, widths):
    chunks = []
    target = 0
    for left, right in pairs:
        width = widths[right]
        low = 0
        while low < width:
            size = min(1024, width - low)
            if width - low - size < 512:
                size = width - low
            chunks.append((left, right, low, size, target))
            low += size
            target += size
    return tuple(chunks), target


FFN_PAIRS = ((1, 2), (0, 0), (0, 1))
HEAD_PAIRS = ((2, 3), (3, 4))


def ffn_kernel(shards, groups, chunks, *refs):
    (
        x_ref,
        part_ref,
        gain_ref,
        grad_ref,
        gate_ref,
        up_ref,
        down_ref,
        gate_behind,
        up_behind,
        down_behind,
        hidden_ref,
        norm_part_ref,
        norm_other_ref,
        out_part_ref,
        carry_ref,
        normed_out,
        grad_out,
        d_gate_out,
        d_up_out,
        act_out,
    ) = refs[:20]
    count = len(groups)
    full = [refs[20 + 3 * group : 23 + 3 * group] for group in range(count)]
    (
        part_other,
        out_total,
        norm_total,
        normed_all,
        grad_all,
        d_gate_all,
        d_up_all,
        act_all,
        turned,
        ring_send,
        ring_recv,
        side_send,
        side_recv,
        own_sem,
        part_sem,
        norm_send,
        norm_recv,
        left_sem,
        right_send,
        right_recv,
        sum_send,
        sum_recv,
        store_sem,
        free_sem,
    ) = refs[20 + 3 * count :]
    shard_refs = (gate_ref, up_ref, down_ref)
    behind_refs = (gate_behind, up_behind, down_behind)
    tokens = part_ref.shape[0]
    rows = gate_ref.shape[0]
    depth = normed_all.shape[1]
    blocks = depth // TILE
    ring = Ring(shards)
    mine = pl.ds(pl.multiple_of(ring.core * tokens, tokens), tokens)

    x_load = pltpu.make_async_copy(x_ref, hidden_ref, part_sem.at[2])
    grad_load = pltpu.make_async_copy(grad_ref, grad_all.at[mine], part_sem.at[3])
    x_load.start()
    grad_load.start()
    ring.greet(partner=True)

    def place(group, kind, shard):
        return full[group][kind].at[pl.ds(pl.multiple_of(shard * rows, rows), rows)]

    def cut(ref, group):
        low, size = groups[group]
        return ref.at[:, pl.ds(low, size)]

    def ring_copy(group, step, kind, shard, source):
        return send_to(
            {"dp": ring.following},
            source,
            place(group, kind, shard),
            ring_send.at[group, step, kind],
            ring_recv.at[group, step, kind],
        )

    def side_copy(group, step, kind, shard, source):
        return send_to(
            {"dp": ring.sibling},
            source,
            place(group, kind, shard),
            side_send.at[group, step, kind],
            side_recv.at[group, step, kind],
        )

    def own_copies(group, kind):
        return (
            pltpu.make_async_copy(
                cut(shard_refs[kind], group),
                place(group, kind, ring.me),
                own_sem.at[group, kind, 0],
            ),
            pltpu.make_async_copy(
                cut(behind_refs[kind], group),
                place(group, kind, ring.behind(1)),
                own_sem.at[group, kind, 1],
            ),
        )

    def begin(group):
        for kind in range(3):
            source = cut(behind_refs[kind], group)
            ring_copy(group, 1, kind, ring.behind(1), source).start()
            side_copy(group, 1, kind, ring.behind(1), source).start()
            side_copy(group, 0, kind, ring.me, cut(shard_refs[kind], group)).start()
            for copy in own_copies(group, kind):
                copy.start()

    def forward(group, step):
        shard = ring.behind(step)
        for kind in range(3):
            here = place(group, kind, shard)
            ring_copy(group, step - 1, kind, shard, here).wait_recv()

            @pl.when(step < ring.count - 1)
            def _():
                ring_copy(group, step, kind, shard, here).start()

            side_copy(group, step, kind, shard, here).start()

    def arrived(group):
        for kind in range(3):
            for copy in own_copies(group, kind):
                copy.wait()

        def one(step, carry):
            for kind in range(3):
                here = place(group, kind, ring.me)
                side_copy(group, step, kind, ring.me, here).wait_recv()
            return carry

        lax.fori_loop(0, ring.count, one, 0)

    def drain(group):
        def one(step, carry):
            for kind in range(3):
                here = place(group, kind, ring.me)

                @pl.when((step > 0) & (step < ring.count - 1))
                def _():
                    ring_copy(group, step, kind, ring.me, here).wait_send()

                side_copy(group, step, kind, ring.me, here).wait_send()
            return carry

        lax.fori_loop(0, ring.count, one, 0)

    lefts = (normed_all, grad_all)
    rights = (d_gate_all, d_up_all, act_all)

    def left_copy(index):
        here = lefts[index].at[mine]
        return send_to(
            {"dp": ring.sibling}, here, here, left_sem.at[0, index], left_sem.at[1, index]
        )

    def right_copy(group, index):
        low, size = groups[group]
        here = rights[index].at[mine, pl.ds(low, size)]
        return send_to(
            {"dp": ring.sibling},
            here,
            here,
            right_send.at[group, index],
            right_recv.at[group, index],
        )

    def hidden_units(group, tile):
        low, _ = groups[group]
        part = pl.ds(pl.multiple_of(tile * TILE, TILE), TILE)
        target = pl.ds(pl.multiple_of(low + tile * TILE, TILE), TILE)
        gate_pre = matmul(normed_all[mine, :], full[group][0][:, part])
        up_pre = matmul(normed_all[mine, :], full[group][1][:, part])
        d_act = matmul(grad_all[mine, :], full[group][2][:, part])
        sigmoid_gate = jax.nn.sigmoid(gate_pre)
        silu_gate = gate_pre * sigmoid_gate
        act_all[mine, target] = (silu_gate * up_pre).astype(jnp.bfloat16)
        d_gate_all[mine, target] = (
            d_act * up_pre * sigmoid_gate * (1.0 + gate_pre * (1.0 - sigmoid_gate))
        ).astype(jnp.bfloat16)
        d_up_all[mine, target] = (d_act * silu_gate).astype(jnp.bfloat16)

    def norm_terms(group, block):
        low, size = groups[group]
        units = pl.ds(low, size)
        features = pl.ds(pl.multiple_of(block * TILE, TILE), TILE)
        return matmul_nt(d_gate_all[mine, units], full[group][0][features, :]) + matmul_nt(
            d_up_all[mine, units], full[group][1][features, :]
        )

    def out_terms(group, block):
        low, size = groups[group]
        features = pl.ds(pl.multiple_of(block * TILE, TILE), TILE)
        return matmul_nt(act_all[mine, pl.ds(low, size)], full[group][2][features, :])

    def accumulate(group, low_block, high_block):
        def one(block, carry):
            features = pl.ds(pl.multiple_of(block * TILE, TILE), TILE)
            norm_new = norm_terms(group, block)
            out_new = out_terms(group, block)
            if group > 0:
                norm_new += norm_total[:, features]
                out_new += out_total[:, features]
            norm_total[:, features] = norm_new
            out_total[:, features] = out_new
            return carry

        lax.fori_loop(low_block, high_block, one, 0)

    part_copy = send_to(partner_id(), part_ref, part_other, part_sem.at[0], part_sem.at[1])
    part_copy.start()
    begin(0)
    grad_load.wait()
    left_copy(1).start()

    def first_steps(step, carry):
        forward(0, step)
        return carry

    lax.fori_loop(2, ring.count, first_steps, 0)
    begin(1)
    x_load.wait()
    part_copy.wait()

    def norm_rows(block, carry):
        here = pl.ds(pl.multiple_of(block * 32, 32), 32)
        there = pl.ds(pl.multiple_of(ring.core * tokens + block * 32, 32), 32)
        hidden = hidden_ref[here, :] + (
            part_ref[here, :].astype(jnp.float32) + part_other[here, :].astype(jnp.float32)
        )
        hidden_ref[here, :] = hidden
        _, norm_two = rms_parts(hidden)
        normed_all[there, :] = (norm_two * gain_ref[...]).astype(jnp.bfloat16)
        return carry

    lax.fori_loop(0, tokens // 32, norm_rows, 0)

    for group in range(1, count):
        before = group - 1
        tiles = groups[before][1] // TILE
        if group > 1:
            begin(group)
        arrived(before)

        def step_and_work(step, carry):
            forward(group, step)
            work = step - 2

            @pl.when(work < tiles)
            def _():
                hidden_units(before, work)

            if group == 1:

                @pl.when(work == 0)
                def _():
                    left_copy(0).start()

            for half in range(2):

                @pl.when(work == tiles + half)
                def _():
                    if half == 0:
                        for index in range(3):
                            right_copy(before, index).start()
                    accumulate(before, half * (blocks // 2), (half + 1) * (blocks // 2))

            return carry

        lax.fori_loop(2, ring.count, step_and_work, 0)
        if tiles + 1 > ring.count - 3:
            accumulate(before, blocks // 2, blocks)
        if group == 1:
            drain(0)
            pl.semaphore_signal(
                free_sem, inc=1, device_id={"dp": ring.previous}, device_id_type=MESH_IDS
            )

    last = count - 1
    arrived(last)

    def last_units(tile, carry):
        hidden_units(last, tile)
        return carry

    lax.fori_loop(0, groups[last][1] // TILE, last_units, 0)

    def norm_copy(block):
        features = pl.ds(pl.multiple_of(block * TILE, TILE), TILE)
        return send_to(
            partner_id(),
            norm_part_ref.at[:, features],
            norm_other_ref.at[:, features],
            norm_send.at[block],
            norm_recv.at[block],
        )

    def last_norm(block, carry):
        features = pl.ds(pl.multiple_of(block * TILE, TILE), TILE)
        norm_part_ref[:, features] = (norm_total[:, features] + norm_terms(last, block)).astype(
            jnp.bfloat16
        )

        @pl.when(block > 0)
        def _():
            norm_copy(block - 1).start()

        if True:

            @pl.when(block == 0)
            def _():
                for index in range(3):
                    right_copy(last, index).start()

        return carry

    lax.fori_loop(0, blocks, last_norm, 0)

    def last_out(block, carry):
        features = pl.ds(pl.multiple_of(block * TILE, TILE), TILE)
        out_part_ref[:, features] = (out_total[:, features] + out_terms(last, block)).astype(
            jnp.bfloat16
        )

        @pl.when(block == 0)
        def _():
            norm_copy(blocks - 1).start()

        return carry

    lax.fori_loop(0, blocks, last_out, 0)

    for index in range(2):
        left_copy(index).wait_recv()
    for group in range(count):
        for index in range(3):
            right_copy(group, index).wait_recv()
    outs = (normed_out, grad_out, d_gate_out, d_up_out, act_out)
    stores = [
        pltpu.make_async_copy(source, target, store_sem.at[index])
        for index, (source, target) in enumerate(zip(lefts + rights, outs))
    ]
    for store in stores:
        store.start()

    def sum_slot(kind, chunk):
        _, _, _, size, _ = chunks[chunk]
        return full[0][kind].at[pl.ds(chunk * rows, rows), pl.ds(0, size)]

    def sum_copy(chunk):
        return send_to(
            {"dp": ring.following},
            sum_slot(0, chunk),
            sum_slot(1, chunk),
            sum_send.at[chunk],
            sum_recv.at[chunk],
        )

    def terms(chunk, chip):
        left, right, low, size, _ = chunks[chunk]
        return chunk_terms(ring, turned, left, rights[right], low, size, chip, rows)

    chip = ring.chip(-1)
    for index in range(2):
        turn_left(ring, lefts[index], turned, index, chip)
    pl.semaphore_wait(free_sem, 1)
    for chunk in range(len(chunks)):
        size = chunks[chunk][3]
        full[0][0][chunk * rows : (chunk + 1) * rows, 0:size] = terms(chunk, chip).astype(
            jnp.bfloat16
        )
        if chunk > 0:
            sum_copy(chunk - 1).start()
    chip = ring.chip(-2)
    for index in range(2):
        turn_left(ring, lefts[index], turned, index, chip)
    sum_copy(len(chunks) - 1).start()
    for chunk in range(len(chunks)):
        _, _, _, size, target = chunks[chunk]
        total = terms(chunk, chip)
        sum_copy(chunk).wait_recv()
        total += full[0][1][chunk * rows : (chunk + 1) * rows, 0:size].astype(jnp.float32)
        carry_ref[:, target : target + size] = total.astype(jnp.bfloat16)

    for group in range(1, count):
        drain(group)
    for index in range(2):
        left_copy(index).wait_send()
    for group in range(count):
        for index in range(3):
            right_copy(group, index).wait_send()
    for chunk in range(len(chunks)):
        sum_copy(chunk).wait_send()
    for store in stores:
        store.wait()

    def drain_norm(block, carry):
        norm_copy(block).wait()
        return carry

    lax.fori_loop(0, blocks, drain_norm, 0)


def ffn_groups(units, steps):
    tiles = units // TILE
    last = max(1, min(2, tiles - 2))
    first = min(max(1, steps - 4), (tiles - last) // 2)
    sizes = [first, tiles - last - first, last]
    groups = []
    low = 0
    for size in sizes:
        groups.append((low * TILE, size * TILE))
        low += size
    return tuple(groups)


def ffn_pass(shards, x_rows, part, gain, grad_rows, own, behind):
    tokens, depth = x_rows.shape
    rows, units = own[0].shape
    steps = shards // 2
    groups = ffn_groups(units, steps)
    chunks, total = cut_columns(FFN_PAIRS, (units,) * 3)
    half = jnp.bfloat16
    wide = jax.ShapeDtypeStruct((tokens, depth), half)
    both_wide = jax.ShapeDtypeStruct((2 * tokens, depth), half)
    both_inner = jax.ShapeDtypeStruct((2 * tokens, units), half)
    full = []
    for _, size in groups:
        full += [pltpu.VMEM((depth, size), half)] * 3
    sems = pltpu.SemaphoreType.DMA((len(groups), steps, 3))
    block_sems = pltpu.SemaphoreType.DMA((depth // TILE,))
    pair_sems = pltpu.SemaphoreType.DMA((len(groups), 3))
    chunk_sems = pltpu.SemaphoreType.DMA((len(chunks),))
    return pl.pallas_call(
        functools.partial(ffn_kernel, shards, groups, chunks),
        out_shape=(
            jax.ShapeDtypeStruct((tokens, depth), jnp.float32),
            wide,
            wide,
            wide,
            jax.ShapeDtypeStruct((rows, total), half),
            both_wide,
            both_wide,
            both_inner,
            both_inner,
            both_inner,
        ),
        in_specs=[ANY_SPEC, VMEM_SPEC, VMEM_SPEC] + [ANY_SPEC] * 7,
        out_specs=(VMEM_SPEC,) * 5 + (ANY_SPEC,) * 5,
        scratch_shapes=full
        + [
            pltpu.VMEM((tokens, depth), half),
            pltpu.VMEM((tokens, depth), jnp.float32),
            pltpu.VMEM((tokens, depth), jnp.float32),
            pltpu.VMEM((2 * tokens, depth), half),
            pltpu.VMEM((2 * tokens, depth), half),
            pltpu.VMEM((2 * tokens, units), half),
            pltpu.VMEM((2 * tokens, units), half),
            pltpu.VMEM((2 * tokens, units), half),
            pltpu.VMEM((2, 128, 2 * tokens), half),
            sems,
            sems,
            sems,
            sems,
            pltpu.SemaphoreType.DMA((len(groups), 3, 2)),
            pltpu.SemaphoreType.DMA((4,)),
            block_sems,
            block_sems,
            pltpu.SemaphoreType.DMA((2, 2)),
            pair_sems,
            pair_sems,
            chunk_sems,
            chunk_sems,
            pltpu.SemaphoreType.DMA((5,)),
            pltpu.SemaphoreType.REGULAR,
        ],
        compiler_params=pltpu.CompilerParams(
            collective_id=1, has_side_effects=True, vmem_limit_bytes=VMEM_BYTES
        ),
        name="ffn_ring",
    )(x_rows, part, gain, grad_rows, *own, *behind)


def reduce_kernel(shards, ffn_chunks, head_chunks, *refs):
    (
        normed_two_ref,
        grad_ref,
        hidden_rows_ref,
        normed_one_ref,
        d_gate_ref,
        d_up_ref,
        act_ref,
        attended_ref,
        d_qkv_ref,
        carry_ref,
        out_part_ref,
        norm_part_ref,
        hidden_ref,
        d_hidden_ref,
        scaled_ref,
        inv_ref,
        gain_ref,
        sums_ref,
        layer_out,
        x_grad_out,
        gate_grad,
        up_grad,
        down_grad,
        o_grad,
        qkv_grad,
        sums_out,
        normed_two_all,
        grad_all,
        hidden_rows_all,
        normed_one_all,
        d_gate_all,
        d_up_all,
        act_all,
        attended_all,
        d_qkv_all,
        turned,
        ffn_slots,
        head_slots,
        norm_here,
        norm_there,
        out_here,
        out_there,
        hidden_buf,
        d_hidden_buf,
        scaled_buf,
        column_total,
        sums_own,
        sums_in,
        ffn_send,
        ffn_recv,
        head_send,
        head_recv,
        load_sem,
        side_send,
        side_recv,
        part_sem,
        row_sem,
        sums_send,
        sums_recv,
    ) = refs
    ring = Ring(shards)
    tokens, depth = out_part_ref.shape
    rows = head_slots.shape[1]
    mine = pl.ds(pl.multiple_of(ring.core * tokens, tokens), tokens)
    lefts = (normed_two_all, grad_all, hidden_rows_all, normed_one_all)
    rights = (d_gate_all, d_up_all, act_all, attended_all, d_qkv_all)

    head_pairs = (
        (hidden_rows_ref, hidden_rows_all),
        (attended_ref, attended_all),
        (normed_one_ref, normed_one_all),
        (d_qkv_ref, d_qkv_all),
    )
    head_loads = [
        pltpu.make_async_copy(source, target.at[mine], load_sem.at[index])
        for index, (source, target) in enumerate(head_pairs)
    ]
    ffn_loads = [
        pltpu.make_async_copy(source, target, load_sem.at[4 + index])
        for index, (source, target) in enumerate(
            (
                (carry_ref, ffn_slots.at[0]),
                (grad_ref, grad_all),
                (act_ref, act_all),
                (normed_two_ref, normed_two_all),
                (d_gate_ref, d_gate_all),
                (d_up_ref, d_up_all),
            )
        )
    ]
    row_loads = [
        pltpu.make_async_copy(source, target, row_sem.at[index])
        for index, (source, target) in enumerate(
            (
                (norm_part_ref, norm_here),
                (d_hidden_ref, d_hidden_buf),
                (scaled_ref, scaled_buf),
                (out_part_ref, out_here),
                (hidden_ref, hidden_buf),
            )
        )
    ]
    for load in head_loads + ffn_loads + row_loads:
        load.start()
    ring.greet(partner=True, everyone=True)
    sides = [
        send_to(
            {"dp": ring.sibling}, source, target.at[mine], side_send.at[index], side_recv.at[index]
        )
        for index, (source, target) in enumerate(head_pairs)
    ]
    for side in sides:
        side.start()
    norm_copy = send_to(partner_id(), norm_part_ref, norm_there, part_sem.at[0], part_sem.at[1])
    out_copy = send_to(partner_id(), out_part_ref, out_there, part_sem.at[2], part_sem.at[3])
    norm_copy.start()
    out_copy.start()

    def ffn_copy(step, chunk):
        _, _, _, size, target = ffn_chunks[chunk]
        columns = pl.ds(target, size)
        return send_to(
            {"dp": ring.following},
            ffn_slots.at[step - 2, :, columns],
            ffn_slots.at[step - 1, :, columns],
            ffn_send.at[step - 2, chunk],
            ffn_recv.at[step - 2, chunk],
        )

    def head_copy(step, chunk):
        _, _, _, size, target = head_chunks[chunk]
        columns = pl.ds(target, size)
        return send_to(
            {"dp": ring.following},
            head_slots.at[step, :, columns],
            head_slots.at[step + 1, :, columns],
            head_send.at[step, chunk],
            head_recv.at[step, chunk],
        )

    def head_terms(chunk, chip):
        left, right, low, size, _ = head_chunks[chunk]
        return chunk_terms(ring, turned, left, rights[right], low, size, chip, rows)

    def ffn_terms(chunk, chip):
        left, right, low, size, _ = ffn_chunks[chunk]
        return chunk_terms(ring, turned, left, rights[right], low, size, chip, rows)

    def turn(chip, indices):
        for index in indices:
            turn_left(ring, lefts[index], turned, index, chip)

    def sums_copy(offset):
        return send_to(
            {"dp": (ring.me + offset) % shards},
            sums_own.at[(ring.me + offset) % shards],
            sums_in.at[ring.me],
            sums_send.at[offset],
            sums_recv.at[offset],
        )

    def finish_input_grad():
        for load in row_loads[:3]:
            load.wait()
        norm_copy.wait()
        sums_own[...] = sums_ref[...]
        column_total[...] = jnp.zeros_like(column_total)

        def one(block, carry):
            here = pl.ds(pl.multiple_of(block * 16, 16), 16)
            total = norm_here[here, :].astype(jnp.float32) + norm_there[here, :].astype(
                jnp.float32
            )
            scaled = scaled_buf[here, :]
            product = total * scaled
            column_total[...] += product[0:8] + product[8:16]
            scaled_gain = total * gain_ref[...]
            mean = jnp.mean(scaled_gain * scaled, axis=-1, keepdims=True)
            d_hidden_buf[here, :] = d_hidden_buf[here, :] + inv_ref[here, :] * (
                scaled_gain - scaled * mean
            )
            return carry

        lax.fori_loop(0, tokens // 16, one, 0)
        width = depth // shards
        band = max(width, 128)
        for low in range(0, depth, band):
            sums = jnp.sum(column_total[:, low : low + band], axis=0, keepdims=True)
            for inner in range(0, band, width):
                sums_own[(low + inner) // width, 1:2, 0:width] = sums[:, inner : inner + width]

    def send_sums():
        pltpu.make_async_copy(d_hidden_buf, x_grad_out, row_sem.at[5]).start()

        def one(offset, carry):
            sums_copy(offset).start()
            return carry

        lax.fori_loop(1, shards, one, 0)

    def finish_output():
        for load in row_loads[3:]:
            load.wait()
        out_copy.wait()

        def one(block, carry):
            here = pl.ds(pl.multiple_of(block * 16, 16), 16)
            hidden_buf[here, :] = hidden_buf[here, :] + (
                out_here[here, :].astype(jnp.float32) + out_there[here, :].astype(jnp.float32)
            )
            return carry

        lax.fori_loop(0, tokens // 16, one, 0)

    heads = len(head_chunks)
    ffns = len(ffn_chunks)

    def head_step(step, chip, chunk):
        _, _, _, size, target = head_chunks[chunk]
        total = head_terms(chunk, chip)
        head_copy(step - 1, chunk).wait_recv()
        return total + head_slots[step, :, target : target + size].astype(jnp.float32)

    def ffn_step(step, chip, chunk, peeled):
        _, _, _, size, target = ffn_chunks[chunk]
        total = ffn_terms(chunk, chip)
        if peeled:
            ffn_copy(step - 1, chunk).wait_recv()
        else:

            @pl.when(step > 2)
            def _():
                ffn_copy(step - 1, chunk).wait_recv()

        return total + ffn_slots[step - 2, :, target : target + size].astype(jnp.float32)

    def store_head(step, chunk, total):
        _, _, _, size, target = head_chunks[chunk]
        head_slots[step, :, target : target + size] = total.astype(jnp.bfloat16)

    def store_ffn(step, chunk, total):
        _, _, _, size, target = ffn_chunks[chunk]
        ffn_slots[step - 2, :, target : target + size] = total.astype(jnp.bfloat16)

    for load in head_loads:
        load.wait()
    for side in sides:
        side.wait_recv()
    chip = ring.chip(-1)
    turn(chip, (2, 3))
    for chunk in range(heads):
        store_head(0, chunk, head_terms(chunk, chip))
        if chunk > 0:
            head_copy(0, chunk - 1).start()
    for load in ffn_loads:
        load.wait()

    def one_step(index, carry):
        ffn_at = index + 2
        head_at = index + 1
        ffn_chip = ring.chip(-1 - ffn_at)
        head_chip = ring.chip(-1 - head_at)
        turn(ffn_chip, (0, 1))
        head_copy(head_at - 1, heads - 1).start()
        turn(head_chip, (2, 3))
        for chunk in range(ffns):
            store_ffn(ffn_at, chunk, ffn_step(ffn_at, ffn_chip, chunk, False))
            if chunk > 0:
                ffn_copy(ffn_at, chunk - 1).start()
        for chunk in range(heads):
            store_head(head_at, chunk, head_step(head_at, head_chip, chunk))
            if chunk > 0:
                head_copy(head_at, chunk - 1).start()
            else:
                ffn_copy(ffn_at, ffns - 1).start()

        @pl.when(index == 1)
        def _():
            finish_input_grad()

        @pl.when(index == 2)
        def _():
            send_sums()
            finish_output()

        @pl.when(index == 3)
        def _():
            pltpu.make_async_copy(hidden_buf, layer_out, row_sem.at[6]).start()

        return carry

    final = ring.count - 1
    lax.fori_loop(0, ring.count - 3, one_step, 0)
    before = ring.chip(-final)
    turn(before, (2, 3))
    head_copy(final - 2, heads - 1).start()
    for chunk in range(heads):
        store_head(final - 1, chunk, head_step(final - 1, before, chunk))
        if chunk > 0:
            head_copy(final - 1, chunk - 1).start()
    chip = ring.chip(0)
    turn(chip, (0, 1))
    head_copy(final - 1, heads - 1).start()
    turn(chip, (2, 3))
    grads = (gate_grad, up_grad, down_grad, o_grad, qkv_grad)
    for chunk in range(ffns):
        _, right, low, size, _ = ffn_chunks[chunk]
        total = ffn_step(final, chip, chunk, True)
        if right == 2:
            down_grad[low : low + size, :] = jnp.transpose(total)
        else:
            grads[right][:, low : low + size] = total
    for chunk in range(heads):
        _, right, low, size, _ = head_chunks[chunk]
        total = head_step(final, chip, chunk)
        if right == 3:
            o_grad[low : low + size, :] = jnp.transpose(total)
        else:
            qkv_grad[:, low : low + size] = total

    def add_sums(offset, total):
        sums_copy(offset).wait_recv()
        return total + sums_in[(ring.me - offset + shards) % shards]

    sums_out[...] = lax.fori_loop(1, shards, add_sums, sums_own[ring.me])

    def drain_heads(step, carry):
        for chunk in range(heads):
            head_copy(step, chunk).wait_send()
        return carry

    def drain_ffn(step, carry):
        for chunk in range(ffns):
            ffn_copy(step, chunk).wait_send()
        return carry

    def drain_sums(offset, carry):
        sums_copy(offset).wait_send()
        return carry

    lax.fori_loop(0, final, drain_heads, 0)
    lax.fori_loop(2, final, drain_ffn, 0)
    lax.fori_loop(1, shards, drain_sums, 0)
    for side in sides:
        side.wait_send()
    pltpu.make_async_copy(d_hidden_buf, x_grad_out, row_sem.at[5]).wait()
    pltpu.make_async_copy(hidden_buf, layer_out, row_sem.at[6]).wait()


def reduce_pass(shards, both, heads, carry, out_part, norm_part, rows_f32, inv, gain, sums):
    normed_two, grad_rows, d_gate, d_up, activated = both
    hidden_rows, normed_one, attended, d_qkv = heads
    tokens, depth = out_part.shape
    units = d_gate.shape[1]
    steps = shards // 2
    rows = depth // shards
    widths = (units, units, units, attended.shape[1], d_qkv.shape[1])
    ffn_chunks, ffn_total = cut_columns(FFN_PAIRS, widths)
    head_chunks, head_total = cut_columns(HEAD_PAIRS, widths)
    half = jnp.bfloat16
    wide = jax.ShapeDtypeStruct((tokens, depth), jnp.float32)
    both_wide = pltpu.VMEM((2 * tokens, depth), half)
    one_half = pltpu.VMEM((tokens, depth), half)
    one_full = pltpu.VMEM((tokens, depth), jnp.float32)
    dma = pltpu.SemaphoreType.DMA
    return pl.pallas_call(
        functools.partial(reduce_kernel, shards, ffn_chunks, head_chunks),
        out_shape=(
            wide,
            wide,
            jax.ShapeDtypeStruct((rows, units), jnp.float32),
            jax.ShapeDtypeStruct((rows, units), jnp.float32),
            jax.ShapeDtypeStruct((units, rows), jnp.float32),
            jax.ShapeDtypeStruct((attended.shape[1], rows), jnp.float32),
            jax.ShapeDtypeStruct((rows, d_qkv.shape[1]), jnp.float32),
            jax.ShapeDtypeStruct(sums.shape[1:], jnp.float32),
        ),
        in_specs=[ANY_SPEC] * 15 + [VMEM_SPEC] * 3,
        out_specs=(ANY_SPEC, ANY_SPEC) + (VMEM_SPEC,) * 6,
        scratch_shapes=[both_wide] * 4
        + [pltpu.VMEM((2 * tokens, width), half) for width in widths]
        + [
            pltpu.VMEM((4, 128, 2 * tokens), half),
            pltpu.VMEM((steps - 2, rows, ffn_total), half),
            pltpu.VMEM((steps, rows, head_total), half),
            one_half,
            one_half,
            one_half,
            one_half,
            one_full,
            one_full,
            one_full,
            pltpu.VMEM((8, depth), jnp.float32),
            pltpu.VMEM(sums.shape, jnp.float32),
            pltpu.VMEM(sums.shape, jnp.float32),
            dma((steps - 3, len(ffn_chunks))),
            dma((steps - 3, len(ffn_chunks))),
            dma((steps - 1, len(head_chunks))),
            dma((steps - 1, len(head_chunks))),
            dma((10,)),
            dma((4,)),
            dma((4,)),
            dma((4,)),
            dma((7,)),
            dma((shards,)),
            dma((shards,)),
        ],
        compiler_params=pltpu.CompilerParams(
            collective_id=2, has_side_effects=True, vmem_limit_bytes=VMEM_BYTES
        ),
        name="reduce_ring",
    )(
        normed_two,
        grad_rows,
        hidden_rows,
        normed_one,
        d_gate,
        d_up,
        activated,
        attended,
        d_qkv,
        carry,
        out_part,
        norm_part,
        *rows_f32,
        inv,
        gain,
        sums,
    )


def body(
    shards,
    layer_input,
    positions,
    norm1_gain,
    w_q,
    w_k,
    w_v,
    w_o,
    norm2_gain,
    w_gate,
    w_up,
    w_down,
    out_grad,
):
    tokens, depth = layer_input.shape
    rows = w_q.shape[0]
    head_count = w_q.shape[1] // HD
    kv_count = w_k.shape[1] // HD
    query_cols = head_count * HD
    kv_cols = kv_count * HD
    pairs = ring_pairs(shards)

    gains = jnp.stack([norm1_gain, norm2_gain]).astype(jnp.float32)
    gains = jnp.pad(gains, ((0, 6), (0, max(128 - rows, 0))))
    gains_all, qkv_all, out_all, down_turned = gather_shards(
        shards, gains, w_q, w_k, w_v, w_o, w_down
    )
    gain_one = gains_all[:, 0, :rows].reshape(1, depth)
    gain_two = gains_all[:, 1, :rows].reshape(1, depth)
    qkv_w = qkv_all.reshape(depth, query_cols + 2 * kv_cols)
    out_w = out_all.reshape(depth, query_cols)
    gate_tied, up_tied, down_tied, _ = lax.optimization_barrier(
        (w_gate, w_up, down_turned, gains_all)
    )
    own = (gate_tied, up_tied, down_tied)
    behind = tuple(lax.ppermute(shard, "dp", pairs) for shard in own)

    inv_one, norm_one = rms_parts(layer_input)
    normed_one = (norm_one * gain_one).astype(jnp.bfloat16)
    cos_table, sin_table = rope_tables(positions, HD)
    qkv = matmul(normed_one, qkv_w)
    queries = rotate(
        qkv[:, :query_cols].reshape(tokens, head_count, HD), cos_table, sin_table, 1.0
    ).astype(jnp.bfloat16)
    key_rows = rotate(
        qkv[:, query_cols : query_cols + kv_cols].reshape(tokens, kv_count, HD),
        cos_table,
        sin_table,
        1.0,
    ).astype(jnp.bfloat16)
    value_rows = qkv[:, query_cols + kv_cols :].astype(jnp.bfloat16).reshape(tokens, kv_count, HD)
    seq_count = tokens // L
    query_seq = queries.reshape(seq_count, L, head_count, HD)
    key_seq = key_rows.reshape(seq_count, L, kv_count, HD)
    value_seq = value_rows.reshape(seq_count, L, kv_count, HD)
    attended, log_total = lax.map(
        lambda block_in: attend(block_in[0], block_in[1], block_in[2]),
        (query_seq, key_seq, value_seq),
    )
    attended_rows = attended.reshape(tokens, query_cols)
    part = matmul_nt(attended_rows, out_w).astype(jnp.bfloat16)
    grad_rows = out_grad.astype(jnp.bfloat16)

    hidden, norm_part, norm_other, out_part, carry, *both = ffn_pass(
        shards, layer_input, part, gain_two, grad_rows, own, behind
    )
    carry = lax.ppermute(carry, "dp", pairs)

    inv_two, norm_two = rms_parts(hidden)
    d_norm_two = norm_part.astype(jnp.float32) + norm_other.astype(jnp.float32)
    grad_gain_two = jnp.sum(d_norm_two * norm_two, axis=0)
    e_two = d_norm_two * gain_two
    d_hidden = out_grad + inv_two * (
        e_two - norm_two * jnp.mean(e_two * norm_two, axis=-1, keepdims=True)
    )
    hidden_rows = d_hidden.astype(jnp.bfloat16)
    d_attended = matmul(hidden_rows, out_w).astype(jnp.bfloat16)
    d_query, d_keys, d_values = lax.map(
        lambda block_in: attend_back(
            block_in[0], block_in[1], block_in[2], block_in[3], block_in[4], block_in[5]
        ),
        (
            query_seq,
            key_seq,
            value_seq,
            attended,
            d_attended.reshape(seq_count, L, query_cols),
            log_total,
        ),
    )
    dq_raw = (
        rotate(d_query.reshape(tokens, head_count, HD), cos_table, sin_table, -1.0)
        .astype(jnp.bfloat16)
        .reshape(tokens, query_cols)
    )
    dk_raw = (
        rotate(d_keys.reshape(tokens, kv_count, HD), cos_table, sin_table, -1.0)
        .astype(jnp.bfloat16)
        .reshape(tokens, kv_cols)
    )
    dv_rows = d_values.astype(jnp.bfloat16).reshape(tokens, kv_cols)
    d_qkv = jnp.concatenate([dq_raw, dk_raw, dv_rows], axis=1)
    norm_one_part = matmul_nt(d_qkv, qkv_w).astype(jnp.bfloat16)

    sums = grad_gain_two.reshape(shards, 1, rows)
    sums = jnp.pad(sums, ((0, 0), (0, 7), (0, max(128 - rows, 0))))
    (
        layer_output,
        x_grad,
        shard_gate,
        shard_up,
        shard_down,
        shard_out,
        shard_qkv,
        sums_out,
    ) = reduce_pass(
        shards,
        both,
        (hidden_rows, normed_one, attended_rows, d_qkv),
        carry,
        out_part,
        norm_one_part,
        (hidden, d_hidden, norm_one),
        inv_one,
        gain_one,
        sums,
    )
    return (
        layer_output,
        x_grad,
        sums_out[1, :rows],
        shard_qkv[:, :query_cols],
        shard_qkv[:, query_cols : query_cols + kv_cols],
        shard_qkv[:, query_cols + kv_cols :],
        shard_out,
        sums_out[0, :rows],
        shard_gate,
        shard_up,
        shard_down,
    )


def solution(mesh):
    in_specs = (
        P("dp", None),
        P("dp"),
        P("dp"),
        P("dp", "tensor"),
        P("dp", "tensor"),
        P("dp", "tensor"),
        P("tensor", "dp"),
        P("dp"),
        P("dp", "tensor"),
        P("dp", "tensor"),
        P("tensor", "dp"),
        P("dp", None),
    )
    out_specs = (
        P("dp", None),
        P("dp", None),
        P("dp"),
        P("dp", "tensor"),
        P("dp", "tensor"),
        P("dp", "tensor"),
        P("tensor", "dp"),
        P("dp"),
        P("dp", "tensor"),
        P("dp", "tensor"),
        P("tensor", "dp"),
    )
    return jax.shard_map(
        functools.partial(body, mesh.shape["dp"]),
        mesh=mesh,
        in_specs=in_specs,
        out_specs=out_specs,
        check_vma=False,
    )
```

```python
import functools
import math

import jax
import jax.numpy as jnp
from jax import lax
from jax.experimental import pallas as pl
from jax.experimental.pallas import tpu as pltpu
from jax.sharding import PartitionSpec as P


HD = 64
L = 256
TILE = 256
VMEM_BYTES = 67043328

epsilon = 1e-05

MESH_IDS = pl.DeviceIdType.MESH
VMEM_SPEC = pl.BlockSpec(memory_space=pltpu.VMEM)
ANY_SPEC = pl.BlockSpec(memory_space=pl.ANY)


def matmul(left_side, right_side):
    return jnp.dot(left_side, right_side, preferred_element_type=jnp.float32)


def matmul_nt(left_side, right_side):
    return lax.dot_general(
        left_side, right_side, (((1,), (1,)), ((), ())), preferred_element_type=jnp.float32
    )


def rms_parts(row_values):
    inv_rms = lax.rsqrt(jnp.mean(row_values * row_values, axis=-1, keepdims=True) + epsilon)
    return (inv_rms, row_values * inv_rms)


def rope_tables(pos_rows, head_dim):
    half_dim = head_dim // 2
    frequency = jnp.exp(
        jnp.arange(half_dim, dtype=jnp.float32) * (-2.0 * math.log(10000.0) / head_dim)
    )
    angles = pos_rows.astype(jnp.float32)[:, None] * frequency[None, :]
    return (jnp.cos(angles), jnp.sin(angles))


def rotate(row_values, cos_table, sin_table, direction_sign):
    half_dim = row_values.shape[-1] // 2
    first_half = row_values[..., :half_dim]
    second = row_values[..., half_dim:]
    cos_part = cos_table[:, None, :]
    sin_part = sin_table[:, None, :] * direction_sign
    return jnp.concatenate(
        [first_half * cos_part - second * sin_part, second * cos_part + first_half * sin_part],
        axis=-1,
    )


def causal_scores(queries, key_rows):
    length, head_count, head_dim = queries.shape
    kv_count = key_rows.shape[1]
    grouped = queries.reshape(length, kv_count, head_count // kv_count, head_dim)
    scores = jnp.einsum(
        "qkgd,pkd->kgqp", grouped, key_rows, preferred_element_type=jnp.float32
    ) * head_dim ** (-0.5)
    future_mask = jnp.arange(length)[None, :] > jnp.arange(length)[:, None]
    return (grouped, jnp.where(future_mask, -jnp.inf, scores))


def attend(queries, key_rows, value_rows):
    _, scores = causal_scores(queries, key_rows)
    row_top = jnp.max(scores, axis=-1, keepdims=True)
    log_total = row_top + jnp.log(jnp.sum(jnp.exp(scores - row_top), axis=-1, keepdims=True))
    weights = jnp.exp(scores - log_total).astype(jnp.bfloat16)
    attended = jnp.einsum("kgqp,pkd->qkgd", weights, value_rows, preferred_element_type=jnp.float32)
    return (attended.reshape(queries.shape[0], -1).astype(jnp.bfloat16), log_total)


def attend_back(queries, key_rows, value_rows, attended, d_attended, log_total):
    length, head_count, head_dim = queries.shape
    kv_count = key_rows.shape[1]
    grouped, scores = causal_scores(queries, key_rows)
    prob_rows = jnp.exp(scores - log_total)
    d_grouped = d_attended.reshape(length, kv_count, head_count // kv_count, head_dim)
    out_grouped = attended.reshape(length, kv_count, head_count // kv_count, head_dim)
    row_delta = jnp.sum(out_grouped.astype(jnp.float32) * d_grouped.astype(jnp.float32), axis=-1)
    row_delta = jnp.transpose(row_delta, (1, 2, 0))[..., None]
    d_probs = jnp.einsum(
        "qkgd,pkd->kgqp", d_grouped, value_rows, preferred_element_type=jnp.float32
    )
    d_scores = (prob_rows * (d_probs - row_delta) * head_dim ** (-0.5)).astype(jnp.bfloat16)
    d_query = jnp.einsum("kgqp,pkd->qkgd", d_scores, key_rows, preferred_element_type=jnp.float32)
    d_keys = jnp.einsum("kgqp,qkgd->pkd", d_scores, grouped, preferred_element_type=jnp.float32)
    d_values = jnp.einsum(
        "kgqp,qkgd->pkd",
        prob_rows.astype(jnp.bfloat16),
        d_grouped,
        preferred_element_type=jnp.float32,
    )
    return (d_query.reshape(length, head_count, head_dim), d_keys, d_values)


def chip_at(place, count):
    side = place // (count // 2)
    row = place + side * (count - 1 - 2 * place)
    return 2 * row + side


def place_of(chip, count):
    side = chip % 2
    row = chip // 2
    return row + side * (count - 1 - 2 * row)


def ring_pairs(shards):
    count = shards // 2
    pairs = []
    for shard in range(shards):
        chip, core = divmod(shard, 2)
        place = (place_of(chip, count) + (1 - 2 * core)) % count
        pairs.append((shard, chip_at(place, count) * 2 + core))
    return pairs


class Ring:
    def __init__(self, shards):
        self.shards = shards
        self.count = shards // 2
        self.me = lax.axis_index("dp")
        self.core = self.me % 2
        self.place = place_of(self.me // 2, self.count)
        self.sign = 1 - 2 * self.core
        self.following = self.device(1, self.core)
        self.previous = self.device(-1, self.core)
        self.sibling = self.device(0, 1 - self.core)

    def chip(self, steps):
        place = (self.place + self.sign * steps + 2 * self.count) % self.count
        return chip_at(place, self.count)

    def device(self, steps, core):
        return self.chip(steps) * 2 + core

    def behind(self, steps):
        return self.device(-steps, self.core)

    def greet(self, partner=False, everyone=False):
        barrier = pltpu.get_barrier_semaphore()

        def signal(device):
            pl.semaphore_signal(barrier, inc=1, device_id=device, device_id_type=MESH_IDS)

        if everyone:

            def one(offset, carry):
                signal({"dp": (self.me + offset) % self.shards})
                return carry

            lax.fori_loop(1, self.shards, one, 0)
            expected = self.shards - 1
        else:
            for other in (self.following, self.previous, self.sibling):
                signal({"dp": other})
            expected = 3
        if partner:
            signal(partner_id())
            expected += 1
        pl.semaphore_wait(barrier, expected)


def send_to(device, source, target, send_sem, recv_sem):
    return pltpu.make_async_remote_copy(
        src_ref=source,
        dst_ref=target,
        send_sem=send_sem,
        recv_sem=recv_sem,
        device_id=device,
        device_id_type=MESH_IDS,
    )


def partner_id():
    return {"tensor": 1 - lax.axis_index("tensor")}


def turn_rows(source, target, low=0):
    def one(block, carry):
        here = pl.ds(pl.multiple_of(block * TILE, TILE), TILE)
        there = pl.ds(pl.multiple_of(low + block * TILE, TILE), TILE)
        target[:, there] = jnp.transpose(source[here, :].astype(jnp.float32)).astype(target.dtype)
        return carry

    lax.fori_loop(0, source.shape[0] // TILE, one, 0)


def gather_kernel(shards, *refs):
    (
        gains_ref,
        q_ref,
        k_ref,
        v_ref,
        out_ref,
        gate_ref,
        up_ref,
        down_ref,
        gains_all,
        qkv_all,
        out_all,
        ffn_shard,
        qkv_own,
        out_load,
        out_own,
        down_load,
        ffn_own,
        ring_send,
        ring_recv,
        side_send,
        side_recv,
        own_sem,
        load_sem,
    ) = refs
    fulls = (qkv_all, out_all, gains_all)
    locals_ = (qkv_own, out_own, gains_ref)
    kinds = len(fulls)
    ring = Ring(shards)

    loads = []
    low = 0
    for index, ref in enumerate((q_ref, k_ref, v_ref)):
        size = ref.shape[1]
        loads.append(
            pltpu.make_async_copy(ref, qkv_own.at[:, pl.ds(low, size)], load_sem.at[index])
        )
        low += size
    loads.append(pltpu.make_async_copy(out_ref, out_load, load_sem.at[3]))
    loads.append(pltpu.make_async_copy(down_ref, down_load, load_sem.at[4]))
    units = gate_ref.shape[1]
    for index, ref in enumerate((gate_ref, up_ref)):
        part = ffn_own.at[:, pl.ds(index * units, units)]
        loads.append(pltpu.make_async_copy(ref, part, load_sem.at[5 + index]))
    for load in loads:
        load.start()
    ring.greet()

    def ring_copy(step, kind, shard, source):
        return send_to(
            {"dp": ring.following},
            source,
            fulls[kind].at[shard],
            ring_send.at[step, kind],
            ring_recv.at[step, kind],
        )

    def side_copy(step, kind, shard, source):
        return send_to(
            {"dp": ring.sibling},
            source,
            fulls[kind].at[shard],
            side_send.at[step, kind],
            side_recv.at[step, kind],
        )

    def own_copy(kind):
        return pltpu.make_async_copy(locals_[kind], fulls[kind].at[ring.me], own_sem.at[kind])

    def begin(kind):
        ring_copy(0, kind, ring.me, locals_[kind]).start()
        side_copy(0, kind, ring.me, locals_[kind]).start()
        own_copy(kind).start()

    for load in loads[:3]:
        load.wait()
    begin(0)
    loads[3].wait()
    turn_rows(out_load, out_own)
    begin(2)
    begin(1)
    loads[4].wait()
    turn_rows(down_load, ffn_own, 2 * units)
    for load in loads[5:]:
        load.wait()
    ffn_store = pltpu.make_async_copy(ffn_own, ffn_shard, load_sem.at[7])

    def forward(step, carry):
        @pl.when(step == 2)
        def _():
            ffn_store.start()

        shard = ring.behind(step)
        for kind in (0, 2, 1):
            here = fulls[kind].at[shard]
            ring_copy(step - 1, kind, shard, here).wait_recv()

            @pl.when(step < ring.count - 1)
            def _():
                ring_copy(step, kind, shard, here).start()

            side_copy(step, kind, shard, here).start()
        return carry

    lax.fori_loop(1, ring.count, forward, 0)

    def drain(step, carry):
        shard = ring.behind(step)
        for kind in range(kinds):
            here = fulls[kind].at[shard]

            @pl.when(step < ring.count - 1)
            def _():
                ring_copy(step, kind, shard, here).wait_send()

            side_copy(step, kind, shard, here).wait_send()
            side_copy(step, kind, shard, here).wait_recv()
        return carry

    lax.fori_loop(0, ring.count, drain, 0)
    ffn_store.wait()
    for kind in range(kinds):
        own_copy(kind).wait()


def gather_shards(shards, gains, w_q, w_k, w_v, w_o, w_gate, w_up, w_down):
    steps = shards // 2
    rows = w_q.shape[0]
    columns = w_q.shape[1] + w_k.shape[1] + w_v.shape[1]
    sems = pltpu.SemaphoreType.DMA((steps, 3))
    half = jnp.bfloat16
    return pl.pallas_call(
        functools.partial(gather_kernel, shards),
        out_shape=(
            jax.ShapeDtypeStruct((shards,) + gains.shape, gains.dtype),
            jax.ShapeDtypeStruct((shards, rows, columns), half),
            jax.ShapeDtypeStruct((shards, rows, w_o.shape[0]), half),
            jax.ShapeDtypeStruct((rows, 3 * w_down.shape[0]), half),
        ),
        in_specs=[VMEM_SPEC] + [ANY_SPEC] * 7,
        out_specs=(ANY_SPEC,) * 4,
        scratch_shapes=[
            pltpu.VMEM((rows, columns), half),
            pltpu.VMEM(w_o.shape, half),
            pltpu.VMEM((rows, w_o.shape[0]), half),
            pltpu.VMEM(w_down.shape, half),
            pltpu.VMEM((rows, 3 * w_down.shape[0]), half),
            sems,
            sems,
            sems,
            sems,
            pltpu.SemaphoreType.DMA((3,)),
            pltpu.SemaphoreType.DMA((8,)),
        ],
        compiler_params=pltpu.CompilerParams(
            collective_id=0, has_side_effects=True, vmem_limit_bytes=VMEM_BYTES
        ),
        name="gather_attention",
    )(gains, w_q, w_k, w_v, w_o, w_gate, w_up, w_down)


def turn_left(ring, left_all, turned, index, chip):
    rows = left_all.shape[1] // ring.shards
    first = (2 * chip + ring.core) * rows
    base = pl.multiple_of(first // 128 * 128, 128)
    block = left_all[:, pl.ds(base, 128)].astype(jnp.float32)
    turned[index] = jnp.transpose(block).astype(jnp.bfloat16)


def chunk_terms(ring, turned, index, right_all, low, size, chip, rows):
    if rows % 128 == 0:
        left = turned[index]
    else:
        first = (2 * chip + ring.core) * rows % 128
        left = turned[index, pl.ds(pl.multiple_of(first, rows), rows), :]
    return matmul(left, right_all[:, low : low + size])


def cut_columns(pairs, widths):
    chunks = []
    target = 0
    for left, right in pairs:
        width = widths[right]
        low = 0
        while low < width:
            size = min(1024, width - low)
            if width - low - size < 512:
                size = width - low
            chunks.append((left, right, low, size, target))
            low += size
            target += size
    return tuple(chunks), target


FFN_PAIRS = ((1, 2), (0, 0), (0, 1))
HEAD_PAIRS = ((2, 3), (3, 4))


def ffn_kernel(shards, groups, chunks, *refs):
    (
        x_ref,
        part_ref,
        gain_ref,
        grad_ref,
        shard_ref,
        behind_ref,
        hidden_ref,
        norm_part_ref,
        norm_other_ref,
        out_part_ref,
        carry_ref,
        normed_out,
        grad_out,
        d_gate_out,
        d_up_out,
        act_out,
    ) = refs[:16]
    count = len(groups)
    full = refs[16 : 16 + count]
    (
        part_other,
        out_total,
        norm_total,
        normed_all,
        grad_all,
        d_gate_all,
        d_up_all,
        act_all,
        turned,
        ring_send,
        ring_recv,
        side_send,
        side_recv,
        own_sem,
        part_sem,
        norm_send,
        norm_recv,
        left_sem,
        right_send,
        right_recv,
        sum_send,
        sum_recv,
        store_sem,
        free_sem,
    ) = refs[16 + count :]
    tokens = part_ref.shape[0]
    rows, units_all = shard_ref.shape
    units_all //= 3
    depth = normed_all.shape[1]
    blocks = depth // TILE
    ring = Ring(shards)
    mine = pl.ds(pl.multiple_of(ring.core * tokens, tokens), tokens)

    ticks = 3 * (ring.count - 2)
    last_tick = ticks - 4
    x_load = pltpu.make_async_copy(x_ref, hidden_ref, part_sem.at[2])
    grad_load = pltpu.make_async_copy(grad_ref, grad_all.at[mine], part_sem.at[3])
    x_load.start()
    grad_load.start()
    ring.greet(partner=True)

    def place(group, kind, shard):
        return full[group].at[kind, pl.ds(pl.multiple_of(shard * rows, rows), rows)]

    def cut(ref, group, kind):
        low, size = groups[group]
        return ref.at[:, pl.ds(kind * units_all + low, size)]

    def ring_copy(group, step, kind, shard, source):
        return send_to(
            {"dp": ring.following},
            source,
            place(group, kind, shard),
            ring_send.at[group, step, kind],
            ring_recv.at[group, step, kind],
        )

    def side_copy(group, step, kind, shard, source):
        return send_to(
            {"dp": ring.sibling},
            source,
            place(group, kind, shard),
            side_send.at[group, step, kind],
            side_recv.at[group, step, kind],
        )

    def own_copies(group, kind):
        return (
            pltpu.make_async_copy(
                cut(shard_ref, group, kind),
                place(group, kind, ring.me),
                own_sem.at[group, kind, 0],
            ),
            pltpu.make_async_copy(
                cut(behind_ref, group, kind),
                place(group, kind, ring.behind(1)),
                own_sem.at[group, kind, 1],
            ),
        )

    def begin(group):
        for kind in range(3):
            source = cut(behind_ref, group, kind)
            ring_copy(group, 1, kind, ring.behind(1), source).start()
            side_copy(group, 1, kind, ring.behind(1), source).start()
            side_copy(group, 0, kind, ring.me, cut(shard_ref, group, kind)).start()
            for copy in own_copies(group, kind):
                copy.start()

    def forward(group, tick):
        step = 2 + tick // 3
        kind = tick % 3
        shard = ring.behind(step)
        here = place(group, kind, shard)
        ring_copy(group, step - 1, kind, shard, here).wait_recv()

        @pl.when(step < ring.count - 1)
        def _():
            ring_copy(group, step, kind, shard, here).start()

        side_copy(group, step, kind, shard, here).start()

        if group + 1 < count:

            @pl.when(tick == last_tick)
            def _():
                begin(group + 1)

    def arrived(group):
        for kind in range(3):
            for copy in own_copies(group, kind):
                copy.wait()

        def one(step, carry):
            for kind in range(3):
                here = place(group, kind, ring.me)
                side_copy(group, step, kind, ring.me, here).wait_recv()
            return carry

        lax.fori_loop(0, ring.count, one, 0)

    def drain(group):
        def one(step, carry):
            for kind in range(3):
                here = place(group, kind, ring.me)

                @pl.when((step > 0) & (step < ring.count - 1))
                def _():
                    ring_copy(group, step, kind, ring.me, here).wait_send()

                side_copy(group, step, kind, ring.me, here).wait_send()
            return carry

        lax.fori_loop(0, ring.count, one, 0)

    lefts = (normed_all, grad_all)
    rights = (d_gate_all, d_up_all, act_all)

    def left_copy(index):
        here = lefts[index].at[mine]
        return send_to(
            {"dp": ring.sibling}, here, here, left_sem.at[0, index], left_sem.at[1, index]
        )

    def right_copy(group, index):
        low, size = groups[group]
        here = rights[index].at[mine, pl.ds(low, size)]
        return send_to(
            {"dp": ring.sibling},
            here,
            here,
            right_send.at[group, index],
            right_recv.at[group, index],
        )

    def hidden_units(group, tile):
        low, _ = groups[group]
        part = pl.ds(pl.multiple_of(tile * TILE, TILE), TILE)
        target = pl.ds(pl.multiple_of(low + tile * TILE, TILE), TILE)
        gate_pre = matmul(normed_all[mine, :], full[group][0, :, part])
        up_pre = matmul(normed_all[mine, :], full[group][1, :, part])
        d_act = matmul(grad_all[mine, :], full[group][2, :, part])
        sigmoid_gate = jax.nn.sigmoid(gate_pre)
        silu_gate = gate_pre * sigmoid_gate
        act_all[mine, target] = (silu_gate * up_pre).astype(jnp.bfloat16)
        d_gate_all[mine, target] = (
            d_act * up_pre * sigmoid_gate * (1.0 + gate_pre * (1.0 - sigmoid_gate))
        ).astype(jnp.bfloat16)
        d_up_all[mine, target] = (d_act * silu_gate).astype(jnp.bfloat16)

    def norm_terms(group, block):
        low, size = groups[group]
        units = pl.ds(low, size)
        features = pl.ds(pl.multiple_of(block * TILE, TILE), TILE)
        return matmul_nt(d_gate_all[mine, units], full[group][0, features, :]) + matmul_nt(
            d_up_all[mine, units], full[group][1, features, :]
        )

    def out_terms(group, block):
        low, size = groups[group]
        features = pl.ds(pl.multiple_of(block * TILE, TILE), TILE)
        return matmul_nt(act_all[mine, pl.ds(low, size)], full[group][2, features, :])

    def accumulate(group, block):
        features = pl.ds(pl.multiple_of(block * TILE, TILE), TILE)
        norm_new = norm_terms(group, block)
        out_new = out_terms(group, block)
        if group > 0:
            norm_new += norm_total[:, features]
            out_new += out_total[:, features]
        norm_total[:, features] = norm_new
        out_total[:, features] = out_new

    part_copy = send_to(partner_id(), part_ref, part_other, part_sem.at[0], part_sem.at[1])
    part_copy.start()
    begin(0)
    grad_load.wait()
    left_copy(1).start()

    def first_ticks(tick, carry):
        forward(0, tick)
        return carry

    lax.fori_loop(0, ticks, first_ticks, 0)
    x_load.wait()
    part_copy.wait()

    def norm_rows(block, carry):
        here = pl.ds(pl.multiple_of(block * 32, 32), 32)
        there = pl.ds(pl.multiple_of(ring.core * tokens + block * 32, 32), 32)
        hidden = hidden_ref[here, :] + (
            part_ref[here, :].astype(jnp.float32) + part_other[here, :].astype(jnp.float32)
        )
        hidden_ref[here, :] = hidden
        _, norm_two = rms_parts(hidden)
        normed_all[there, :] = (norm_two * gain_ref[...]).astype(jnp.bfloat16)
        return carry

    lax.fori_loop(0, tokens // 32, norm_rows, 0)

    for group in range(1, count):
        before = group - 1
        tiles = groups[before][1] // TILE
        arrived(before)
        if group == 1:
            left_copy(0).start()

        def tick_and_work(tick, carry):
            forward(group, tick)

            @pl.when((tick % 2 == 0) & (tick < 2 * tiles))
            def _():
                hidden_units(before, tick // 2)

            block = tick - (2 * tiles - 1)

            @pl.when(block == 0)
            def _():
                for index in range(3):
                    right_copy(before, index).start()

            @pl.when((block >= 0) & (block < blocks))
            def _():
                accumulate(before, block)

            return carry

        lax.fori_loop(0, ticks, tick_and_work, 0)
        if group == 1:
            drain(0)
            pl.semaphore_signal(
                free_sem, inc=1, device_id={"dp": ring.previous}, device_id_type=MESH_IDS
            )

    last = count - 1
    arrived(last)

    def last_units(tile, carry):
        hidden_units(last, tile)
        return carry

    lax.fori_loop(0, groups[last][1] // TILE, last_units, 0)

    def norm_copy(block):
        features = pl.ds(pl.multiple_of(block * TILE, TILE), TILE)
        return send_to(
            partner_id(),
            norm_part_ref.at[:, features],
            norm_other_ref.at[:, features],
            norm_send.at[block],
            norm_recv.at[block],
        )

    def last_norm(block, carry):
        features = pl.ds(pl.multiple_of(block * TILE, TILE), TILE)
        norm_part_ref[:, features] = (norm_total[:, features] + norm_terms(last, block)).astype(
            jnp.bfloat16
        )

        @pl.when(block > 0)
        def _():
            norm_copy(block - 1).start()

        @pl.when(block == 0)
        def _():
            for index in range(3):
                right_copy(last, index).start()

        return carry

    lax.fori_loop(0, blocks, last_norm, 0)

    def last_out(block, carry):
        features = pl.ds(pl.multiple_of(block * TILE, TILE), TILE)
        out_part_ref[:, features] = (out_total[:, features] + out_terms(last, block)).astype(
            jnp.bfloat16
        )

        @pl.when(block == 0)
        def _():
            norm_copy(blocks - 1).start()

        return carry

    lax.fori_loop(0, blocks, last_out, 0)

    for index in range(2):
        left_copy(index).wait_recv()
    for group in range(count):
        for index in range(3):
            right_copy(group, index).wait_recv()
    outs = (normed_out, grad_out, d_gate_out, d_up_out, act_out)
    stores = [
        pltpu.make_async_copy(source, target, store_sem.at[index])
        for index, (source, target) in enumerate(zip(lefts + rights, outs))
    ]
    for store in stores:
        store.start()

    def sum_slot(kind, chunk):
        _, _, _, size, _ = chunks[chunk]
        return full[0].at[kind, pl.ds(chunk * rows, rows), pl.ds(0, size)]

    def sum_copy(chunk):
        return send_to(
            {"dp": ring.following},
            sum_slot(0, chunk),
            sum_slot(1, chunk),
            sum_send.at[chunk],
            sum_recv.at[chunk],
        )

    def terms(chunk, chip):
        left, right, low, size, _ = chunks[chunk]
        return chunk_terms(ring, turned, left, rights[right], low, size, chip, rows)

    chip = ring.chip(-1)
    for index in range(2):
        turn_left(ring, lefts[index], turned, index, chip)
    pl.semaphore_wait(free_sem, 1)
    for chunk in range(len(chunks)):
        size = chunks[chunk][3]
        full[0][0, chunk * rows : (chunk + 1) * rows, 0:size] = terms(chunk, chip).astype(
            jnp.bfloat16
        )
        if chunk > 0:
            sum_copy(chunk - 1).start()
    chip = ring.chip(-2)
    for index in range(2):
        turn_left(ring, lefts[index], turned, index, chip)
    sum_copy(len(chunks) - 1).start()
    for chunk in range(len(chunks)):
        _, _, _, size, target = chunks[chunk]
        total = terms(chunk, chip)
        sum_copy(chunk).wait_recv()
        total += full[0][1, chunk * rows : (chunk + 1) * rows, 0:size].astype(jnp.float32)
        carry_ref[:, target : target + size] = total.astype(jnp.bfloat16)

    for group in range(1, count):
        drain(group)
    for index in range(2):
        left_copy(index).wait_send()
    for group in range(count):
        for index in range(3):
            right_copy(group, index).wait_send()
    for chunk in range(len(chunks)):
        sum_copy(chunk).wait_send()
    for store in stores:
        store.wait()

    def drain_norm(block, carry):
        norm_copy(block).wait()
        return carry

    lax.fori_loop(0, blocks, drain_norm, 0)


def ffn_groups(units, steps):
    tiles = units // TILE
    last = max(1, min(2, tiles - 2))
    first = min(max(1, steps - 4), (tiles - last) // 2)
    sizes = [first, tiles - last - first, last]
    groups = []
    low = 0
    for size in sizes:
        groups.append((low * TILE, size * TILE))
        low += size
    return tuple(groups)


def ffn_pass(shards, x_rows, part, gain, grad_rows, own, behind):
    tokens, depth = x_rows.shape
    rows, units = own.shape
    units //= 3
    steps = shards // 2
    groups = ffn_groups(units, steps)
    chunks, total = cut_columns(FFN_PAIRS, (units,) * 3)
    half = jnp.bfloat16
    wide = jax.ShapeDtypeStruct((tokens, depth), half)
    both_wide = jax.ShapeDtypeStruct((2 * tokens, depth), half)
    both_inner = jax.ShapeDtypeStruct((2 * tokens, units), half)
    full = []
    for _, size in groups:
        full.append(pltpu.VMEM((3, depth, size), half))
    sems = pltpu.SemaphoreType.DMA((len(groups), steps, 3))
    block_sems = pltpu.SemaphoreType.DMA((depth // TILE,))
    pair_sems = pltpu.SemaphoreType.DMA((len(groups), 3))
    chunk_sems = pltpu.SemaphoreType.DMA((len(chunks),))
    return pl.pallas_call(
        functools.partial(ffn_kernel, shards, groups, chunks),
        out_shape=(
            jax.ShapeDtypeStruct((tokens, depth), jnp.float32),
            wide,
            wide,
            wide,
            jax.ShapeDtypeStruct((rows, total), half),
            both_wide,
            both_wide,
            both_inner,
            both_inner,
            both_inner,
        ),
        in_specs=[ANY_SPEC, VMEM_SPEC, VMEM_SPEC] + [ANY_SPEC] * 3,
        out_specs=(VMEM_SPEC,) * 5 + (ANY_SPEC,) * 5,
        scratch_shapes=full
        + [
            pltpu.VMEM((tokens, depth), half),
            pltpu.VMEM((tokens, depth), jnp.float32),
            pltpu.VMEM((tokens, depth), jnp.float32),
            pltpu.VMEM((2 * tokens, depth), half),
            pltpu.VMEM((2 * tokens, depth), half),
            pltpu.VMEM((2 * tokens, units), half),
            pltpu.VMEM((2 * tokens, units), half),
            pltpu.VMEM((2 * tokens, units), half),
            pltpu.VMEM((2, 128, 2 * tokens), half),
            sems,
            sems,
            sems,
            sems,
            pltpu.SemaphoreType.DMA((len(groups), 3, 2)),
            pltpu.SemaphoreType.DMA((4,)),
            block_sems,
            block_sems,
            pltpu.SemaphoreType.DMA((2, 2)),
            pair_sems,
            pair_sems,
            chunk_sems,
            chunk_sems,
            pltpu.SemaphoreType.DMA((5,)),
            pltpu.SemaphoreType.REGULAR,
        ],
        compiler_params=pltpu.CompilerParams(
            collective_id=1, has_side_effects=True, vmem_limit_bytes=VMEM_BYTES
        ),
        name="ffn_ring",
    )(x_rows, part, gain, grad_rows, own, behind)


def reduce_kernel(shards, ffn_chunks, head_chunks, *refs):
    (
        normed_two_ref,
        grad_ref,
        hidden_rows_ref,
        normed_one_ref,
        d_gate_ref,
        d_up_ref,
        act_ref,
        attended_ref,
        d_qkv_ref,
        carry_ref,
        out_part_ref,
        norm_part_ref,
        hidden_ref,
        d_hidden_ref,
        scaled_ref,
        inv_ref,
        gain_ref,
        sums_ref,
        layer_out,
        x_grad_out,
        gate_grad,
        up_grad,
        down_grad,
        o_grad,
        qkv_grad,
        sums_out,
        normed_two_all,
        grad_all,
        hidden_rows_all,
        normed_one_all,
        d_gate_all,
        d_up_all,
        act_all,
        attended_all,
        d_qkv_all,
        turned,
        ffn_slots,
        head_slots,
        norm_here,
        norm_there,
        out_here,
        out_there,
        hidden_buf,
        d_hidden_buf,
        scaled_buf,
        column_total,
        sums_own,
        sums_in,
        ffn_send,
        ffn_recv,
        head_send,
        head_recv,
        load_sem,
        side_send,
        side_recv,
        part_sem,
        row_sem,
        sums_send,
        sums_recv,
    ) = refs
    ring = Ring(shards)
    tokens, depth = out_part_ref.shape
    rows = head_slots.shape[1]
    mine = pl.ds(pl.multiple_of(ring.core * tokens, tokens), tokens)
    lefts = (normed_two_all, grad_all, hidden_rows_all, normed_one_all)
    rights = (d_gate_all, d_up_all, act_all, attended_all, d_qkv_all)

    head_pairs = (
        (hidden_rows_ref, hidden_rows_all),
        (attended_ref, attended_all),
        (normed_one_ref, normed_one_all),
        (d_qkv_ref, d_qkv_all),
    )
    head_loads = [
        pltpu.make_async_copy(source, target.at[mine], load_sem.at[index])
        for index, (source, target) in enumerate(head_pairs)
    ]
    ffn_loads = [
        pltpu.make_async_copy(source, target, load_sem.at[4 + index])
        for index, (source, target) in enumerate(
            (
                (carry_ref, ffn_slots.at[0]),
                (grad_ref, grad_all),
                (act_ref, act_all),
                (normed_two_ref, normed_two_all),
                (d_gate_ref, d_gate_all),
                (d_up_ref, d_up_all),
            )
        )
    ]
    row_loads = [
        pltpu.make_async_copy(source, target, row_sem.at[index])
        for index, (source, target) in enumerate(
            (
                (norm_part_ref, norm_here),
                (d_hidden_ref, d_hidden_buf),
                (scaled_ref, scaled_buf),
                (out_part_ref, out_here),
                (hidden_ref, hidden_buf),
            )
        )
    ]
    for load in head_loads + ffn_loads + row_loads:
        load.start()
    ring.greet(partner=True, everyone=True)
    sides = [
        send_to(
            {"dp": ring.sibling}, source, target.at[mine], side_send.at[index], side_recv.at[index]
        )
        for index, (source, target) in enumerate(head_pairs)
    ]
    for side in sides:
        side.start()
    norm_copy = send_to(partner_id(), norm_part_ref, norm_there, part_sem.at[0], part_sem.at[1])
    out_copy = send_to(partner_id(), out_part_ref, out_there, part_sem.at[2], part_sem.at[3])
    norm_copy.start()
    out_copy.start()

    def ffn_copy(step, chunk):
        _, _, _, size, target = ffn_chunks[chunk]
        columns = pl.ds(target, size)
        return send_to(
            {"dp": ring.following},
            ffn_slots.at[step - 2, :, columns],
            ffn_slots.at[step - 1, :, columns],
            ffn_send.at[step - 2, chunk],
            ffn_recv.at[step - 2, chunk],
        )

    def head_copy(step, chunk):
        _, _, _, size, target = head_chunks[chunk]
        columns = pl.ds(target, size)
        return send_to(
            {"dp": ring.following},
            head_slots.at[step, :, columns],
            head_slots.at[step + 1, :, columns],
            head_send.at[step, chunk],
            head_recv.at[step, chunk],
        )

    def head_terms(chunk, chip):
        left, right, low, size, _ = head_chunks[chunk]
        return chunk_terms(ring, turned, left, rights[right], low, size, chip, rows)

    def ffn_terms(chunk, chip):
        left, right, low, size, _ = ffn_chunks[chunk]
        return chunk_terms(ring, turned, left, rights[right], low, size, chip, rows)

    def turn(chip, indices):
        for index in indices:
            turn_left(ring, lefts[index], turned, index, chip)

    def sums_copy(offset):
        return send_to(
            {"dp": (ring.me + offset) % shards},
            sums_own.at[(ring.me + offset) % shards],
            sums_in.at[ring.me],
            sums_send.at[offset],
            sums_recv.at[offset],
        )

    def finish_input_grad():
        for load in row_loads[:3]:
            load.wait()
        norm_copy.wait()
        sums_own[...] = sums_ref[...]
        column_total[...] = jnp.zeros_like(column_total)

        def one(block, carry):
            here = pl.ds(pl.multiple_of(block * 16, 16), 16)
            total = norm_here[here, :].astype(jnp.float32) + norm_there[here, :].astype(
                jnp.float32
            )
            scaled = scaled_buf[here, :]
            product = total * scaled
            column_total[...] += product[0:8] + product[8:16]
            scaled_gain = total * gain_ref[...]
            mean = jnp.mean(scaled_gain * scaled, axis=-1, keepdims=True)
            d_hidden_buf[here, :] = d_hidden_buf[here, :] + inv_ref[here, :] * (
                scaled_gain - scaled * mean
            )
            return carry

        lax.fori_loop(0, tokens // 16, one, 0)
        width = depth // shards
        band = max(width, 128)
        for low in range(0, depth, band):
            sums = jnp.sum(column_total[:, low : low + band], axis=0, keepdims=True)
            for inner in range(0, band, width):
                sums_own[(low + inner) // width, 1:2, 0:width] = sums[:, inner : inner + width]

    def send_sums():
        pltpu.make_async_copy(d_hidden_buf, x_grad_out, row_sem.at[5]).start()

        def one(offset, carry):
            sums_copy(offset).start()
            return carry

        lax.fori_loop(1, shards, one, 0)

    def finish_output():
        for load in row_loads[3:]:
            load.wait()
        out_copy.wait()

        def one(block, carry):
            here = pl.ds(pl.multiple_of(block * 16, 16), 16)
            hidden_buf[here, :] = hidden_buf[here, :] + (
                out_here[here, :].astype(jnp.float32) + out_there[here, :].astype(jnp.float32)
            )
            return carry

        lax.fori_loop(0, tokens // 16, one, 0)

    heads = len(head_chunks)
    ffns = len(ffn_chunks)

    def head_step(step, chip, chunk):
        _, _, _, size, target = head_chunks[chunk]
        total = head_terms(chunk, chip)
        head_copy(step - 1, chunk).wait_recv()
        return total + head_slots[step, :, target : target + size].astype(jnp.float32)

    def ffn_step(step, chip, chunk, peeled):
        _, _, _, size, target = ffn_chunks[chunk]
        total = ffn_terms(chunk, chip)
        if peeled:
            ffn_copy(step - 1, chunk).wait_recv()
        else:

            @pl.when(step > 2)
            def _():
                ffn_copy(step - 1, chunk).wait_recv()

        return total + ffn_slots[step - 2, :, target : target + size].astype(jnp.float32)

    def store_head(step, chunk, total):
        _, _, _, size, target = head_chunks[chunk]
        head_slots[step, :, target : target + size] = total.astype(jnp.bfloat16)

    def store_ffn(step, chunk, total):
        _, _, _, size, target = ffn_chunks[chunk]
        ffn_slots[step - 2, :, target : target + size] = total.astype(jnp.bfloat16)

    for load in head_loads:
        load.wait()
    for side in sides:
        side.wait_recv()
    chip = ring.chip(-1)
    turn(chip, (2, 3))
    for chunk in range(heads):
        store_head(0, chunk, head_terms(chunk, chip))
        if chunk > 0:
            head_copy(0, chunk - 1).start()
    for load in ffn_loads:
        load.wait()

    def one_step(index, carry):
        ffn_at = index + 2
        head_at = index + 1
        ffn_chip = ring.chip(-1 - ffn_at)
        head_chip = ring.chip(-1 - head_at)
        turn(ffn_chip, (0, 1))
        head_copy(head_at - 1, heads - 1).start()
        turn(head_chip, (2, 3))
        for chunk in range(ffns):
            store_ffn(ffn_at, chunk, ffn_step(ffn_at, ffn_chip, chunk, False))
            if chunk > 0:
                ffn_copy(ffn_at, chunk - 1).start()
        for chunk in range(heads):
            store_head(head_at, chunk, head_step(head_at, head_chip, chunk))
            if chunk > 0:
                head_copy(head_at, chunk - 1).start()
            else:
                ffn_copy(ffn_at, ffns - 1).start()

        @pl.when(index == 1)
        def _():
            finish_input_grad()

        @pl.when(index == 2)
        def _():
            send_sums()
            finish_output()

        @pl.when(index == 3)
        def _():
            pltpu.make_async_copy(hidden_buf, layer_out, row_sem.at[6]).start()

        return carry

    final = ring.count - 1
    lax.fori_loop(0, ring.count - 3, one_step, 0)
    before = ring.chip(-final)
    turn(before, (2, 3))
    head_copy(final - 2, heads - 1).start()
    for chunk in range(heads):
        store_head(final - 1, chunk, head_step(final - 1, before, chunk))
        if chunk > 0:
            head_copy(final - 1, chunk - 1).start()
    chip = ring.chip(0)
    turn(chip, (0, 1))
    head_copy(final - 1, heads - 1).start()
    turn(chip, (2, 3))
    grads = (gate_grad, up_grad, down_grad, o_grad, qkv_grad)
    for chunk in range(ffns):
        _, right, low, size, _ = ffn_chunks[chunk]
        total = ffn_step(final, chip, chunk, True)
        if right == 2:
            down_grad[low : low + size, :] = jnp.transpose(total)
        else:
            grads[right][:, low : low + size] = total
    for chunk in range(heads):
        _, right, low, size, _ = head_chunks[chunk]
        total = head_step(final, chip, chunk)
        if right == 3:
            o_grad[low : low + size, :] = jnp.transpose(total)
        else:
            qkv_grad[:, low : low + size] = total

    def add_sums(offset, total):
        sums_copy(offset).wait_recv()
        return total + sums_in[(ring.me - offset + shards) % shards]

    sums_out[...] = lax.fori_loop(1, shards, add_sums, sums_own[ring.me])

    def drain_heads(step, carry):
        for chunk in range(heads):
            head_copy(step, chunk).wait_send()
        return carry

    def drain_ffn(step, carry):
        for chunk in range(ffns):
            ffn_copy(step, chunk).wait_send()
        return carry

    def drain_sums(offset, carry):
        sums_copy(offset).wait_send()
        return carry

    lax.fori_loop(0, final, drain_heads, 0)
    lax.fori_loop(2, final, drain_ffn, 0)
    lax.fori_loop(1, shards, drain_sums, 0)
    for side in sides:
        side.wait_send()
    pltpu.make_async_copy(d_hidden_buf, x_grad_out, row_sem.at[5]).wait()
    pltpu.make_async_copy(hidden_buf, layer_out, row_sem.at[6]).wait()


def reduce_pass(shards, both, heads, carry, out_part, norm_part, rows_f32, inv, gain, sums):
    normed_two, grad_rows, d_gate, d_up, activated = both
    hidden_rows, normed_one, attended, d_qkv = heads
    tokens, depth = out_part.shape
    units = d_gate.shape[1]
    steps = shards // 2
    rows = depth // shards
    widths = (units, units, units, attended.shape[1], d_qkv.shape[1])
    ffn_chunks, ffn_total = cut_columns(FFN_PAIRS, widths)
    head_chunks, head_total = cut_columns(HEAD_PAIRS, widths)
    half = jnp.bfloat16
    wide = jax.ShapeDtypeStruct((tokens, depth), jnp.float32)
    both_wide = pltpu.VMEM((2 * tokens, depth), half)
    one_half = pltpu.VMEM((tokens, depth), half)
    one_full = pltpu.VMEM((tokens, depth), jnp.float32)
    dma = pltpu.SemaphoreType.DMA
    return pl.pallas_call(
        functools.partial(reduce_kernel, shards, ffn_chunks, head_chunks),
        out_shape=(
            wide,
            wide,
            jax.ShapeDtypeStruct((rows, units), jnp.float32),
            jax.ShapeDtypeStruct((rows, units), jnp.float32),
            jax.ShapeDtypeStruct((units, rows), jnp.float32),
            jax.ShapeDtypeStruct((attended.shape[1], rows), jnp.float32),
            jax.ShapeDtypeStruct((rows, d_qkv.shape[1]), jnp.float32),
            jax.ShapeDtypeStruct(sums.shape[1:], jnp.float32),
        ),
        in_specs=[ANY_SPEC] * 15 + [VMEM_SPEC] * 3,
        out_specs=(ANY_SPEC, ANY_SPEC) + (VMEM_SPEC,) * 6,
        scratch_shapes=[both_wide] * 4
        + [pltpu.VMEM((2 * tokens, width), half) for width in widths]
        + [
            pltpu.VMEM((4, 128, 2 * tokens), half),
            pltpu.VMEM((steps - 2, rows, ffn_total), half),
            pltpu.VMEM((steps, rows, head_total), half),
            one_half,
            one_half,
            one_half,
            one_half,
            one_full,
            one_full,
            one_full,
            pltpu.VMEM((8, depth), jnp.float32),
            pltpu.VMEM(sums.shape, jnp.float32),
            pltpu.VMEM(sums.shape, jnp.float32),
            dma((steps - 3, len(ffn_chunks))),
            dma((steps - 3, len(ffn_chunks))),
            dma((steps - 1, len(head_chunks))),
            dma((steps - 1, len(head_chunks))),
            dma((10,)),
            dma((4,)),
            dma((4,)),
            dma((4,)),
            dma((7,)),
            dma((shards,)),
            dma((shards,)),
        ],
        compiler_params=pltpu.CompilerParams(
            collective_id=2, has_side_effects=True, vmem_limit_bytes=VMEM_BYTES
        ),
        name="reduce_ring",
    )(
        normed_two,
        grad_rows,
        hidden_rows,
        normed_one,
        d_gate,
        d_up,
        activated,
        attended,
        d_qkv,
        carry,
        out_part,
        norm_part,
        *rows_f32,
        inv,
        gain,
        sums,
    )


def emit_kernel(cuts, *refs):
    ins = refs[: len(cuts)]
    count = sum(len(cut) for cut in cuts)
    outs = refs[len(cuts) : len(cuts) + count]
    sums_ref, sums_one, sums_two = refs[len(cuts) + count : len(cuts) + count + 3]
    bufs = refs[len(cuts) + count + 3 : -2]
    load_sem, store_sem = refs[-2:]
    loads = [
        pltpu.make_async_copy(source, buf, load_sem.at[index])
        for index, (source, buf) in enumerate(zip(ins, bufs))
    ]
    for load in loads:
        load.start()
    stores = []
    for index, cut in enumerate(cuts):
        loads[index].wait()
        for low, size in cut:
            at = len(stores)
            source = bufs[index] if len(cut) == 1 else bufs[index].at[:, pl.ds(low, size)]
            stores.append(pltpu.make_async_copy(source, outs[at], store_sem.at[at]))
            stores[-1].start()
    sums_one[...] = sums_ref[1, : sums_one.shape[0]]
    sums_two[...] = sums_ref[0, : sums_two.shape[0]]
    for store in stores:
        store.wait()


def emit(arrays, cuts, sums, rows):
    outs = []
    for array, cut in zip(arrays, cuts):
        for _, size in cut:
            outs.append(jax.ShapeDtypeStruct((array.shape[0], size), array.dtype))
    count = len(outs)
    line = jax.ShapeDtypeStruct((rows,), jnp.float32)

    def kernel(*refs):
        ins = refs[: len(arrays)]
        sums_ref = refs[len(arrays)]
        rest = refs[len(arrays) + 1 :]
        emit_kernel(
            cuts, *ins, *rest[:count], sums_ref, rest[count], rest[count + 1], *rest[count + 2 :]
        )

    return pl.pallas_call(
        kernel,
        out_shape=tuple(outs) + (line, line),
        in_specs=[ANY_SPEC] * len(arrays) + [VMEM_SPEC],
        out_specs=(ANY_SPEC,) * count + (VMEM_SPEC, VMEM_SPEC),
        scratch_shapes=[pltpu.VMEM(array.shape, array.dtype) for array in arrays]
        + [pltpu.SemaphoreType.DMA((len(arrays),)), pltpu.SemaphoreType.DMA((count,))],
        compiler_params=pltpu.CompilerParams(vmem_limit_bytes=VMEM_BYTES),
        name="emit_results",
    )(*arrays, sums)


def body(
    shards,
    layer_input,
    positions,
    norm1_gain,
    w_q,
    w_k,
    w_v,
    w_o,
    norm2_gain,
    w_gate,
    w_up,
    w_down,
    out_grad,
):
    tokens, depth = layer_input.shape
    rows = w_q.shape[0]
    head_count = w_q.shape[1] // HD
    kv_count = w_k.shape[1] // HD
    query_cols = head_count * HD
    kv_cols = kv_count * HD
    pairs = ring_pairs(shards)

    gains = jnp.stack([norm1_gain, norm2_gain]).astype(jnp.float32)
    gains = jnp.pad(gains, ((0, 6), (0, max(128 - rows, 0))))
    gains_all, qkv_all, out_all, own = gather_shards(
        shards, gains, w_q, w_k, w_v, w_o, w_gate, w_up, w_down
    )
    gain_one = gains_all[:, 0, :rows].reshape(1, depth)
    gain_two = gains_all[:, 1, :rows].reshape(1, depth)
    qkv_w = qkv_all.reshape(depth, query_cols + 2 * kv_cols)
    out_w = out_all.reshape(depth, query_cols)
    behind = lax.ppermute(own, "dp", pairs)

    inv_one, norm_one = rms_parts(layer_input)
    normed_one = (norm_one * gain_one).astype(jnp.bfloat16)
    cos_table, sin_table = rope_tables(positions, HD)
    qkv = matmul(normed_one, qkv_w)
    queries = rotate(
        qkv[:, :query_cols].reshape(tokens, head_count, HD), cos_table, sin_table, 1.0
    ).astype(jnp.bfloat16)
    key_rows = rotate(
        qkv[:, query_cols : query_cols + kv_cols].reshape(tokens, kv_count, HD),
        cos_table,
        sin_table,
        1.0,
    ).astype(jnp.bfloat16)
    value_rows = qkv[:, query_cols + kv_cols :].astype(jnp.bfloat16).reshape(tokens, kv_count, HD)
    seq_count = tokens // L
    query_seq = queries.reshape(seq_count, L, head_count, HD)
    key_seq = key_rows.reshape(seq_count, L, kv_count, HD)
    value_seq = value_rows.reshape(seq_count, L, kv_count, HD)
    attended, log_total = lax.map(
        lambda block_in: attend(block_in[0], block_in[1], block_in[2]),
        (query_seq, key_seq, value_seq),
    )
    attended_rows = attended.reshape(tokens, query_cols)
    part = matmul_nt(attended_rows, out_w).astype(jnp.bfloat16)
    grad_rows = out_grad.astype(jnp.bfloat16)

    hidden, norm_part, norm_other, out_part, carry, *both = ffn_pass(
        shards, layer_input, part, gain_two, grad_rows, own, behind
    )
    carry = lax.ppermute(carry, "dp", pairs)

    inv_two, norm_two = rms_parts(hidden)
    d_norm_two = norm_part.astype(jnp.float32) + norm_other.astype(jnp.float32)
    grad_gain_two = jnp.sum(d_norm_two * norm_two, axis=0)
    e_two = d_norm_two * gain_two
    d_hidden = out_grad + inv_two * (
        e_two - norm_two * jnp.mean(e_two * norm_two, axis=-1, keepdims=True)
    )
    hidden_rows = d_hidden.astype(jnp.bfloat16)
    d_attended = matmul(hidden_rows, out_w).astype(jnp.bfloat16)
    d_query, d_keys, d_values = lax.map(
        lambda block_in: attend_back(
            block_in[0], block_in[1], block_in[2], block_in[3], block_in[4], block_in[5]
        ),
        (
            query_seq,
            key_seq,
            value_seq,
            attended,
            d_attended.reshape(seq_count, L, query_cols),
            log_total,
        ),
    )
    dq_raw = (
        rotate(d_query.reshape(tokens, head_count, HD), cos_table, sin_table, -1.0)
        .astype(jnp.bfloat16)
        .reshape(tokens, query_cols)
    )
    dk_raw = (
        rotate(d_keys.reshape(tokens, kv_count, HD), cos_table, sin_table, -1.0)
        .astype(jnp.bfloat16)
        .reshape(tokens, kv_cols)
    )
    dv_rows = d_values.astype(jnp.bfloat16).reshape(tokens, kv_cols)
    d_qkv = jnp.concatenate([dq_raw, dk_raw, dv_rows], axis=1)
    norm_one_part = matmul_nt(d_qkv, qkv_w).astype(jnp.bfloat16)

    sums = grad_gain_two.reshape(shards, 1, rows)
    sums = jnp.pad(sums, ((0, 0), (0, 7), (0, max(128 - rows, 0))))
    (
        layer_output,
        x_grad,
        shard_gate,
        shard_up,
        shard_down,
        shard_out,
        shard_qkv,
        sums_out,
    ) = reduce_pass(
        shards,
        both,
        (hidden_rows, normed_one, attended_rows, d_qkv),
        carry,
        out_part,
        norm_one_part,
        (hidden, d_hidden, norm_one),
        inv_one,
        gain_one,
        sums,
    )
    cuts = [((0, array.shape[1]),) for array in (layer_output, x_grad)]
    cuts.append(
        ((0, query_cols), (query_cols, kv_cols), (query_cols + kv_cols, kv_cols))
    )
    cuts += [((0, array.shape[1]),) for array in (shard_out, shard_gate, shard_up, shard_down)]
    (
        layer_output,
        x_grad,
        shard_query,
        shard_key,
        shard_value,
        shard_out,
        shard_gate,
        shard_up,
        shard_down,
        sums_one,
        sums_two,
    ) = emit(
        (layer_output, x_grad, shard_qkv, shard_out, shard_gate, shard_up, shard_down),
        cuts,
        sums_out,
        rows,
    )
    return (
        layer_output,
        x_grad,
        sums_one,
        shard_query,
        shard_key,
        shard_value,
        shard_out,
        sums_two,
        shard_gate,
        shard_up,
        shard_down,
    )


def solution(mesh):
    in_specs = (
        P("dp", None),
        P("dp"),
        P("dp"),
        P("dp", "tensor"),
        P("dp", "tensor"),
        P("dp", "tensor"),
        P("tensor", "dp"),
        P("dp"),
        P("dp", "tensor"),
        P("dp", "tensor"),
        P("tensor", "dp"),
        P("dp", None),
    )
    out_specs = (
        P("dp", None),
        P("dp", None),
        P("dp"),
        P("dp", "tensor"),
        P("dp", "tensor"),
        P("dp", "tensor"),
        P("tensor", "dp"),
        P("dp"),
        P("dp", "tensor"),
        P("dp", "tensor"),
        P("tensor", "dp"),
    )

    def layer(*args):
        return body(mesh.shape["dp"], *args)

    return jax.shard_map(
        layer, mesh=mesh, in_specs=in_specs, out_specs=out_specs, check_vma=False
    )
```

```python
import functools
import math

import jax
import jax.numpy as jnp
from jax import lax
from jax.experimental import pallas as pl
from jax.experimental.pallas import tpu as pltpu
from jax.sharding import PartitionSpec as P


HD = 64
L = 256
TILE = 256
VMEM_BYTES = 67043328

epsilon = 1e-05

MESH_IDS = pl.DeviceIdType.MESH
VMEM_SPEC = pl.BlockSpec(memory_space=pltpu.VMEM)
ANY_SPEC = pl.BlockSpec(memory_space=pl.ANY)


def matmul(left_side, right_side):
    return jnp.dot(left_side, right_side, preferred_element_type=jnp.float32)


def matmul_nt(left_side, right_side):
    return lax.dot_general(
        left_side, right_side, (((1,), (1,)), ((), ())), preferred_element_type=jnp.float32
    )


def rms_parts(row_values):
    inv_rms = lax.rsqrt(jnp.mean(row_values * row_values, axis=-1, keepdims=True) + epsilon)
    return (inv_rms, row_values * inv_rms)


def rope_tables(pos_rows, head_dim):
    half_dim = head_dim // 2
    frequency = jnp.exp(
        jnp.arange(half_dim, dtype=jnp.float32) * (-2.0 * math.log(10000.0) / head_dim)
    )
    angles = pos_rows.astype(jnp.float32)[:, None] * frequency[None, :]
    return (jnp.cos(angles), jnp.sin(angles))


def rotate(row_values, cos_table, sin_table, direction_sign):
    half_dim = row_values.shape[-1] // 2
    first_half = row_values[..., :half_dim]
    second = row_values[..., half_dim:]
    cos_part = cos_table[:, None, :]
    sin_part = sin_table[:, None, :] * direction_sign
    return jnp.concatenate(
        [first_half * cos_part - second * sin_part, second * cos_part + first_half * sin_part],
        axis=-1,
    )


def causal_scores(queries, key_rows):
    length, head_count, head_dim = queries.shape
    kv_count = key_rows.shape[1]
    grouped = queries.reshape(length, kv_count, head_count // kv_count, head_dim)
    scores = jnp.einsum(
        "qkgd,pkd->kgqp", grouped, key_rows, preferred_element_type=jnp.float32
    ) * head_dim ** (-0.5)
    future_mask = jnp.arange(length)[None, :] > jnp.arange(length)[:, None]
    return (grouped, jnp.where(future_mask, -jnp.inf, scores))


def attend(queries, key_rows, value_rows):
    _, scores = causal_scores(queries, key_rows)
    row_top = jnp.max(scores, axis=-1, keepdims=True)
    log_total = row_top + jnp.log(jnp.sum(jnp.exp(scores - row_top), axis=-1, keepdims=True))
    weights = jnp.exp(scores - log_total).astype(jnp.bfloat16)
    attended = jnp.einsum("kgqp,pkd->qkgd", weights, value_rows, preferred_element_type=jnp.float32)
    return (attended.reshape(queries.shape[0], -1).astype(jnp.bfloat16), log_total)


def attend_back(queries, key_rows, value_rows, attended, d_attended, log_total):
    length, head_count, head_dim = queries.shape
    kv_count = key_rows.shape[1]
    grouped, scores = causal_scores(queries, key_rows)
    prob_rows = jnp.exp(scores - log_total)
    d_grouped = d_attended.reshape(length, kv_count, head_count // kv_count, head_dim)
    out_grouped = attended.reshape(length, kv_count, head_count // kv_count, head_dim)
    row_delta = jnp.sum(out_grouped.astype(jnp.float32) * d_grouped.astype(jnp.float32), axis=-1)
    row_delta = jnp.transpose(row_delta, (1, 2, 0))[..., None]
    d_probs = jnp.einsum(
        "qkgd,pkd->kgqp", d_grouped, value_rows, preferred_element_type=jnp.float32
    )
    d_scores = (prob_rows * (d_probs - row_delta) * head_dim ** (-0.5)).astype(jnp.bfloat16)
    d_query = jnp.einsum("kgqp,pkd->qkgd", d_scores, key_rows, preferred_element_type=jnp.float32)
    d_keys = jnp.einsum("kgqp,qkgd->pkd", d_scores, grouped, preferred_element_type=jnp.float32)
    d_values = jnp.einsum(
        "kgqp,qkgd->pkd",
        prob_rows.astype(jnp.bfloat16),
        d_grouped,
        preferred_element_type=jnp.float32,
    )
    return (d_query.reshape(length, head_count, head_dim), d_keys, d_values)


def chip_at(place, count):
    side = place // (count // 2)
    row = place + side * (count - 1 - 2 * place)
    return 2 * row + side


def place_of(chip, count):
    side = chip % 2
    row = chip // 2
    return row + side * (count - 1 - 2 * row)


class Ring:
    def __init__(self, shards):
        self.shards = shards
        self.count = shards // 2
        self.me = lax.axis_index("dp")
        self.core = self.me % 2
        self.place = place_of(self.me // 2, self.count)
        self.sign = 1 - 2 * self.core
        self.rows = shards // 4
        self.row = self.me // 4
        self.side = self.me // 2 % 2
        self.following = self.device(1, self.core)
        self.previous = self.device(-1, self.core)
        self.sibling = self.device(0, 1 - self.core)

    def chip(self, steps):
        place = (self.place + self.sign * steps + 2 * self.count) % self.count
        return chip_at(place, self.count)

    def device(self, steps, core):
        return self.chip(steps) * 2 + core

    def at(self, row, side):
        return (2 * row + side) * 2 + self.core

    def owner(self, slot):
        short = jnp.minimum(self.row, self.rows - 1 - self.row)
        far = self.rows - 1 - short
        way = 1 - 2 * (self.row // (self.rows // 2))
        turn = slot - (far - short)
        return jnp.where(
            turn < 0, way * (far - slot), (1 - 2 * (turn % 2)) * way * (short - turn // 2)
        )

    def behind(self, steps):
        return self.device(-steps, self.core)

    def greet(self, partner=False, everyone=False):
        barrier = pltpu.get_barrier_semaphore()

        def signal(device):
            pl.semaphore_signal(barrier, inc=1, device_id=device, device_id_type=MESH_IDS)

        if everyone:

            def one(offset, carry):
                signal({"dp": (self.me + offset) % self.shards})
                return carry

            lax.fori_loop(1, self.shards, one, 0)
            expected = self.shards - 1
        else:
            for other in (self.following, self.previous, self.sibling):
                signal({"dp": other})
            expected = 3
        if partner:
            signal(partner_id())
            expected += 1
        pl.semaphore_wait(barrier, expected)


def send_to(device, source, target, send_sem, recv_sem):
    return pltpu.make_async_remote_copy(
        src_ref=source,
        dst_ref=target,
        send_sem=send_sem,
        recv_sem=recv_sem,
        device_id=device,
        device_id_type=MESH_IDS,
    )


def partner_id():
    return {"tensor": 1 - lax.axis_index("tensor")}


def turn_rows(source, target, low=0):
    def one(block, carry):
        here = pl.ds(pl.multiple_of(block * TILE, TILE), TILE)
        there = pl.ds(pl.multiple_of(low + block * TILE, TILE), TILE)
        target[:, there] = jnp.transpose(source[here, :].astype(jnp.float32)).astype(target.dtype)
        return carry

    lax.fori_loop(0, source.shape[0] // TILE, one, 0)


def gather_kernel(shards, *refs):
    (
        gains_ref,
        q_ref,
        k_ref,
        v_ref,
        out_ref,
        gate_ref,
        up_ref,
        down_ref,
        gains_all,
        qkv_all,
        out_all,
        same_shard,
        other_shard,
        qkv_own,
        out_load,
        out_own,
        down_load,
        ffn_own,
        ring_send,
        ring_recv,
        side_send,
        side_recv,
        own_sem,
        load_sem,
    ) = refs
    fulls = (qkv_all, out_all, gains_all)
    locals_ = (qkv_own, out_own, gains_ref)
    kinds = len(fulls)
    ring = Ring(shards)

    loads = []
    low = 0
    for index, ref in enumerate((q_ref, k_ref, v_ref)):
        size = ref.shape[1]
        loads.append(
            pltpu.make_async_copy(ref, qkv_own.at[:, pl.ds(low, size)], load_sem.at[index])
        )
        low += size
    loads.append(pltpu.make_async_copy(out_ref, out_load, load_sem.at[3]))
    loads.append(pltpu.make_async_copy(down_ref, down_load, load_sem.at[4]))
    part = gate_ref.shape[1] // 2
    sets = (ring.row % 2, 1 - ring.row % 2)
    for index, ref in enumerate((gate_ref, up_ref)):
        for which in range(2):
            source = ref.at[:, pl.ds(pl.multiple_of(sets[which] * part, 128), part)]
            target = ffn_own.at[which, :, pl.ds(index * part, part)]
            loads.append(
                pltpu.make_async_copy(source, target, load_sem.at[5 + 2 * index + which])
            )
    for load in loads:
        load.start()
    ring.greet()

    def ring_copy(step, kind, shard, source):
        return send_to(
            {"dp": ring.following},
            source,
            fulls[kind].at[shard],
            ring_send.at[step, kind],
            ring_recv.at[step, kind],
        )

    def side_copy(step, kind, shard, source):
        return send_to(
            {"dp": ring.sibling},
            source,
            fulls[kind].at[shard],
            side_send.at[step, kind],
            side_recv.at[step, kind],
        )

    def own_copy(kind):
        return pltpu.make_async_copy(locals_[kind], fulls[kind].at[ring.me], own_sem.at[kind])

    def begin(kind):
        ring_copy(0, kind, ring.me, locals_[kind]).start()
        side_copy(0, kind, ring.me, locals_[kind]).start()
        own_copy(kind).start()

    for load in loads[:3]:
        load.wait()
    begin(0)
    loads[3].wait()
    turn_rows(out_load, out_own)
    begin(2)
    begin(1)
    loads[4].wait()

    def turn_down(block, carry):
        for which in range(2):
            here = pl.ds(pl.multiple_of(sets[which] * part + block * 128, 128), 128)
            there = pl.ds(pl.multiple_of(2 * part + block * 128, 128), 128)
            piece = jnp.transpose(down_load[here, :].astype(jnp.float32))
            ffn_own[which, :, there] = piece.astype(jnp.bfloat16)
        return carry

    lax.fori_loop(0, part // 128, turn_down, 0)
    for load in loads[5:]:
        load.wait()
    ffn_stores = [
        pltpu.make_async_copy(ffn_own.at[which], target, load_sem.at[9 + which])
        for which, target in enumerate((same_shard, other_shard))
    ]

    def forward(step, carry):
        @pl.when(step == 2)
        def _():
            for store in ffn_stores:
                store.start()

        shard = ring.behind(step)
        for kind in (0, 2, 1):
            here = fulls[kind].at[shard]
            ring_copy(step - 1, kind, shard, here).wait_recv()

            @pl.when(step < ring.count - 1)
            def _():
                ring_copy(step, kind, shard, here).start()

            side_copy(step, kind, shard, here).start()
        return carry

    lax.fori_loop(1, ring.count, forward, 0)

    def drain(step, carry):
        shard = ring.behind(step)
        for kind in range(kinds):
            here = fulls[kind].at[shard]

            @pl.when(step < ring.count - 1)
            def _():
                ring_copy(step, kind, shard, here).wait_send()

            side_copy(step, kind, shard, here).wait_send()
            side_copy(step, kind, shard, here).wait_recv()
        return carry

    lax.fori_loop(0, ring.count, drain, 0)
    for store in ffn_stores:
        store.wait()
    for kind in range(kinds):
        own_copy(kind).wait()


def gather_shards(shards, gains, w_q, w_k, w_v, w_o, w_gate, w_up, w_down):
    steps = shards // 2
    rows = w_q.shape[0]
    columns = w_q.shape[1] + w_k.shape[1] + w_v.shape[1]
    sems = pltpu.SemaphoreType.DMA((steps, 3))
    half = jnp.bfloat16
    return pl.pallas_call(
        functools.partial(gather_kernel, shards),
        out_shape=(
            jax.ShapeDtypeStruct((shards,) + gains.shape, gains.dtype),
            jax.ShapeDtypeStruct((shards, rows, columns), half),
            jax.ShapeDtypeStruct((shards, rows, w_o.shape[0]), half),
            jax.ShapeDtypeStruct((rows, 3 * w_down.shape[0] // 2), half),
            jax.ShapeDtypeStruct((rows, 3 * w_down.shape[0] // 2), half),
        ),
        in_specs=[VMEM_SPEC] + [ANY_SPEC] * 7,
        out_specs=(ANY_SPEC,) * 5,
        scratch_shapes=[
            pltpu.VMEM((rows, columns), half),
            pltpu.VMEM(w_o.shape, half),
            pltpu.VMEM((rows, w_o.shape[0]), half),
            pltpu.VMEM(w_down.shape, half),
            pltpu.VMEM((2, rows, 3 * w_down.shape[0] // 2), half),
            sems,
            sems,
            sems,
            sems,
            pltpu.SemaphoreType.DMA((3,)),
            pltpu.SemaphoreType.DMA((11,)),
        ],
        compiler_params=pltpu.CompilerParams(
            collective_id=0, has_side_effects=True, vmem_limit_bytes=VMEM_BYTES
        ),
        name="gather_attention",
    )(gains, w_q, w_k, w_v, w_o, w_gate, w_up, w_down)


def turn_left(ring, left_all, target, shard):
    rows = left_all.shape[1] // ring.shards
    base = pl.multiple_of(shard * rows // 128 * 128, 128)
    block = left_all[:, pl.ds(base, 128)].astype(jnp.float32)
    target[...] = jnp.transpose(block).astype(jnp.bfloat16)


def shard_terms(turned, right_all, low, size, shard, rows):
    if rows % 128 == 0:
        left = turned[...]
    else:
        first = shard * rows % 128
        left = turned[pl.ds(pl.multiple_of(first, rows), rows), :]
    return matmul(left, right_all[:, low : low + size])


def cut_columns(pairs, widths, limit, least):
    chunks = []
    target = 0
    for left, right in pairs:
        width = widths[right]
        low = 0
        while low < width:
            size = min(limit, width - low)
            if width - low - size < least:
                size = width - low
            chunks.append((left, right, low, size, target))
            low += size
            target += size
    return tuple(chunks), target


FFN_PAIRS = ((1, 2), (0, 0), (0, 1))
HEAD_PAIRS = ((2, 3), (3, 4))


def ffn_chunks_of(units):
    return cut_columns(FFN_PAIRS, (units,) * 3, 768, 384)


def early_columns(chunks):
    return chunks[len(chunks) // 2][4]


def ffn_kernel(shards, groups, chunks, *refs):
    (
        x_ref,
        part_ref,
        gain_ref,
        grad_ref,
        same_ref,
        below_ref,
        above_ref,
        across_ref,
        hidden_ref,
        norm_part_ref,
        norm_other_ref,
        out_own_ref,
        out_pair_ref,
        partial_ref,
        sum_early_ref,
        sum_late_ref,
        normed_out,
        grad_out,
        d_gate_out,
        d_up_out,
        act_out,
    ) = refs[:21]
    count = len(groups)
    full = refs[21 : 21 + count]
    (
        part_other,
        out_total,
        norm_total,
        normed_all,
        grad_all,
        d_gate_all,
        d_up_all,
        act_all,
        turned,
        pair_send_buf,
        pair_recv_buf,
        across_send_buf,
        across_recv_buf,
        far_send,
        far_recv,
        across_send,
        across_recv,
        side_send,
        side_recv,
        own_sem,
        part_send,
        part_recv,
        load_sem,
        normed_send,
        normed_recv,
        pair_send,
        pair_recv,
        norm_send,
        norm_recv,
        left_sem,
        right_send,
        right_recv,
        sum_send,
        sum_recv,
        store_sem,
    ) = refs[21 + count :]
    tokens, depth = part_ref.shape
    rows, units = same_ref.shape
    units //= 3
    blocks = depth // TILE
    early = early_columns(chunks)
    ring = Ring(shards)
    line = ring.rows
    row, side = ring.row, ring.side
    pair = {"dp": ring.at(row + 1 - 2 * (row % 2), side)}
    across = {"dp": ring.at(row, 1 - side)}
    base = ring.core * (2 * tokens)
    mine = pl.ds(pl.multiple_of(base, 2 * tokens), 2 * tokens)
    has_far = (row + 2 < line, row >= 2)
    far = ({"dp": ring.at(row + 2, side)}, {"dp": ring.at(row - 2, side)})

    def half_rows(half):
        return pl.ds(pl.multiple_of(base + half * tokens, tokens), tokens)

    x_load = pltpu.make_async_copy(x_ref, hidden_ref, load_sem.at[0])
    grad_load = pltpu.make_async_copy(grad_ref, grad_all.at[half_rows(0)], load_sem.at[1])
    x_load.start()
    grad_load.start()
    barrier = pltpu.get_barrier_semaphore()

    def greet(device):
        pl.semaphore_signal(barrier, inc=1, device_id=device, device_id_type=MESH_IDS)

    for device in (pair, across, {"dp": ring.sibling}, partner_id()):
        greet(device)
    for way in range(2):

        @pl.when(has_far[way])
        def _():
            greet(far[way])

    pl.semaphore_wait(
        barrier, 4 + has_far[0].astype(jnp.int32) + has_far[1].astype(jnp.int32)
    )

    def place(group, kind, shard):
        return full[group].at[kind, pl.ds(pl.multiple_of(shard * rows, rows), rows)]

    def cut(ref, group, kind):
        low, size = groups[group]
        return ref.at[:, pl.ds(kind * units + low, size)]

    def far_copy(group, way, distance, kind, shard, source):
        return send_to(
            far[way],
            source,
            place(group, kind, shard),
            far_send.at[group, way, distance - 2, kind],
            far_recv.at[group, way, distance - 2, kind],
        )

    def across_copy(group, source_row, kind, shard, source):
        return send_to(
            across,
            source,
            place(group, kind, shard),
            across_send.at[group, source_row, kind],
            across_recv.at[group, source_row, kind],
        )

    def side_copy(group, index, kind, shard, source):
        return send_to(
            {"dp": ring.sibling},
            source,
            place(group, kind, shard),
            side_send.at[group, index, kind],
            side_recv.at[group, index, kind],
        )

    def own_copy(group, which, kind):
        source, shard = (
            (same_ref, ring.me),
            (below_ref, ring.at(row - 1, side)),
            (above_ref, ring.at(row + 1, side)),
            (across_ref, ring.at(row, 1 - side)),
        )[which]
        return pltpu.make_async_copy(
            cut(source, group, kind), place(group, kind, shard), own_sem.at[group, which, kind]
        )

    has_near = (row >= 1, row + 1 < line)

    def begin(group):
        for kind in range(3):
            source = cut(same_ref, group, kind)
            for way in range(2):

                @pl.when(has_far[way])
                def _():
                    far_copy(group, way, 2, kind, ring.me, source).start()

            own_copy(group, 0, kind).start()
            side_copy(group, row, kind, ring.me, source).start()
            for way, near in enumerate((below_ref, above_ref)):
                near_row = row - 1 + 2 * way
                shard = ring.at(near_row, side)

                @pl.when(has_near[way])
                def _():
                    here = cut(near, group, kind)

                    @pl.when(has_far[way])
                    def _():
                        far_copy(group, way, 3, kind, shard, here).start()

                    across_copy(group, near_row, kind, shard, here).start()
                    own_copy(group, 1 + way, kind).start()
                    side_copy(group, near_row, kind, shard, here).start()

            own_copy(group, 3, kind).start()
            side_copy(
                group, line + row, kind, ring.at(row, 1 - side), cut(across_ref, group, kind)
            ).start()

    events = 4 * (line - 1) - 2
    ticks = 3 * events

    def forward(group, tick):
        event = tick // 3 + 2
        kind = tick % 3
        distance = 1 + event // 4
        what = event % 4
        for way in range(2):
            source_row = row - distance * (1 - 2 * way)
            reachable = (source_row >= 0) & (source_row < line)

            @pl.when(reachable & (what == way))
            def _():
                shard = ring.at(source_row, side)
                here = place(group, kind, shard)
                far_copy(group, way, distance, kind, shard, here).wait_recv()

                @pl.when(has_far[way])
                def _():
                    far_copy(group, way, distance + 2, kind, shard, here).start()

                across_copy(group, source_row, kind, shard, here).start()
                side_copy(group, source_row, kind, shard, here).start()

            @pl.when(reachable & (what == 2 + way))
            def _():
                shard = ring.at(source_row, 1 - side)
                here = place(group, kind, shard)
                across_copy(group, source_row, kind, shard, here).wait_recv()
                side_copy(group, line + source_row, kind, shard, here).start()

        if group + 1 < count:

            @pl.when(tick == ticks - 12)
            def _():
                begin(group + 1)

    def arrived(group):
        for kind in range(3):
            for which in (0, 3):
                own_copy(group, which, kind).wait()
            for way in range(2):

                @pl.when(has_near[way])
                def _():
                    own_copy(group, 1 + way, kind).wait()

        def one(index, carry):
            for kind in range(3):
                here = place(group, kind, ring.me)
                side_copy(group, index, kind, ring.me, here).wait_recv()
            return carry

        lax.fori_loop(0, 2 * line, one, 0)

    def drain(group):
        def sides(index, carry):
            for kind in range(3):
                here = place(group, kind, ring.me)
                side_copy(group, index, kind, ring.me, here).wait_send()
            return carry

        def columns(source_row, carry):
            for kind in range(3):
                here = place(group, kind, ring.me)

                @pl.when(source_row != row)
                def _():
                    across_copy(group, source_row, kind, ring.me, here).wait_send()

            return carry

        def distances(distance, carry):
            reach = (row + 2, line + 1 - row)
            for way in range(2):

                @pl.when(has_far[way] & (distance <= reach[way]))
                def _():
                    for kind in range(3):
                        here = place(group, kind, ring.me)
                        far_copy(group, way, distance, kind, ring.me, here).wait_send()

            return carry

        lax.fori_loop(0, 2 * line, sides, 0)
        lax.fori_loop(0, line, columns, 0)
        lax.fori_loop(2, line, distances, 0)

    lefts = (normed_all, grad_all)
    rights = (d_gate_all, d_up_all, act_all)

    def left_copy(index):
        here = lefts[index].at[mine]
        return send_to(
            {"dp": ring.sibling}, here, here, left_sem.at[0, index], left_sem.at[1, index]
        )

    def right_copy(group, half, index):
        low, size = groups[group]
        here = rights[index].at[half_rows(half), pl.ds(low, size)]
        return send_to(
            {"dp": ring.sibling},
            here,
            here,
            right_send.at[group, half, index],
            right_recv.at[group, half, index],
        )

    def share_rights(group, half):
        for index in range(3):
            right_copy(group, half, index).start()

    def tile_of(group):
        return TILE if groups[group][1] % TILE == 0 else TILE // 2

    def hidden_units(group, tile, half):
        low, _ = groups[group]
        wide = tile_of(group)
        here = half_rows(half)
        part = pl.ds(pl.multiple_of(tile * wide, wide), wide)
        target = pl.ds(pl.multiple_of(low + tile * wide, 128), wide)
        gate_pre = matmul(normed_all[here, :], full[group][0, :, part])
        up_pre = matmul(normed_all[here, :], full[group][1, :, part])
        d_act = matmul(grad_all[here, :], full[group][2, :, part])
        sigmoid_gate = jax.nn.sigmoid(gate_pre)
        silu_gate = gate_pre * sigmoid_gate
        act_all[here, target] = (silu_gate * up_pre).astype(jnp.bfloat16)
        d_gate_all[here, target] = (
            d_act * up_pre * sigmoid_gate * (1.0 + gate_pre * (1.0 - sigmoid_gate))
        ).astype(jnp.bfloat16)
        d_up_all[here, target] = (d_act * silu_gate).astype(jnp.bfloat16)

    def feature_block(block):
        if isinstance(block, int):
            return slice(block * TILE, (block + 1) * TILE)
        return pl.ds(pl.multiple_of(block * TILE, TILE), TILE)

    def norm_terms(group, block, here):
        low, size = groups[group]
        cols = slice(low, low + size)
        features = feature_block(block)
        return matmul_nt(d_gate_all[here, cols], full[group][0, features, :]) + matmul_nt(
            d_up_all[here, cols], full[group][1, features, :]
        )

    def out_terms(group, block, here):
        low, size = groups[group]
        features = feature_block(block)
        return matmul_nt(act_all[here, low : low + size], full[group][2, features, :])

    def accumulate(group, block):
        features = feature_block(block)
        norm_new = norm_terms(group, block, half_rows(0))
        out_new = out_terms(group, block, half_rows(0))
        if group > 0:
            norm_new += norm_total[:, features]
            out_new += out_total[:, features]
        norm_total[:, features] = norm_new
        out_total[:, features] = out_new

    quarter = tokens // 4

    def part_copy(piece):
        here = pl.ds(piece * quarter, quarter)
        return send_to(
            partner_id(),
            part_ref.at[here],
            part_other.at[here],
            part_send.at[piece],
            part_recv.at[piece],
        )

    def normed_copy(piece):
        here = pl.ds(pl.multiple_of(base + piece * quarter, quarter), quarter)
        there = pl.ds(pl.multiple_of(base + tokens + piece * quarter, quarter), quarter)
        return send_to(
            pair,
            normed_all.at[here],
            normed_all.at[there],
            normed_send.at[piece],
            normed_recv.at[piece],
        )

    grad_copy = send_to(
        pair,
        grad_all.at[half_rows(0)],
        grad_all.at[half_rows(1)],
        load_sem.at[2],
        load_sem.at[3],
    )

    for piece in range(4):
        part_copy(piece).start()
    begin(0)
    x_load.wait()
    grad_load.wait()

    def norm_rows(piece):
        part_copy(piece).wait_recv()

        def one(block, carry):
            first = piece * quarter + block * 32
            here = pl.ds(pl.multiple_of(first, 32), 32)
            there = pl.ds(pl.multiple_of(base + first, 32), 32)
            hidden = hidden_ref[here, :] + (
                part_ref[here, :].astype(jnp.float32) + part_other[here, :].astype(jnp.float32)
            )
            hidden_ref[here, :] = hidden
            _, norm_two = rms_parts(hidden)
            normed_all[there, :] = (norm_two * gain_ref[...]).astype(jnp.bfloat16)
            return carry

        lax.fori_loop(0, quarter // 32, one, 0)

    pause = ticks // 4

    def first_ticks(tick, carry):
        forward(0, tick)
        for piece in range(4):

            @pl.when(tick == pause * (piece + 1))
            def _():
                norm_rows(piece)
                if piece > 0:
                    normed_copy(piece - 1).start()

        return carry

    grad_copy.start()
    lax.fori_loop(0, ticks, first_ticks, 0)
    arrived(0)
    normed_copy(3).start()

    first_tiles = groups[0][1] // tile_of(0)

    def wait_pair():
        for piece in range(4):
            normed_copy(piece).wait_recv()
        grad_copy.wait_recv()

    for group in range(1, count):
        before = group - 1
        tiles = groups[before][1] // tile_of(before)
        if group > 1:
            arrived(before)

        later = ticks - 10

        def tick_and_work(tick, carry):
            forward(group, tick)

            @pl.when(tick < tiles)
            def _():
                hidden_units(before, tick, 0)

            block = tick - tiles

            @pl.when(block == 0)
            def _():
                share_rights(before, 0)

            @pl.when((block >= 0) & (block < blocks))
            def _():
                accumulate(before, block)

            if group == count - 1:

                @pl.when(tick == later)
                def _():
                    wait_pair()

                @pl.when((tick >= later) & (tick < later + first_tiles))
                def _():
                    hidden_units(0, tick - later, 1)

            return carry

        lax.fori_loop(0, ticks, tick_and_work, 0)

    last = count - 1
    share_rights(0, 1)
    for index in range(2):
        left_copy(index).start()

    def loop_units(group, half):
        def one(tile, carry):
            hidden_units(group, tile, half)
            return carry

        lax.fori_loop(0, groups[group][1] // tile_of(group), one, 0)
        share_rights(group, half)

    for group in range(1, last):
        loop_units(group, 1)
    arrived(last)
    loop_units(last, 1)

    def pair_copy(block):
        features = pl.ds(pl.multiple_of(block * TILE, TILE), TILE)
        return send_to(
            pair,
            pair_send_buf.at[:, features],
            pair_recv_buf.at[:, features],
            pair_send.at[block],
            pair_recv.at[block],
        )

    def pair_norm(block, carry):
        features = feature_block(block)
        total = norm_terms(0, block, half_rows(1))
        for group in range(1, count):
            total += norm_terms(group, block, half_rows(1))
        pair_send_buf[:, features] = total.astype(jnp.bfloat16)

        @pl.when(block > 0)
        def _():
            pair_copy(block - 1).start()

        return carry

    lax.fori_loop(0, blocks, pair_norm, 0)
    loop_units(last, 0)
    pair_copy(blocks - 1).start()

    def norm_copy(block):
        features = pl.ds(block * TILE, TILE)
        return send_to(
            partner_id(),
            norm_part_ref.at[:, features],
            norm_other_ref.at[:, features],
            norm_send.at[block],
            norm_recv.at[block],
        )

    def turn(shard):
        for index in range(2):
            turn_left(ring, lefts[index], turned.at[index], shard)

    def terms(chunk, shard):
        left, right, low, size, _ = chunks[chunk]
        return shard_terms(turned.at[left], rights[right], low, size, shard, rows)

    def sum_copy(chunk):
        _, _, _, size, target = chunks[chunk]
        columns = pl.ds(target, size)
        return send_to(
            across,
            across_send_buf.at[:, columns],
            across_recv_buf.at[:, columns],
            sum_send.at[chunk],
            sum_recv.at[chunk],
        )

    for index in range(2):
        left_copy(index).wait_recv()
    for group in range(count):
        for half in range(2):
            for index in range(3):
                right_copy(group, half, index).wait_recv()
    outs = (normed_out, grad_out, d_gate_out, d_up_out, act_out)
    stores = [
        pltpu.make_async_copy(source, target, store_sem.at[index])
        for index, (source, target) in enumerate(zip(lefts + rights, outs))
    ]
    for store in stores:
        store.start()

    first_owner = row + ring.owner(0)
    second_owner = row + ring.owner(1)
    shard = ring.at(first_owner, 1 - side)
    turn(shard)
    for block in range(max(blocks, len(chunks))):
        if block < len(chunks):
            _, _, _, size, target = chunks[block]
            across_send_buf[:, target : target + size] = terms(block, shard).astype(jnp.bfloat16)
            if block > 0:
                sum_copy(block - 1).start()
        if block < blocks:
            features = feature_block(block)
            total = norm_total[0:tokens, features] + norm_terms(last, block, half_rows(0))
            pair_copy(block).wait_recv()
            total += pair_recv_buf[:, features].astype(jnp.float32)
            norm_part_ref[:, features] = total.astype(jnp.bfloat16)
            if block > 0:
                norm_copy(block - 1).start()
    sum_copy(len(chunks) - 1).start()

    def last_out(block, carry):
        features = feature_block(block)
        total = out_total[:, features] + out_terms(last, block, half_rows(0))
        out_own_ref[:, features] = total.astype(jnp.bfloat16)
        total = out_terms(0, block, half_rows(1))
        for group in range(1, count):
            total += out_terms(group, block, half_rows(1))
        out_pair_ref[:, features] = total.astype(jnp.bfloat16)
        return carry

    lax.fori_loop(0, blocks, last_out, 0)
    norm_copy(blocks - 1).start()
    shard = ring.at(second_owner, 1 - side)
    turn(shard)
    for chunk in range(len(chunks)):
        _, _, _, size, target = chunks[chunk]
        partial_ref[:, target : target + size] = terms(chunk, shard).astype(jnp.bfloat16)
    shard = ring.at(first_owner, side)
    turn(shard)
    for chunk in range(len(chunks)):
        _, _, _, size, target = chunks[chunk]
        total = terms(chunk, shard)
        sum_copy(chunk).wait_recv()
        total += across_recv_buf[:, target : target + size].astype(jnp.float32)
        if target < early:
            sum_early_ref[:, target : target + size] = total.astype(jnp.bfloat16)
        else:
            at = target - early
            sum_late_ref[:, at : at + size] = total.astype(jnp.bfloat16)

    for group in range(count):
        drain(group)
    for piece in range(4):
        part_copy(piece).wait_send()
        normed_copy(piece).wait_send()
    grad_copy.wait_send()
    for index in range(2):
        left_copy(index).wait_send()
    for group in range(count):
        for half in range(2):
            for index in range(3):
                right_copy(group, half, index).wait_send()
    for chunk in range(len(chunks)):
        sum_copy(chunk).wait_send()
    for block in range(blocks):
        pair_copy(block).wait_send()
    for store in stores:
        store.wait()
    for block in range(blocks):
        norm_copy(block).wait()


def ffn_groups(units):
    tiles = units // 128
    last = 2
    second = (tiles - last) // 4 * 2
    sizes = [tiles - last - second, second, last]
    groups = []
    low = 0
    for size in sizes:
        groups.append((low * 128, size * 128))
        low += size
    return tuple(groups)


def ffn_pass(shards, x_rows, part, gain, grad_rows, pieces):
    tokens, depth = x_rows.shape
    rows, units = pieces[0].shape
    units //= 3
    line = shards // 4
    groups = ffn_groups(units)
    chunks, total = ffn_chunks_of(units)
    half = jnp.bfloat16
    dma = pltpu.SemaphoreType.DMA
    wide = jax.ShapeDtypeStruct((tokens, depth), half)
    all_wide = (4 * tokens, depth)
    all_inner = (4 * tokens, units)
    blocks = depth // TILE
    full = [pltpu.VMEM((3, depth, size), half) for _, size in groups]
    return pl.pallas_call(
        functools.partial(ffn_kernel, shards, groups, chunks),
        out_shape=(
            jax.ShapeDtypeStruct((tokens, depth), jnp.float32),
            wide,
            wide,
            wide,
            wide,
            jax.ShapeDtypeStruct((rows, total), half),
            jax.ShapeDtypeStruct((rows, early_columns(chunks)), half),
            jax.ShapeDtypeStruct((rows, total - early_columns(chunks)), half),
            jax.ShapeDtypeStruct(all_wide, half),
            jax.ShapeDtypeStruct(all_wide, half),
            jax.ShapeDtypeStruct(all_inner, half),
            jax.ShapeDtypeStruct(all_inner, half),
            jax.ShapeDtypeStruct(all_inner, half),
        ),
        in_specs=[ANY_SPEC, VMEM_SPEC, VMEM_SPEC] + [ANY_SPEC] * 5,
        out_specs=(VMEM_SPEC,) * 8 + (ANY_SPEC,) * 5,
        scratch_shapes=full
        + [
            pltpu.VMEM((tokens, depth), half),
            pltpu.VMEM((tokens, depth), jnp.float32),
            pltpu.VMEM((tokens, depth), jnp.float32),
            pltpu.VMEM(all_wide, half),
            pltpu.VMEM(all_wide, half),
            pltpu.VMEM(all_inner, half),
            pltpu.VMEM(all_inner, half),
            pltpu.VMEM(all_inner, half),
            pltpu.VMEM((2, 128, 4 * tokens), half),
            pltpu.VMEM((tokens, depth), half),
            pltpu.VMEM((tokens, depth), half),
            pltpu.VMEM((rows, total), half),
            pltpu.VMEM((rows, total), half),
            dma((len(groups), 2, line - 2, 3)),
            dma((len(groups), 2, line - 2, 3)),
            dma((len(groups), line, 3)),
            dma((len(groups), line, 3)),
            dma((len(groups), 2 * line, 3)),
            dma((len(groups), 2 * line, 3)),
            dma((len(groups), 4, 3)),
            dma((4,)),
            dma((4,)),
            dma((4,)),
            dma((4,)),
            dma((4,)),
            dma((blocks,)),
            dma((blocks,)),
            dma((blocks,)),
            dma((blocks,)),
            dma((2, 2)),
            dma((len(groups), 2, 3)),
            dma((len(groups), 2, 3)),
            dma((len(chunks),)),
            dma((len(chunks),)),
            dma((5,)),
        ],
        compiler_params=pltpu.CompilerParams(
            collective_id=1, has_side_effects=True, vmem_limit_bytes=VMEM_BYTES
        ),
        name="ffn_pairs",
    )(x_rows, part, gain, grad_rows, *pieces)


def reduce_kernel(shards, ffn_chunks, head_chunks, *refs):
    (
        normed_two_ref,
        grad_ref,
        hidden_rows_ref,
        normed_one_ref,
        d_gate_ref,
        d_up_ref,
        act_ref,
        attended_ref,
        d_qkv_ref,
        across_ref,
        sum_ref,
        up_ref,
        down_ref,
        out_part_ref,
        out_pair_ref,
        norm_part_ref,
        hidden_ref,
        d_hidden_ref,
        scaled_ref,
        inv_ref,
        gain_ref,
        sums_ref,
        layer_out,
        x_grad_out,
        gate_grad,
        up_grad,
        down_grad,
        o_grad,
        qkv_grad,
        sums_out,
        normed_two_all,
        grad_all,
        hidden_rows_all,
        normed_one_all,
        d_gate_all,
        d_up_all,
        act_all,
        attended_all,
        d_qkv_all,
        ffn_turned,
        head_turned,
        total_buf,
        partials,
        across_in,
        ffn_sums,
        relay,
        other_in,
        head_slots,
        norm_here,
        norm_there,
        out_here,
        out_pair,
        out_there,
        hidden_buf,
        d_hidden_buf,
        scaled_buf,
        column_total,
        sums_own,
        sums_in,
        across_send,
        across_recv,
        sum_send,
        relay_recv,
        other_recv,
        head_send,
        head_recv,
        load_sem,
        side_send,
        side_recv,
        part_sem,
        row_sem,
        sums_send,
        sums_recv,
    ) = refs
    ring = Ring(shards)
    line = ring.rows
    row, side = ring.row, ring.side
    tokens, depth = out_part_ref.shape
    rows = head_slots.shape[1]
    mine = pl.ds(pl.multiple_of(ring.core * tokens, tokens), tokens)
    rights = (d_gate_all, d_up_all, act_all, attended_all, d_qkv_all)
    heads = len(head_chunks)
    ffns = len(ffn_chunks)
    early = early_columns(ffn_chunks)

    head_pairs = (
        (hidden_rows_ref, hidden_rows_all),
        (attended_ref, attended_all),
        (normed_one_ref, normed_one_all),
        (d_qkv_ref, d_qkv_all),
    )
    head_loads = [
        pltpu.make_async_copy(source, target.at[mine], load_sem.at[index])
        for index, (source, target) in enumerate(head_pairs)
    ]
    ffn_loads = [
        pltpu.make_async_copy(source, target, load_sem.at[4 + index])
        for index, (source, target) in enumerate(
            (
                (sum_ref, ffn_sums.at[0, :, pl.ds(early, sum_ref.shape[1])]),
                (grad_ref, grad_all),
                (act_ref, act_all),
                (normed_two_ref, normed_two_all),
                (d_gate_ref, d_gate_all),
                (d_up_ref, d_up_all),
                (across_ref, across_in.at[0]),
            )
        )
    ]
    row_loads = [
        pltpu.make_async_copy(source, target, row_sem.at[index])
        for index, (source, target) in enumerate(
            (
                (norm_part_ref, norm_here),
                (d_hidden_ref, d_hidden_buf),
                (scaled_ref, scaled_buf),
                (out_part_ref, out_here),
                (hidden_ref, hidden_buf),
            )
        )
    ]
    half_line = line // 2
    preloaded = (
        (row >= 2) & (row - 2 < half_line),
        (row + 2 < line) & (row + 2 >= half_line),
    )
    early_at = (line - 1 - row, row)
    early_loads = [
        pltpu.make_async_copy(
            source,
            relay.at[way, jnp.minimum(early_at[way], line - 3), :, pl.ds(0, early)],
            load_sem.at[11 + way],
        )
        for way, source in enumerate((up_ref, down_ref))
    ]
    for load in head_loads + ffn_loads[:1]:
        load.start()
    for way in range(2):

        @pl.when(preloaded[way])
        def _():
            early_loads[way].start()

    for load in ffn_loads[1:] + row_loads:
        load.start()
    ring.greet(partner=True, everyone=True)
    sides = [
        send_to(
            {"dp": ring.sibling}, source, target.at[mine], side_send.at[index], side_recv.at[index]
        )
        for index, (source, target) in enumerate(head_pairs)
    ]
    for copy in sides:
        copy.start()
    norm_copy = send_to(partner_id(), norm_part_ref, norm_there, part_sem.at[0], part_sem.at[1])
    out_copy = send_to(partner_id(), out_here, out_there, part_sem.at[2], part_sem.at[3])
    pair_copy = send_to(
        {"dp": ring.at(row + 1 - 2 * (row % 2), side)},
        out_pair_ref,
        out_pair,
        part_sem.at[4],
        part_sem.at[5],
    )
    norm_copy.start()

    def columns_of(chunk):
        _, _, _, size, target = ffn_chunks[chunk]
        return pl.ds(target, size)

    def across_copy(slot, chunk):
        columns = columns_of(chunk)
        return send_to(
            {"dp": ring.at(row, 1 - side)},
            partials.at[slot % 2, :, columns],
            across_in.at[slot - 1, :, columns],
            across_send.at[slot, chunk],
            across_recv.at[slot, chunk],
        )

    def near_copy(slot, way, chunk):
        columns = columns_of(chunk)
        return send_to(
            {"dp": ring.at(row + 1 - 2 * way, side)},
            ffn_sums.at[slot, :, columns],
            other_in.at[way, :, columns],
            sum_send.at[slot, chunk],
            other_recv.at[way, chunk],
        )

    def far_copy(slot, way, distance, chunk):
        columns = columns_of(chunk)
        return send_to(
            {"dp": ring.at(row + 2 - 4 * way, side)},
            ffn_sums.at[slot, :, columns],
            relay.at[way, distance, :, columns],
            sum_send.at[slot, chunk],
            relay_recv.at[way, distance, chunk],
        )

    def send_sum(slot, chunk):
        offset = ring.owner(slot)
        for way in range(2):
            distance = offset * (1 - 2 * way)

            @pl.when(distance == 1)
            def _():
                near_copy(slot, way, chunk).start()

            @pl.when(distance >= 2)
            def _():
                far_copy(slot, way, distance - 2, chunk).start()

    def head_copy(step, chunk):
        _, _, _, size, target = head_chunks[chunk]
        columns = pl.ds(target, size)
        return send_to(
            {"dp": ring.following},
            head_slots.at[step, :, columns],
            head_slots.at[step + 1, :, columns],
            head_send.at[step, chunk],
            head_recv.at[step, chunk],
        )

    def turn_ffn(shard):
        turn_left(ring, normed_two_all, ffn_turned.at[0], shard)
        turn_left(ring, grad_all, ffn_turned.at[1], shard)

    def turn_head(chip):
        shard = 2 * chip + ring.core
        turn_left(ring, hidden_rows_all, head_turned.at[0], shard)
        turn_left(ring, normed_one_all, head_turned.at[1], shard)

    def head_terms(chunk, chip):
        left, right, low, size, _ = head_chunks[chunk]
        shard = 2 * chip + ring.core
        return shard_terms(head_turned.at[left - 2], rights[right], low, size, shard, rows)

    def ffn_terms(chunk, shard):
        left, right, low, size, _ = ffn_chunks[chunk]
        return shard_terms(ffn_turned.at[left], rights[right], low, size, shard, rows)

    def sums_copy(offset):
        return send_to(
            {"dp": (ring.me + offset) % shards},
            sums_own.at[(ring.me + offset) % shards],
            sums_in.at[ring.me],
            sums_send.at[offset],
            sums_recv.at[offset],
        )

    def finish_input_grad():
        for load in row_loads[:3]:
            load.wait()
        norm_copy.wait()
        sums_own[...] = sums_ref[...]
        column_total[...] = jnp.zeros_like(column_total)

        def one(block, carry):
            here = pl.ds(pl.multiple_of(block * 16, 16), 16)
            total = norm_here[here, :].astype(jnp.float32) + norm_there[here, :].astype(
                jnp.float32
            )
            scaled = scaled_buf[here, :]
            product = total * scaled
            column_total[...] += product[0:8] + product[8:16]
            scaled_gain = total * gain_ref[...]
            mean = jnp.mean(scaled_gain * scaled, axis=-1, keepdims=True)
            d_hidden_buf[here, :] = d_hidden_buf[here, :] + inv_ref[here, :] * (
                scaled_gain - scaled * mean
            )
            return carry

        lax.fori_loop(0, tokens // 16, one, 0)
        width = depth // shards
        band = max(width, 128)
        for low in range(0, depth, band):
            sums = jnp.sum(column_total[:, low : low + band], axis=0, keepdims=True)
            for inner in range(0, band, width):
                sums_own[(low + inner) // width, 1:2, 0:width] = sums[:, inner : inner + width]

    def send_sums():
        pltpu.make_async_copy(d_hidden_buf, x_grad_out, row_sem.at[5]).start()

        def one(offset, carry):
            sums_copy(offset).start()
            return carry

        lax.fori_loop(1, shards, one, 0)

    def join_pair():
        row_loads[3].wait()
        pair_copy.wait_recv()

        def one(block, carry):
            here = pl.ds(pl.multiple_of(block * 16, 16), 16)
            total = out_here[here, :].astype(jnp.float32) + out_pair[here, :].astype(jnp.float32)
            out_here[here, :] = total.astype(jnp.bfloat16)
            return carry

        lax.fori_loop(0, tokens // 16, one, 0)

    def finish_output():
        row_loads[4].wait()
        out_copy.wait_recv()

        def one(block, carry):
            here = pl.ds(pl.multiple_of(block * 16, 16), 16)
            hidden_buf[here, :] = hidden_buf[here, :] + (
                out_here[here, :].astype(jnp.float32) + out_there[here, :].astype(jnp.float32)
            )
            return carry

        lax.fori_loop(0, tokens // 16, one, 0)

    def head_total(step, chip, chunk):
        _, _, _, size, target = head_chunks[chunk]
        total = head_terms(chunk, chip)
        head_copy(step - 1, chunk).wait_recv()
        return total + head_slots[step, :, target : target + size].astype(jnp.float32)

    def head_step(step, chip):
        for chunk in range(heads):
            _, _, _, size, target = head_chunks[chunk]
            head_slots[step, :, target : target + size] = head_total(step, chip, chunk).astype(
                jnp.bfloat16
            )
            if chunk > 0:
                head_copy(step, chunk - 1).start()

    def head_end(step):
        head_copy(step, heads - 1).start()

    def send_partials(slot):
        shard = ring.at(row + ring.owner(slot), 1 - side)
        turn_ffn(shard)
        for chunk in range(ffns):
            _, _, _, size, target = ffn_chunks[chunk]

            @pl.when(slot >= 4)
            def _():
                across_copy(slot - 2, chunk).wait_send()

            partials[slot % 2, :, target : target + size] = ffn_terms(chunk, shard).astype(
                jnp.bfloat16
            )
            if chunk > 0:
                across_copy(slot, chunk - 1).start()

        @pl.when(slot == 2)
        def _():
            pair_copy.start()

    def sum_up(slot, chunk, shard, offset):
        _, _, _, size, target = ffn_chunks[chunk]
        total = ffn_terms(chunk, shard)

        @pl.when(slot >= 2)
        def _():
            across_copy(slot, chunk).wait_recv()

        total_buf[:, 0:size] = total + across_in[slot - 1, :, target : target + size].astype(
            jnp.float32
        )
        for way in range(2):
            distance = offset * (1 - 2 * way)
            source_row = row - 2 + 4 * way

            @pl.when((distance >= 0) & (source_row >= 0) & (source_row < line))
            def _():
                if target < early:

                    @pl.when(jnp.logical_not(preloaded[way] & (distance == early_at[way])))
                    def _():
                        far_copy(0, way, distance, chunk).wait_recv()

                else:
                    far_copy(0, way, distance, chunk).wait_recv()
                total_buf[:, 0:size] += relay[way, distance, :, target : target + size].astype(
                    jnp.float32
                )

    grads = (gate_grad, up_grad, down_grad)
    part = down_grad.shape[0] // 2

    def store_final(chunk, which):
        _, right, low, size, _ = ffn_chunks[chunk]
        first = pl.multiple_of(which * part + low, 128)
        if right == 2:
            down_grad[pl.ds(first, size), :] = jnp.transpose(total_buf[:, 0:size])
        else:
            grads[right][:, pl.ds(first, size)] = total_buf[:, 0:size]

    ffn_loads[0].wait()
    for chunk in range(ffns):
        if ffn_chunks[chunk][4] >= early:
            send_sum(0, chunk)
    for load in head_loads:
        load.wait()
    for copy in sides:
        copy.wait_recv()
    chip = ring.chip(-1)
    turn_head(chip)
    for chunk in range(heads):
        _, _, _, size, target = head_chunks[chunk]
        head_slots[0, :, target : target + size] = head_terms(chunk, chip).astype(jnp.bfloat16)
        if chunk > 0:
            head_copy(0, chunk - 1).start()
    for load in ffn_loads[1:]:
        load.wait()
    for way in range(2):

        @pl.when(preloaded[way])
        def _():
            early_loads[way].wait()

    def one_slot(slot, carry):
        send_partials(slot + 1)

        @pl.when(slot == 1)
        def _():
            head_end(0)

        offset = ring.owner(slot)
        shard = ring.at(row + offset, side)
        turn_ffn(shard)
        across_copy(slot + 1, ffns - 1).start()
        for chunk in range(ffns):
            _, _, _, size, target = ffn_chunks[chunk]
            sum_up(slot, chunk, shard, offset)
            ffn_sums[slot, :, target : target + size] = total_buf[:, 0:size].astype(jnp.bfloat16)
            if chunk > 0:
                send_sum(slot, chunk - 1)
        chip = ring.chip(-2 * slot)
        turn_head(chip)
        send_sum(slot, ffns - 1)
        head_step(2 * slot - 1, chip)
        chip = ring.chip(-1 - 2 * slot)
        turn_head(chip)
        head_end(2 * slot - 1)
        head_step(2 * slot, chip)

        @pl.when(slot == 1)
        def _():
            finish_input_grad()

        head_end(2 * slot)

        @pl.when(slot == 2)
        def _():
            send_sums()
            join_pair()

        return carry

    own = line - 1
    lax.fori_loop(1, own, one_slot, 0)
    out_copy.start()
    final = ring.count - 1
    chip = ring.chip(1 - final)
    turn_head(chip)
    head_step(final - 2, chip)
    shard = ring.at(row, side)
    turn_ffn(shard)
    head_end(final - 2)
    for chunk in range(ffns):
        sum_up(own, chunk, shard, 0)
        store_final(chunk, row % 2)
    chip = ring.chip(-final)
    turn_head(chip)
    head_step(final - 1, chip)
    chip = ring.chip(0)
    turn_head(chip)
    head_end(final - 1)
    finish_output()
    pltpu.make_async_copy(hidden_buf, layer_out, row_sem.at[6]).start()
    for chunk in range(ffns):
        _, _, _, size, target = ffn_chunks[chunk]
        total_buf[...] = jnp.zeros_like(total_buf)
        for way in range(2):
            source_row = row - 1 + 2 * way

            @pl.when((source_row >= 0) & (source_row < line))
            def _():
                near_copy(0, way, chunk).wait_recv()
                total_buf[:, 0:size] += other_in[way, :, target : target + size].astype(
                    jnp.float32
                )

        store_final(chunk, 1 - row % 2)
    for chunk in range(heads):
        _, right, low, size, _ = head_chunks[chunk]
        total = head_total(final, chip, chunk)
        if right == 3:
            o_grad[low : low + size, :] = jnp.transpose(total)
        else:
            qkv_grad[:, low : low + size] = total

    def add_sums(offset, total):
        sums_copy(offset).wait_recv()
        return total + sums_in[(ring.me - offset + shards) % shards]

    sums_out[...] = lax.fori_loop(1, shards, add_sums, sums_own[ring.me])

    def drain_heads(step, carry):
        for chunk in range(heads):
            head_copy(step, chunk).wait_send()
        return carry

    def drain_sums(offset, carry):
        sums_copy(offset).wait_send()
        return carry

    def drain_slots(slot, carry):
        for chunk in range(ffns):
            near_copy(slot, 0, chunk).wait_send()
        return carry

    lax.fori_loop(0, final, drain_heads, 0)
    lax.fori_loop(1, shards, drain_sums, 0)
    lax.fori_loop(1, own, drain_slots, 0)
    for chunk in range(ffns):
        if ffn_chunks[chunk][4] >= early:
            near_copy(0, 0, chunk).wait_send()
        for slot in range(max(2, line - 2), line):
            across_copy(slot, chunk).wait_send()
    for copy in sides:
        copy.wait_send()
    pair_copy.wait_send()
    out_copy.wait_send()
    pltpu.make_async_copy(d_hidden_buf, x_grad_out, row_sem.at[5]).wait()
    pltpu.make_async_copy(hidden_buf, layer_out, row_sem.at[6]).wait()


def reduce_pass(shards, both, heads, travelled, out_part, out_pair, norm_part, rows_f32, inv, gain, sums):
    normed_two, grad_rows, d_gate, d_up, activated = both
    hidden_rows, normed_one, attended, d_qkv = heads
    tokens, depth = out_part.shape
    units = d_gate.shape[1]
    line = shards // 4
    steps = shards // 2
    rows = depth // shards
    widths = (units, units, units, attended.shape[1], d_qkv.shape[1])
    ffn_chunks, ffn_total = ffn_chunks_of(units)
    head_chunks, head_total = cut_columns(HEAD_PAIRS, widths, 1024, 512)
    half = jnp.bfloat16
    wide = jax.ShapeDtypeStruct((tokens, depth), jnp.float32)
    one_half = pltpu.VMEM((tokens, depth), half)
    one_full = pltpu.VMEM((tokens, depth), jnp.float32)
    dma = pltpu.SemaphoreType.DMA
    ffns, heads_count = len(ffn_chunks), len(head_chunks)
    return pl.pallas_call(
        functools.partial(reduce_kernel, shards, ffn_chunks, head_chunks),
        out_shape=(
            wide,
            wide,
            jax.ShapeDtypeStruct((rows, 2 * units), jnp.float32),
            jax.ShapeDtypeStruct((rows, 2 * units), jnp.float32),
            jax.ShapeDtypeStruct((2 * units, rows), jnp.float32),
            jax.ShapeDtypeStruct((attended.shape[1], rows), jnp.float32),
            jax.ShapeDtypeStruct((rows, d_qkv.shape[1]), jnp.float32),
            jax.ShapeDtypeStruct(sums.shape[1:], jnp.float32),
        ),
        in_specs=[ANY_SPEC] * 19 + [VMEM_SPEC] * 3,
        out_specs=(ANY_SPEC, ANY_SPEC) + (VMEM_SPEC,) * 6,
        scratch_shapes=[pltpu.VMEM((4 * tokens, depth), half)] * 2
        + [pltpu.VMEM((2 * tokens, depth), half)] * 2
        + [pltpu.VMEM((4 * tokens, units), half)] * 3
        + [pltpu.VMEM((2 * tokens, width), half) for width in widths[3:]]
        + [
            pltpu.VMEM((2, 128, 4 * tokens), half),
            pltpu.VMEM((2, 128, 2 * tokens), half),
            pltpu.VMEM((rows, max(chunk[3] for chunk in ffn_chunks)), jnp.float32),
            pltpu.VMEM((2, rows, ffn_total), half),
            pltpu.VMEM((line - 1, rows, ffn_total), half),
            pltpu.VMEM((line - 1, rows, ffn_total), half),
            pltpu.VMEM((2, line - 2, rows, ffn_total), half),
            pltpu.VMEM((2, rows, ffn_total), half),
            pltpu.VMEM((steps, rows, head_total), half),
            one_half,
            one_half,
            one_half,
            one_half,
            one_half,
            one_full,
            one_full,
            one_full,
            pltpu.VMEM((8, depth), jnp.float32),
            pltpu.VMEM(sums.shape, jnp.float32),
            pltpu.VMEM(sums.shape, jnp.float32),
            dma((line, ffns)),
            dma((line, ffns)),
            dma((line, ffns)),
            dma((2, line - 2, ffns)),
            dma((2, ffns)),
            dma((steps - 1, heads_count)),
            dma((steps - 1, heads_count)),
            dma((13,)),
            dma((4,)),
            dma((4,)),
            dma((6,)),
            dma((7,)),
            dma((shards,)),
            dma((shards,)),
        ],
        compiler_params=pltpu.CompilerParams(
            collective_id=2, has_side_effects=True, vmem_limit_bytes=VMEM_BYTES
        ),
        name="reduce_pairs",
    )(
        normed_two,
        grad_rows,
        hidden_rows,
        normed_one,
        d_gate,
        d_up,
        activated,
        attended,
        d_qkv,
        *travelled,
        out_part,
        out_pair,
        norm_part,
        *rows_f32,
        inv,
        gain,
        sums,
    )


def emit_kernel(cuts, *refs):
    ins = refs[: len(cuts)]
    count = sum(len(cut) for cut in cuts)
    outs = refs[len(cuts) : len(cuts) + count]
    sums_ref, sums_one, sums_two = refs[len(cuts) + count : len(cuts) + count + 3]
    bufs = refs[len(cuts) + count + 3 : -2]
    load_sem, store_sem = refs[-2:]
    loads = [
        pltpu.make_async_copy(source, buf, load_sem.at[index])
        for index, (source, buf) in enumerate(zip(ins, bufs))
    ]
    for load in loads:
        load.start()
    stores = []
    for index, cut in enumerate(cuts):
        loads[index].wait()
        for low, size in cut:
            at = len(stores)
            source = bufs[index] if len(cut) == 1 else bufs[index].at[:, pl.ds(low, size)]
            stores.append(pltpu.make_async_copy(source, outs[at], store_sem.at[at]))
            stores[-1].start()
    sums_one[...] = sums_ref[1, : sums_one.shape[0]]
    sums_two[...] = sums_ref[0, : sums_two.shape[0]]
    for store in stores:
        store.wait()


def emit(arrays, cuts, sums, rows):
    outs = []
    for array, cut in zip(arrays, cuts):
        for _, size in cut:
            outs.append(jax.ShapeDtypeStruct((array.shape[0], size), array.dtype))
    count = len(outs)
    line = jax.ShapeDtypeStruct((rows,), jnp.float32)

    def kernel(*refs):
        ins = refs[: len(arrays)]
        sums_ref = refs[len(arrays)]
        rest = refs[len(arrays) + 1 :]
        emit_kernel(
            cuts, *ins, *rest[:count], sums_ref, rest[count], rest[count + 1], *rest[count + 2 :]
        )

    return pl.pallas_call(
        kernel,
        out_shape=tuple(outs) + (line, line),
        in_specs=[ANY_SPEC] * len(arrays) + [VMEM_SPEC],
        out_specs=(ANY_SPEC,) * count + (VMEM_SPEC, VMEM_SPEC),
        scratch_shapes=[pltpu.VMEM(array.shape, array.dtype) for array in arrays]
        + [pltpu.SemaphoreType.DMA((len(arrays),)), pltpu.SemaphoreType.DMA((count,))],
        compiler_params=pltpu.CompilerParams(vmem_limit_bytes=VMEM_BYTES),
        name="emit_results",
    )(*arrays, sums)


def device_pairs(shards, move):
    line = shards // 4
    pairs = []
    for shard in range(shards):
        chip, core = divmod(shard, 2)
        target = move(*divmod(chip, 2))
        if target is not None and 0 <= target[0] < line:
            pairs.append((shard, (2 * target[0] + target[1]) * 2 + core))
    return pairs


def body(
    shards,
    layer_input,
    positions,
    norm1_gain,
    w_q,
    w_k,
    w_v,
    w_o,
    norm2_gain,
    w_gate,
    w_up,
    w_down,
    out_grad,
):
    tokens, depth = layer_input.shape
    rows = w_q.shape[0]
    head_count = w_q.shape[1] // HD
    kv_count = w_k.shape[1] // HD
    query_cols = head_count * HD
    kv_cols = kv_count * HD

    def hop(value, move):
        return lax.ppermute(value, "dp", device_pairs(shards, move))

    half_line = shards // 8

    gains = jnp.stack([norm1_gain, norm2_gain]).astype(jnp.float32)
    gains = jnp.pad(gains, ((0, 6), (0, max(128 - rows, 0))))
    gains_all, qkv_all, out_all, same, other = gather_shards(
        shards, gains, w_q, w_k, w_v, w_o, w_gate, w_up, w_down
    )
    gain_one = gains_all[:, 0, :rows].reshape(1, depth)
    gain_two = gains_all[:, 1, :rows].reshape(1, depth)
    qkv_w = qkv_all.reshape(depth, query_cols + 2 * kv_cols)
    out_w = out_all.reshape(depth, query_cols)
    below = hop(other, lambda row, side: (row + 1, side))
    above = hop(other, lambda row, side: (row - 1, side))
    across = hop(same, lambda row, side: (row, 1 - side))

    inv_one, norm_one = rms_parts(layer_input)
    normed_one = (norm_one * gain_one).astype(jnp.bfloat16)
    cos_table, sin_table = rope_tables(positions, HD)
    qkv = matmul(normed_one, qkv_w)
    queries = rotate(
        qkv[:, :query_cols].reshape(tokens, head_count, HD), cos_table, sin_table, 1.0
    ).astype(jnp.bfloat16)
    key_rows = rotate(
        qkv[:, query_cols : query_cols + kv_cols].reshape(tokens, kv_count, HD),
        cos_table,
        sin_table,
        1.0,
    ).astype(jnp.bfloat16)
    value_rows = qkv[:, query_cols + kv_cols :].astype(jnp.bfloat16).reshape(tokens, kv_count, HD)
    seq_count = tokens // L
    query_seq = queries.reshape(seq_count, L, head_count, HD)
    key_seq = key_rows.reshape(seq_count, L, kv_count, HD)
    value_seq = value_rows.reshape(seq_count, L, kv_count, HD)
    attended, log_total = lax.map(
        lambda block_in: attend(block_in[0], block_in[1], block_in[2]),
        (query_seq, key_seq, value_seq),
    )
    attended_rows = attended.reshape(tokens, query_cols)
    part = matmul_nt(attended_rows, out_w).astype(jnp.bfloat16)
    grad_rows = out_grad.astype(jnp.bfloat16)

    hidden, norm_part, norm_other, out_part, out_pair, partial, sums_early, sums_late, *both = ffn_pass(
        shards, layer_input, part, gain_two, grad_rows, (same, below, above, across)
    )
    partial = hop(partial, lambda row, side: (row, 1 - side))
    from_below = hop(
        sums_early, lambda row, side: (row + 2, side) if row < half_line else None
    )
    from_above = hop(sums_early, lambda row, side: (row - 2, side) if row >= half_line else None)
    inv_two, norm_two = rms_parts(hidden)
    d_norm_two = norm_part.astype(jnp.float32) + norm_other.astype(jnp.float32)
    grad_gain_two = jnp.sum(d_norm_two * norm_two, axis=0)
    e_two = d_norm_two * gain_two
    d_hidden = out_grad + inv_two * (
        e_two - norm_two * jnp.mean(e_two * norm_two, axis=-1, keepdims=True)
    )
    hidden_rows = d_hidden.astype(jnp.bfloat16)
    d_attended = matmul(hidden_rows, out_w).astype(jnp.bfloat16)
    d_query, d_keys, d_values = lax.map(
        lambda block_in: attend_back(
            block_in[0], block_in[1], block_in[2], block_in[3], block_in[4], block_in[5]
        ),
        (
            query_seq,
            key_seq,
            value_seq,
            attended,
            d_attended.reshape(seq_count, L, query_cols),
            log_total,
        ),
    )
    dq_raw = (
        rotate(d_query.reshape(tokens, head_count, HD), cos_table, sin_table, -1.0)
        .astype(jnp.bfloat16)
        .reshape(tokens, query_cols)
    )
    dk_raw = (
        rotate(d_keys.reshape(tokens, kv_count, HD), cos_table, sin_table, -1.0)
        .astype(jnp.bfloat16)
        .reshape(tokens, kv_cols)
    )
    dv_rows = d_values.astype(jnp.bfloat16).reshape(tokens, kv_cols)
    d_qkv = jnp.concatenate([dq_raw, dk_raw, dv_rows], axis=1)
    norm_one_part = matmul_nt(d_qkv, qkv_w).astype(jnp.bfloat16)

    sums = grad_gain_two.reshape(shards, 1, rows)
    sums = jnp.pad(sums, ((0, 0), (0, 7), (0, max(128 - rows, 0))))
    (
        layer_output,
        x_grad,
        shard_gate,
        shard_up,
        shard_down,
        shard_out,
        shard_qkv,
        sums_out,
    ) = reduce_pass(
        shards,
        both,
        (hidden_rows, normed_one, attended_rows, d_qkv),
        (partial, sums_late, from_below, from_above),
        out_part,
        out_pair,
        norm_one_part,
        (hidden, d_hidden, norm_one),
        inv_one,
        gain_one,
        sums,
    )
    cuts = [((0, array.shape[1]),) for array in (layer_output, x_grad)]
    cuts.append(
        ((0, query_cols), (query_cols, kv_cols), (query_cols + kv_cols, kv_cols))
    )
    cuts += [((0, array.shape[1]),) for array in (shard_out, shard_gate, shard_up, shard_down)]
    (
        layer_output,
        x_grad,
        shard_query,
        shard_key,
        shard_value,
        shard_out,
        shard_gate,
        shard_up,
        shard_down,
        sums_one,
        sums_two,
    ) = emit(
        (layer_output, x_grad, shard_qkv, shard_out, shard_gate, shard_up, shard_down),
        cuts,
        sums_out,
        rows,
    )
    return (
        layer_output,
        x_grad,
        sums_one,
        shard_query,
        shard_key,
        shard_value,
        shard_out,
        sums_two,
        shard_gate,
        shard_up,
        shard_down,
    )


def solution(mesh):
    in_specs = (
        P("dp", None),
        P("dp"),
        P("dp"),
        P("dp", "tensor"),
        P("dp", "tensor"),
        P("dp", "tensor"),
        P("tensor", "dp"),
        P("dp"),
        P("dp", "tensor"),
        P("dp", "tensor"),
        P("tensor", "dp"),
        P("dp", None),
    )
    out_specs = (
        P("dp", None),
        P("dp", None),
        P("dp"),
        P("dp", "tensor"),
        P("dp", "tensor"),
        P("dp", "tensor"),
        P("tensor", "dp"),
        P("dp"),
        P("dp", "tensor"),
        P("dp", "tensor"),
        P("tensor", "dp"),
    )

    def layer(*args):
        return body(mesh.shape["dp"], *args)

    return jax.shard_map(
        layer, mesh=mesh, in_specs=in_specs, out_specs=out_specs, check_vma=False
    )
```
